128 devices in a mesh: frames: 16 (over z, y_lo, core), heads: 8 (over x, y_hi).
Axes of the slice: x: 4, y: 4 (y_hi: 2, y_lo: 2; y = y_hi * 2 + y_lo), z: 4, core: 2. Of those that a mesh axis runs over, the one named last changes fastest.
Arguments:
- clip: bfloat16 [32, 16, 128, 320], P('frames', 'heads'), may hold values from -6 to 6
- w_time: bfloat16 [3, 320, 320], replicated, may hold values from -0.1875 to 0.1875
- w_down: bfloat16 [320, 1280], replicated, may hold values from -0.3125 to 0.3125
- w_embed: bfloat16 [320, 1280], replicated, may hold values from -0.3125 to 0.3125
- w_qkv: bfloat16 [1280, 3840], P(None, 'heads'), may hold values from -0.15625 to 0.15625
- w_out: bfloat16 [1280, 1280], P('heads'), may hold values from -0.15625 to 0.15625
- w_up: bfloat16 [1280, 320], replicated, may hold values from -0.15625 to 0.15625
- timestep: int32 [1], replicated, may hold values from 0 to 999
- cotangent: bfloat16 [32, 16, 128, 320], P('frames', 'heads'), may hold values from -6 to 6
Outputs:
- output: bfloat16 [32, 16, 128, 320], P('frames', 'heads')
- grad_clip: float32 [32, 16, 128, 320], P('frames', 'heads')
- grad_time: float32 [3, 320, 320], replicated
- grad_down: float32 [320, 1280], replicated
- grad_embed: float32 [320, 1280], replicated
- grad_qkv: float32 [1280, 3840], P(None, 'heads')
- grad_out: float32 [1280, 1280], P('heads')
- grad_up: float32 [1280, 320], replicated
The draws below stay inside these ranges and needn't reach their ends.
All inputs are finite; a program needn't handle non-finite values.
Results may differ from the reference program's by a relative error of at most 0.024.
Values may be sent and summed in bfloat16 or wider, within the bound.
A program may use at most 128 MiB of HBM per device.

```python
import math
import jax
import jax.numpy as jnp
from jax import lax

C = 320
CC = 1280
HEADS = 16
HD = 80
TEMB = 320
COLS = 128
F = 32
ROWS = 16


def steps_of(own_key, shape, cuts, least, largest):
    gain = 1.0
    for position, blocks in cuts:
        draws = jax.random.uniform(jax.random.fold_in(jax.random.fold_in(own_key, 6), position), (blocks,), jnp.float32, least / len(cuts), largest / len(cuts))
        gain = gain * jnp.repeat(jnp.exp(draws), shape[position] // blocks).reshape((-1,) + (1,) * (len(shape) - 1 - position))
    return gain


def scatter_about(key, extent, scale, limit, cuts=(), held_as=jnp.bfloat16):
    level = steps_of(key, extent, cuts, -0.22, 0.18) if cuts else 1.0
    entries = jax.random.normal(key, extent, jnp.float32) * scale * level
    return jnp.minimum(jnp.maximum(entries, -limit), limit).astype(held_as)


def setup_inputs(seed: int = 0) -> dict:
    splits = jax.random.split(jax.random.key(seed), 10)
    return {
        "clip": scatter_about(splits[0], (F, ROWS, COLS, C), 1.0, 6.0, ((0, 16), (1, 8))),
        "w_time": scatter_about(splits[1], (3, C, C), (3 * C) ** -0.5, 0.1875),
        "w_down": scatter_about(splits[2], (C, CC), C ** -0.5, 0.3125),
        "w_embed": scatter_about(splits[3], (TEMB, CC), TEMB ** -0.5, 0.3125),
        "w_qkv": scatter_about(splits[4], (CC, 3 * CC), CC ** -0.5, 0.15625, ((1, 8),)),
        "w_out": scatter_about(splits[5], (CC, CC), CC ** -0.5, 0.15625, ((0, 8),)),
        "w_up": scatter_about(splits[6], (CC, C), CC ** -0.5, 0.15625),
        "timestep": jax.random.randint(splits[7], (1,), 0, 1000).astype(jnp.int32),
        "cotangent": scatter_about(splits[8], (F, ROWS, COLS, C), 1.0, 6.0, ((0, 16), (1, 8))),
    }


def matmul(left, right):
    return jnp.dot(left, right, preferred_element_type=jnp.float32)

def upsample(field):
    return jnp.repeat(jnp.repeat(jnp.repeat(field, 2, 0), 2, 1), 2, 2)

def time_embed(timestep, width):
    half = width // 2
    freqs = jnp.exp(-math.log(10000.0) * jnp.arange(half, dtype=jnp.float32) / half)
    angle = timestep.astype(jnp.float32)[0] * freqs
    return jax.nn.silu(jnp.concatenate([jnp.cos(angle), jnp.sin(angle)])).astype(jnp.bfloat16)

def reference(clip, w_time, w_down, w_embed, w_qkv, w_out, w_up, timestep, cotangent):
    frames, rows, columns, chans = clip.shape
    width = w_down.shape[1]
    half_f, half_r, half_c = (frames // 2, rows // 2, columns // 2)
    places = half_r * half_c
    scale = 1.0 / math.sqrt(HD)
    padded = jnp.pad(clip, ((1, 1), (0, 0), (0, 0), (0, 0)))
    branch = jnp.zeros((frames * rows * columns, chans), jnp.float32)
    for tap in range(3):
        branch = branch + matmul(padded[tap:tap + frames].reshape(-1, chans), w_time[tap])
    hidden = (clip.astype(jnp.float32).reshape(-1, chans) + branch).astype(jnp.bfloat16)
    hidden_f = hidden.astype(jnp.float32).reshape(frames, rows, columns, chans)
    pooled = hidden_f.reshape(half_f, 2, half_r, 2, half_c, 2, chans).mean(axis=(1, 3, 5))
    pooled = pooled.astype(jnp.bfloat16).reshape(-1, chans)
    embed = time_embed(timestep, w_embed.shape[0])
    shift = matmul(embed[None, :], w_embed)
    coarse = (matmul(pooled, w_down) + shift).astype(jnp.bfloat16)
    qkv = matmul(coarse, w_qkv).astype(jnp.bfloat16).reshape(half_f, places, HEADS, 3, HD)
    query = qkv[:, :, :, 0].astype(jnp.float32)
    keys = qkv[:, :, :, 1].astype(jnp.float32)
    values = qkv[:, :, :, 2].astype(jnp.float32)
    scores = jnp.einsum('tpnd,spnd->ntsp', query, keys) * scale
    probs = jax.nn.softmax(scores, axis=2)
    weights = probs.astype(jnp.bfloat16)
    attended = jnp.einsum('ntsp,spnd->tpnd', weights.astype(jnp.float32), values)
    attended = attended.astype(jnp.bfloat16).reshape(-1, width)
    coarse_out = (coarse.astype(jnp.float32) + matmul(attended, w_out)).astype(jnp.bfloat16)
    lifted = matmul(coarse_out, w_up).reshape(half_f, half_r, half_c, chans)
    output = (hidden_f + upsample(lifted)).astype(jnp.bfloat16)
    upstream = cotangent.astype(jnp.float32)
    pooled_grad = upstream.reshape(half_f, 2, half_r, 2, half_c, 2, chans).sum(axis=(1, 3, 5))
    pooled_grad = pooled_grad.astype(jnp.bfloat16).reshape(-1, chans)
    grad_up = matmul(coarse_out.T, pooled_grad)
    back_in = matmul(pooled_grad, w_up.T).astype(jnp.bfloat16)
    grad_out = matmul(attended.T, back_in)
    attend_grad = matmul(back_in, w_out.T).astype(jnp.bfloat16).reshape(half_f, places, HEADS, HD)
    attend_f = attend_grad.astype(jnp.float32)
    weight_grad = jnp.einsum('tpnd,spnd->ntsp', attend_f, values)
    score_grad = probs * (weight_grad - lax.optimization_barrier(jnp.sum(probs * weight_grad, axis=2, keepdims=True))) * scale
    score_f = score_grad.astype(jnp.bfloat16).astype(jnp.float32)
    query_grad = jnp.einsum('ntsp,spnd->tpnd', score_f, keys)
    keys_grad = jnp.einsum('ntsp,tpnd->spnd', score_f, query)
    values_grad = jnp.einsum('ntsp,tpnd->spnd', weights.astype(jnp.float32), attend_f)
    qkv_grad = jnp.stack([query_grad, keys_grad, values_grad], axis=3).astype(jnp.bfloat16)
    qkv_grad = qkv_grad.reshape(-1, 3 * width)
    grad_qkv = matmul(coarse.T, qkv_grad)
    coarse_grad = (matmul(qkv_grad, w_qkv.T) + back_in.astype(jnp.float32)).astype(jnp.bfloat16)
    column_sum = lax.optimization_barrier(jnp.sum(coarse_grad.astype(jnp.float32), axis=0))
    grad_embed = embed.astype(jnp.float32)[:, None] * column_sum[None, :]
    grad_down = matmul(pooled.T, coarse_grad)
    spread = matmul(coarse_grad, w_down.T).reshape(half_f, half_r, half_c, chans)
    hidden_grad = (upstream + upsample(spread) * 0.125).astype(jnp.bfloat16)
    grad_padded = jnp.pad(hidden_grad, ((1, 1), (0, 0), (0, 0), (0, 0)))
    flat_grad = hidden_grad.reshape(-1, chans)
    grad_clip = flat_grad.astype(jnp.float32)
    taps = []
    for tap in range(3):
        grad_clip = grad_clip + matmul(grad_padded[2 - tap:2 - tap + frames].reshape(-1, chans), w_time[tap].T)
        taps.append(matmul(padded[tap:tap + frames].reshape(-1, chans).T, flat_grad))
    grad_clip = grad_clip.reshape(frames, rows, columns, chans)
    grad_time = jnp.stack(taps)
    return (output, grad_clip, grad_time, grad_down, grad_embed, grad_qkv, grad_out, grad_up)
```

```python
import functools
import math

import jax
import jax.numpy as jnp
from jax import lax
from jax.experimental import pallas as pl
from jax.experimental.pallas import tpu as pltpu
from jax.sharding import PartitionSpec as P

HD = 80
MESH = pl.DeviceIdType.MESH
BF = jnp.bfloat16
F32 = jnp.float32
SCALE = 1.0 / math.sqrt(HD)
C = 320
CA = 384
CC = 1280
FPR = 1024


def mm(a, b):
    return jnp.dot(a, b, preferred_element_type=F32)


def mm_t0(a, b):
    return lax.dot_general(a, b, (((0,), (0,)), ((), ())), preferred_element_type=F32)


def mm_t1(a, b):
    return lax.dot_general(a, b, (((1,), (1,)), ((), ())), preferred_element_type=F32)


def iota(shape, dim):
    return lax.broadcasted_iota(jnp.int32, shape, dim)


def ones_where(cond):
    return jnp.where(cond, 1.0, 0.0).astype(BF)


def eye(n):
    return ones_where(iota((n, n), 0) == iota((n, n), 1))


def time_embed(timestep, width):
    half = width // 2
    freqs = jnp.exp(-math.log(10000.0) * jnp.arange(half, dtype=jnp.float32) / half)
    angle = timestep.astype(jnp.float32)[0] * freqs
    return jax.nn.silu(jnp.concatenate([jnp.cos(angle), jnp.sin(angle)])).astype(jnp.bfloat16)


class Sizes:
    def __init__(self, nf, nh, cols):
        self.nf, self.nh, self.cols = nf, nh, cols
        self.nc = nf // 2
        self.cells = 2 * cols
        self.tok = 4 * nf
        self.fr = FPR // nf
        self.yr = 2 * CC // nf
        self.ch = 32 if nh == 8 else self.yr // nh
        self.na = self.yr // self.ch


def main_kernel(
    z, clip, w_time, w_down, w_embed, w_qkv, w_out, w_up, embed, cot,
    out, grad_clip, fp_full, y_full, tap_full, w_aug,
    clip_l, clip_r, hidden, hg, hg_l, hg_r, acc,
    w_qkvp, w2, mh, wdu, w_out_t, w_aug_t,
    p_send, g_send, p_got, g_got, p_all, g_all, dg_all, att_all,
    ls_send, ls_got, slab_send, slab_got,
    fp, fp_pair, fp_sum, fp_got, tp, tp_pair, tp_sum, tp_got, tp_h, tp_hgot,
    y_send, y_got,
    halo_s, halo_r, hgs, hgr, a2a_s, a2a_r, ag_s, ag_r, rs_s, rs_r, sl_s, sl_r,
    pair_s, pair_r, fr_s, fr_r, ff_s, ff_r, fw_s, fw_r,
    th_s, th_r, ys_s, ys_r, yh_s, yh_r, yf_s, yf_r, yw_s, yw_r,
):
    nf, nh, nc = z.nf, z.nh, z.nc
    f, h = lax.axis_index("frames"), lax.axis_index("heads")
    chip, core = f // 2, lax.rem(f, 2)
    partner = chip * 2 + 1 - core

    def send(src, dst, ssem, rsem, to):
        copy = pltpu.make_async_remote_copy(
            src_ref=src, dst_ref=dst, send_sem=ssem, recv_sem=rsem, device_id=to, device_id_type=MESH
        )
        copy.start()

    def wait_send(src, sem):
        pltpu.make_async_remote_copy(
            src_ref=src, dst_ref=src, send_sem=sem, recv_sem=sem, device_id=(f, h), device_id_type=MESH
        ).wait_send()

    def wait_recv(dst, sem):
        pltpu.make_async_remote_copy(
            src_ref=dst, dst_ref=dst, send_sem=sem, recv_sem=sem, device_id=(f, h), device_id_type=MESH
        ).wait_recv()

    def other_f(k):
        return lax.rem(f + k, nf)

    def other_h(k):
        return lax.rem(h + k, nh)

    def other_c(k):
        return lax.rem(chip + k, nc)

    barrier = pltpu.get_barrier_semaphore()
    for k in range(1, nf):
        pl.semaphore_signal(barrier, inc=1, device_id=(other_f(k), h), device_id_type=MESH)
    for k in range(1, nh):
        pl.semaphore_signal(barrier, inc=1, device_id=(f, other_h(k)), device_id_type=MESH)
    pl.semaphore_wait(barrier, nf + nh - 2)

    @pl.when(f > 0)
    def _():
        send(clip.at[0], clip_r, halo_s.at[0], halo_r.at[0], (f - 1, h))

    @pl.when(f < nf - 1)
    def _():
        send(clip.at[1], clip_l, halo_s.at[1], halo_r.at[1], (f + 1, h))

    srow, scell = iota((8 * nf, z.cells), 0), iota((8 * nf, z.cells), 1)
    spos, sp = (srow // 8) * 4, lax.rem(srow, 8)
    column = lax.rem(scell, z.cols) // 2
    pool_p = ones_where((sp < 4) & (spos + sp == column))
    pool_g = ones_where((sp >= 4) & (spos + sp - 4 == column))
    g_slab = mm(pool_g, cot[0]) + mm(pool_g, cot[1])
    g_send[...] = jnp.zeros_like(g_send)
    g_send[:, :, 0:C] = g_slab.reshape(nf, 8, C).astype(BF)
    for k in range(1, nf):
        to = other_f(k)
        send(g_send.at[to], g_got.at[f], a2a_s.at[0, to], a2a_r.at[0, f], (to, h))
    g_got[f] = g_send[f]

    acc[0] = mm(clip[0], w_time[1]) + mm(clip[1], w_time[2])
    acc[1] = mm(clip[0], w_time[0]) + mm(clip[1], w_time[1])

    sel_rows, sel_cols = iota((z.tok, 8 * nf), 0), iota((z.tok, 8 * nf), 1)
    want = (sel_rows // 4) * 8 + lax.rem(sel_rows, 4)
    sel_p = ones_where(sel_cols == want)
    sel_g = ones_where(sel_cols == want + 4)

    for k in range(1, nf):
        fr = other_f(k)
        wait_recv(g_got.at[fr], a2a_r.at[0, fr])
    g_all[h] = mm(sel_g, g_got[...].astype(F32).reshape(8 * nf, CA).astype(BF)).astype(BF)
    for k in range(1, nh):
        to = other_h(k)
        send(g_all.at[h], g_all.at[h], ag_s.at[0, to], ag_r.at[0, h], (f, to))

    @pl.when(f > 0)
    def _():
        wait_recv(clip_l, halo_r.at[1])

    @pl.when(f == 0)
    def _():
        clip_l[...] = jnp.zeros_like(clip_l)

    @pl.when(f < nf - 1)
    def _():
        wait_recv(clip_r, halo_r.at[0])

    @pl.when(f == nf - 1)
    def _():
        clip_r[...] = jnp.zeros_like(clip_r)

    hidden[0] = (clip[0].astype(F32) + acc[0] + mm(clip_l[...], w_time[0])).astype(BF)
    hidden[1] = (clip[1].astype(F32) + acc[1] + mm(clip_r[...], w_time[2])).astype(BF)
    p_slab = (mm(pool_p, hidden[0]) + mm(pool_p, hidden[1])) * 0.125
    lane, prow = iota((nf, 8, CA), 2), iota((nf, 8, CA), 1)
    p_send[...] = ones_where((lane == C) & (prow < 4))
    p_send[:, :, 0:C] = p_slab.reshape(nf, 8, C).astype(BF)
    for k in range(1, nf):
        to = other_f(k)
        send(p_send.at[to], p_got.at[f], a2a_s.at[1, to], a2a_r.at[1, f], (to, h))
    p_got[f] = p_send[f]

    shift = mm(embed[...], w_embed[...])
    w_aug[0:C] = w_down[...]
    w_aug[C:CA] = jnp.where(iota((CA - C, CC), 0) == 0, jnp.broadcast_to(shift[0:1], (CA - C, CC)), 0.0).astype(BF)
    wide_row, wide_col = iota((6 * HD, 768), 0), iota((6 * HD, 768), 1)
    spread_cols = ones_where((wide_row // HD == wide_col // 128) & (lax.rem(wide_row, HD) == lax.rem(wide_col, 128)))
    w_qkvp[...] = mm(w_qkv[...], spread_cols).astype(BF)
    w2[...] = mm(w_aug[...], w_qkvp[...]).astype(BF)
    mix = mm(w_out[...], w_up[...]).astype(BF)
    mh[...] = jnp.zeros_like(mh)
    mh[0:HD, 0:C] = mix[0:HD]
    mh[128 : 128 + HD, 0:C] = mix[HD : 2 * HD]
    wdu[...] = jnp.zeros_like(wdu)
    wdu[:, 0:C] = mm(w_aug[...], w_up[...]).astype(BF)

    for k in range(1, nf):
        fr = other_f(k)
        wait_recv(p_got.at[fr], a2a_r.at[1, fr])
    p_all[h] = mm(sel_p, p_got[...].astype(F32).reshape(8 * nf, CA).astype(BF)).astype(BF)
    for k in range(1, nh):
        to = other_h(k)
        send(p_all.at[h], p_all.at[h], ag_s.at[1, to], ag_r.at[1, h], (f, to))

    w_out_t[...] = mm_t0(w_out[...], eye(2 * HD)).astype(BF)
    w_aug_t[...] = mm_t0(w_aug[...], eye(CA)).astype(BF)

    for k in range(1, nh):
        fr = other_h(k)
        wait_recv(g_all.at[fr], ag_r.at[0, fr])
        wait_recv(p_all.at[fr], ag_r.at[1, fr])

    bt = 2 * z.tok
    arow, acol = iota((bt, bt), 0), iota((bt, bt), 1)
    mask = (arow // z.tok == acol // z.tok) & (lax.rem(arow, 4) == lax.rem(acol, 4))

    def block(b, carry):
        two = pl.ds(2 * b, 2)
        rows = pl.ds(pl.multiple_of(b * bt, bt), bt)
        pb = p_all[two].reshape(bt, CA)
        gb = g_all[two].reshape(bt, CA)
        qkv = mm(pb, w2[...]).astype(BF)
        ag = mm_t1(gb, mh[...]).astype(BF)
        grads, atts = [], []
        for n in range(2):
            q, k, v = (qkv[:, (3 * n + i) * 128 : (3 * n + i + 1) * 128] for i in range(3))
            a = ag[:, n * 128 : (n + 1) * 128]
            scores = jnp.where(mask, mm_t1(q, k) * SCALE, -1e30)
            e = jnp.exp(scores - jnp.max(scores, axis=1, keepdims=True))
            probs = e / jnp.sum(e, axis=1, keepdims=True)
            weights = probs.astype(BF)
            atts.append(mm(weights, v).astype(BF))
            wg = mm_t1(a, v)
            sg = (probs * (wg - jnp.sum(probs * wg, axis=1, keepdims=True)) * SCALE).astype(BF)
            grads += [mm(sg, k).astype(BF), mm_t0(sg, q).astype(BF), mm_t0(weights, a).astype(BF)]
        dg = jnp.concatenate(grads, axis=1)
        att = jnp.concatenate(atts, axis=1)
        dg_all[rows] = dg
        att_all[rows] = att
        ls_send[two, :, 0:CA] = mm(att, mh[...]).astype(BF).reshape(2, z.tok, CA)
        ls_send[two, :, CA : 2 * CA] = mm_t1(dg, w2[...]).astype(BF).reshape(2, z.tok, CA)
        return carry

    lax.fori_loop(0, nh // 2, block, 0)

    for k in range(1, nh):
        to = other_h(k)
        send(ls_send.at[to], ls_got.at[h], rs_s.at[to], rs_r.at[h], (f, to))

    tokens = z.nh * z.tok
    p_mat, g_mat = p_all[...].reshape(tokens, CA), g_all[...].reshape(tokens, CA)
    r_pad = mm_t0(dg_all[...], p_mat)
    a_pad = mm_t0(att_all[...], g_mat)
    x_pad = mm_t0(g_mat, p_mat)
    rows_of = [r_pad[128 * i : 128 * i + HD] for i in range(6)] + [a_pad[0:HD], a_pad[128 : 128 + HD]]
    sums = jnp.concatenate(rows_of + [x_pad[0:C], jnp.zeros((FPR - 960, CA), F32)], axis=0)
    fp[...] = sums.astype(BF).reshape(nc, 2, z.fr, CA)
    send(fp.at[:, 1 - core], fp_pair, pair_s.at[0], pair_r.at[0], (partner, h))

    def reduce_scatter(own, pair, total, got, n):
        wait_recv(pair, pair_r.at[n])
        total[...] = (own[:, core].astype(F32) + pair[...].astype(F32)).astype(BF)
        for k in range(1, nc):
            to = other_c(k)
            send(total.at[to], got.at[chip], fr_s.at[n, to], fr_r.at[n, chip], (to * 2 + core, h))

    def reduced(total, got, n):
        value = total[chip].astype(F32)
        for k in range(1, nc):
            fr = other_c(k)
            wait_recv(got.at[fr], fr_r.at[n, fr])
            value = value + got[fr].astype(F32)
        return value

    def gather_start(full, ssem, rsem):
        for k in range(1, nc):
            to = other_c(k)
            send(full.at[chip, core], full.at[chip, core], ssem.at[to], rsem.at[chip], (to * 2 + core, h))

    def gather_pass(full, rsem, wsem, wrsem):
        send(full.at[chip, core], full.at[chip, core], wsem.at[chip], wrsem.at[chip], (partner, h))
        for k in range(1, nc):
            fr = other_c(k)
            wait_recv(full.at[fr, core], rsem.at[fr])
            send(full.at[fr, core], full.at[fr, core], wsem.at[fr], wrsem.at[fr], (partner, h))

    def gather_end(full, wrsem):
        for k in range(nc):
            fr = other_c(k)
            wait_recv(full.at[fr, 1 - core], wrsem.at[fr])

    reduce_scatter(fp, fp_pair, fp_sum, fp_got, 0)

    ls = ls_send[h].astype(F32)
    for k in range(1, nh):
        fr = other_h(k)
        wait_recv(ls_got.at[fr], rs_r.at[fr])
        ls = ls + ls_got[fr].astype(F32)
    ls = ls.astype(BF)
    erow, ecol = iota((8 * nf, z.tok), 0), iota((8 * nf, z.tok), 1)
    ep, et = lax.rem(erow, 8), (erow // 8) * 4
    put_l = ones_where((ep < 4) & (et + ep == ecol))
    put_s = ones_where((ep >= 4) & (et + ep - 4 == ecol))
    slab = mm(put_l, ls[:, 0:CA]) + mm(put_s, ls[:, CA : 2 * CA])
    slab_send[...] = slab.reshape(nf, 8, CA).astype(BF)
    for k in range(1, nf):
        to = other_f(k)
        send(slab_send.at[to], slab_got.at[f], sl_s.at[to], sl_r.at[f], (to, h))
    slab_got[f] = slab_send[f]

    local = mm(p_send[...].astype(F32).reshape(8 * nf, CA).astype(BF), wdu[...])
    local = local + mm_t1(g_send[...].astype(F32).reshape(8 * nf, CA).astype(BF), wdu[...])

    fp_full[chip, core] = reduced(fp_sum, fp_got, 0).astype(BF)
    gather_start(fp_full, ff_s.at[0], ff_r.at[0])

    for k in range(1, nf):
        fr = other_f(k)
        wait_recv(slab_got.at[fr], sl_r.at[fr])
    lsf = (slab_got[...].astype(F32).reshape(8 * nf, CA) + local).astype(BF)
    urow, ucol = iota((z.cells, 8 * nf), 0), iota((z.cells, 8 * nf), 1)
    upos = lax.rem(urow, z.cols) // 2
    ucell = (upos // 4) * 8 + lax.rem(upos, 4)
    up_l = ones_where(ucol == ucell)
    up_s = ones_where(ucol == ucell + 4)
    spread = mm(up_s, lsf)[:, 0:C] * 0.125
    hg[0] = (cot[0].astype(F32) + spread).astype(BF)
    hg[1] = (cot[1].astype(F32) + spread).astype(BF)

    @pl.when(f > 0)
    def _():
        send(hg.at[0], hg_r, hgs.at[0], hgr.at[0], (f - 1, h))

    @pl.when(f < nf - 1)
    def _():
        send(hg.at[1], hg_l, hgs.at[1], hgr.at[1], (f + 1, h))

    tap0 = mm_t0(clip_l[...], hg[0]) + mm_t0(clip[0], hg[1])
    tap1 = mm_t0(clip[0], hg[0]) + mm_t0(clip[1], hg[1])
    tap2 = mm_t0(clip[1], hg[0]) + mm_t0(clip_r[...], hg[1])
    taps = jnp.concatenate([tap0, tap1, tap2, jnp.zeros((FPR - 960, C), F32)], axis=0)
    tp[...] = jnp.zeros_like(tp)
    tp[:, :, :, 0:C] = taps.astype(BF).reshape(nc, 2, z.fr, C)
    send(tp.at[:, 1 - core], tp_pair, pair_s.at[1], pair_r.at[1], (partner, h))

    gather_pass(fp_full, ff_r.at[0], fw_s.at[0], fw_r.at[0])
    reduce_scatter(tp, tp_pair, tp_sum, tp_got, 1)
    lifted = mm(up_l, lsf)[:, 0:C]
    out[0] = (hidden[0].astype(F32) + lifted).astype(BF)
    out[1] = (hidden[1].astype(F32) + lifted).astype(BF)

    gather_end(fp_full, fw_r.at[0])
    whole = fp_full[...].reshape(FPR, CA)

    @pl.when(f < nf // 2)
    def _():
        rows = pl.ds(pl.multiple_of(f * z.yr, 32), z.yr)
        y_send[...] = mm(w_qkv[rows], whole[0:480]).astype(BF).reshape(z.na, z.ch, CA)

    @pl.when(f >= nf // 2)
    def _():
        rows = pl.ds(pl.multiple_of((f - nf // 2) * z.yr, 32), z.yr)
        y_send[...] = mm(w_out_t[rows], whole[480:640]).astype(BF).reshape(z.na, z.ch, CA)

    for j in range(z.na):

        @pl.when(h != j)
        def _():
            send(y_send.at[j], y_got.at[h], ys_s.at[j], ys_r.at[h], (f, j))

    tp_h[...] = reduced(tp_sum, tp_got, 1).astype(BF)
    for k in range(1, nh):
        to = other_h(k)
        send(tp_h, tp_hgot.at[h], th_s.at[to], th_r.at[h], (f, to))

    @pl.when(h < z.na)
    def _():
        value = y_send[h].astype(F32)
        for k in range(1, nh):
            fr = other_h(k)
            wait_recv(y_got.at[fr], ys_r.at[fr])
            value = value + y_got[fr].astype(F32)
        x_t = whole[640:960]

        @pl.when(f < nf // 2)
        def _():
            rows = pl.ds(pl.multiple_of(f * z.yr + h * z.ch, 32), z.ch)
            y_full[chip, core, h] = (value + mm(w_up[rows], x_t)).astype(BF)

        @pl.when(f >= nf // 2)
        def _():
            rows = pl.ds(pl.multiple_of((f - nf // 2) * z.yr + h * z.ch, 32), z.ch)
            x_part = mm_t1(w_aug_t[rows], x_t)
            y_full[chip, core, h] = value.astype(BF)
            y_full[chip, core, h, :, 0:C] = (value[:, 0:C] + x_part).astype(BF)

        for k in range(1, nh):
            to = other_h(k)
            send(y_full.at[chip, core, h], y_full.at[chip, core, h], yh_s.at[to], yh_r.at[h], (f, to))

    @pl.when(f > 0)
    def _():
        wait_recv(hg_l, hgr.at[1])

    @pl.when(f == 0)
    def _():
        hg_l[...] = jnp.zeros_like(hg_l)

    @pl.when(f < nf - 1)
    def _():
        wait_recv(hg_r, hgr.at[0])

    @pl.when(f == nf - 1)
    def _():
        hg_r[...] = jnp.zeros_like(hg_r)

    grad_clip[0] = (
        hg[0].astype(F32) + mm_t1(hg[1], w_time[0]) + mm_t1(hg[0], w_time[1]) + mm_t1(hg_l[...], w_time[2])
    )
    grad_clip[1] = (
        hg[1].astype(F32) + mm_t1(hg_r[...], w_time[0]) + mm_t1(hg[1], w_time[1]) + mm_t1(hg[0], w_time[2])
    )

    value = tp_h[...].astype(F32)
    for k in range(1, nh):
        fr = other_h(k)
        wait_recv(tp_hgot.at[fr], th_r.at[fr])
        value = value + tp_hgot[fr].astype(F32)
    tap_full[chip, core] = value.astype(BF)
    gather_start(tap_full, ff_s.at[1], ff_r.at[1])

    for j in range(z.na):

        @pl.when(h != j)
        def _():
            wait_recv(y_full.at[chip, core, j], yh_r.at[j])

    gather_start(y_full, yf_s, yf_r)
    gather_pass(tap_full, ff_r.at[1], fw_s.at[1], fw_r.at[1])
    gather_pass(y_full, yf_r, yw_s, yw_r)
    gather_end(tap_full, fw_r.at[1])
    gather_end(y_full, yw_r)

    @pl.when(f > 0)
    def _():
        wait_send(clip.at[0], halo_s.at[0])
        wait_send(hg.at[0], hgs.at[0])

    @pl.when(f < nf - 1)
    def _():
        wait_send(clip.at[1], halo_s.at[1])
        wait_send(hg.at[1], hgs.at[1])

    for k in range(1, nf):
        to = other_f(k)
        wait_send(g_send.at[to], a2a_s.at[0, to])
        wait_send(p_send.at[to], a2a_s.at[1, to])
        wait_send(slab_send.at[to], sl_s.at[to])
    for k in range(1, nh):
        to = other_h(k)
        wait_send(g_all.at[h], ag_s.at[0, to])
        wait_send(p_all.at[h], ag_s.at[1, to])
        wait_send(ls_send.at[to], rs_s.at[to])
        wait_send(tp_h, th_s.at[to])
    wait_send(fp_pair, pair_s.at[0])
    wait_send(tp_pair, pair_s.at[1])
    for k in range(1, nc):
        to = other_c(k)
        wait_send(fp_sum.at[to], fr_s.at[0, to])
        wait_send(tp_sum.at[to], fr_s.at[1, to])
        wait_send(fp_full.at[chip, core], ff_s.at[0, to])
        wait_send(tap_full.at[chip, core], ff_s.at[1, to])
        wait_send(y_full.at[chip, core], yf_s.at[to])
    for k in range(nc):
        to = other_c(k)
        wait_send(fp_full.at[to, core], fw_s.at[0, to])
        wait_send(tap_full.at[to, core], fw_s.at[1, to])
        wait_send(y_full.at[to, core], yw_s.at[to])
    for j in range(z.na):

        @pl.when(h != j)
        def _():
            wait_send(y_send.at[j], ys_s.at[j])

    @pl.when(h < z.na)
    def _():
        for k in range(1, nh):
            to = other_h(k)
            wait_send(y_full.at[chip, core, h], yh_s.at[to])


def final_kernel(
    fp_full, y_full, tap_full, w_aug, w_up, embed_col,
    grad_time, grad_down, grad_embed, grad_qkv, grad_out, grad_up,
):
    grad_time[...] = tap_full[0:960, 0:C].astype(F32)
    down = mm_t1(eye(CA), y_full[0:CC])
    grad_down[...] = down[0:C]
    grad_embed[...] = embed_col[...] * down[C : C + 1]
    grad_up[...] = y_full[CC : 2 * CC, 0:C].astype(F32)
    grad_qkv[...] = lax.dot_general(
        w_aug[...], fp_full[0:480], (((0,), (1,)), ((), ())), preferred_element_type=F32
    )
    grad_out[...] = mm_t1(fp_full[480:640, 0:C], w_up[...])


def shards(z, clip, w_time, w_down, w_embed, w_qkv, w_out, w_up, timestep, cotangent):
    nf, nh, nc = z.nf, z.nh, z.nc
    shape4 = clip.shape
    embed = time_embed(timestep, w_embed.shape[0])
    embed_rows = jnp.broadcast_to(embed[None, :], (16, C))
    vm = pl.BlockSpec(memory_space=pltpu.VMEM)
    dma = pltpu.SemaphoreType.DMA

    def bf(*shape):
        return pltpu.VMEM(shape, BF)

    frame = (z.cells, C)
    outs = pl.pallas_call(
        functools.partial(main_kernel, z),
        out_shape=(
            jax.ShapeDtypeStruct((2, *frame), BF),
            jax.ShapeDtypeStruct((2, *frame), F32),
            jax.ShapeDtypeStruct((nc, 2, z.fr, CA), BF),
            jax.ShapeDtypeStruct((nc, 2, z.na, z.ch, CA), BF),
            jax.ShapeDtypeStruct((nc, 2, z.fr, CA), BF),
            jax.ShapeDtypeStruct((CA, CC), BF),
        ),
        in_specs=[vm] * 9,
        out_specs=(vm,) * 6,
        scratch_shapes=[
            bf(*frame), bf(*frame), bf(2, *frame), bf(2, *frame), bf(*frame), bf(*frame),
            pltpu.VMEM((2, *frame), F32),
            bf(CC, 768), bf(CA, 768), bf(256, CA), bf(CA, CA), bf(CC, 2 * HD), bf(CC, CA),
            bf(nf, 8, CA), bf(nf, 8, CA), bf(nf, 8, CA), bf(nf, 8, CA),
            bf(nh, z.tok, CA), bf(nh, z.tok, CA), bf(nh * z.tok, 768), bf(nh * z.tok, 256),
            bf(nh, z.tok, 2 * CA), bf(nh, z.tok, 2 * CA), bf(nf, 8, CA), bf(nf, 8, CA),
            bf(nc, 2, z.fr, CA), bf(nc, z.fr, CA), bf(nc, z.fr, CA), bf(nc, z.fr, CA),
            bf(nc, 2, z.fr, CA), bf(nc, z.fr, CA), bf(nc, z.fr, CA), bf(nc, z.fr, CA),
            bf(z.fr, CA), bf(nh, z.fr, CA),
            bf(z.na, z.ch, CA), bf(nh, z.ch, CA),
            dma((2,)), dma((2,)), dma((2,)), dma((2,)),
            dma((2, nf)), dma((2, nf)), dma((2, nh)), dma((2, nh)),
            dma((nh,)), dma((nh,)), dma((nf,)), dma((nf,)),
            dma((2,)), dma((2,)), dma((2, nc)), dma((2, nc)),
            dma((2, nc)), dma((2, nc)), dma((2, nc)), dma((2, nc)),
            dma((nh,)), dma((nh,)), dma((nh,)), dma((nh,)),
            dma((nh,)), dma((nh,)), dma((nc,)), dma((nc,)), dma((nc,)), dma((nc,)),
        ],
        compiler_params=pltpu.CompilerParams(
            collective_id=0, has_side_effects=True, vmem_limit_bytes=60 * 1024 * 1024
        ),
    )(
        clip.reshape(2, *frame), w_time, w_down, w_embed, w_qkv, w_out, w_up, embed_rows,
        cotangent.reshape(2, *frame),
    )
    out, grad_clip, fp_full, y_full, tap_full, w_aug = outs
    grads = pl.pallas_call(
        final_kernel,
        out_shape=(
            jax.ShapeDtypeStruct((960, C), F32),
            jax.ShapeDtypeStruct((C, CC), F32),
            jax.ShapeDtypeStruct((C, CC), F32),
            jax.ShapeDtypeStruct((CC, 480), F32),
            jax.ShapeDtypeStruct((2 * HD, CC), F32),
            jax.ShapeDtypeStruct((CC, C), F32),
        ),
        in_specs=[vm] * 6,
        out_specs=(vm,) * 6,
        compiler_params=pltpu.CompilerParams(vmem_limit_bytes=48 * 1024 * 1024),
    )(
        fp_full.reshape(FPR, CA), y_full.reshape(2 * CC, CA), tap_full.reshape(FPR, CA),
        w_aug, w_up, embed.astype(F32)[:, None],
    )
    grad_time, grad_down, grad_embed, grad_qkv, grad_out, grad_up = grads
    return (
        out.reshape(shape4),
        grad_clip.reshape(shape4),
        grad_time.reshape(3, C, C),
        grad_down,
        grad_embed,
        grad_qkv,
        grad_out,
        grad_up,
    )


def solution(mesh, cols=128):
    z = Sizes(mesh.shape["frames"], mesh.shape["heads"], cols)
    return jax.shard_map(
        functools.partial(shards, z),
        mesh=mesh,
        in_specs=(
            P("frames", "heads", None, None),
            P(),
            P(),
            P(),
            P(None, "heads"),
            P("heads", None),
            P(),
            P(),
            P("frames", "heads", None, None),
        ),
        out_specs=(
            P("frames", "heads", None, None),
            P("frames", "heads", None, None),
            P(),
            P(),
            P(),
            P(None, "heads"),
            P("heads", None),
            P(),
        ),
        check_vma=False,
    )
```

```python
import functools
import math

import jax
import jax.numpy as jnp
from jax import lax
from jax.experimental import pallas as pl
from jax.experimental.pallas import tpu as pltpu
from jax.sharding import PartitionSpec as P

HD = 80
MESH = pl.DeviceIdType.MESH
BF = jnp.bfloat16
F32 = jnp.float32
SCALE = 1.0 / math.sqrt(HD)
C = 320
CA = 384
CC = 1280
LW = 2 * C
RAW = 8 * HD
FPW = RAW + 2 * CA


def mm(a, b):
    return jnp.dot(a, b, preferred_element_type=F32)


def mm_t0(a, b):
    return lax.dot_general(a, b, (((0,), (0,)), ((), ())), preferred_element_type=F32)


def mm_t1(a, b):
    return lax.dot_general(a, b, (((1,), (1,)), ((), ())), preferred_element_type=F32)


def iota(shape, dim):
    return lax.broadcasted_iota(jnp.int32, shape, dim)


def ones_where(cond):
    return jnp.where(cond, 1.0, 0.0).astype(BF)


def eye(n):
    return ones_where(iota((n, n), 0) == iota((n, n), 1))


def time_embed(timestep, width):
    half = width // 2
    freqs = jnp.exp(-math.log(10000.0) * jnp.arange(half, dtype=jnp.float32) / half)
    angle = timestep.astype(jnp.float32)[0] * freqs
    return jax.nn.silu(jnp.concatenate([jnp.cos(angle), jnp.sin(angle)])).astype(jnp.bfloat16)


class Sizes:
    def __init__(self, nf, nh, cols):
        self.nf, self.nh, self.cols = nf, nh, cols
        self.nc, self.nx = nf // 2, nh // 2
        self.cells = 2 * cols
        self.tok = 4 * nf
        self.nr = CA // nf // 8
        self.na = 6 if nh == 8 else nh
        self.ns = 2 * self.nr // self.na
        self.tr = 1024 // (2 * nh * self.nc)


def wide(frame):
    return jnp.concatenate([frame[0], frame[1]], axis=1)


def flat(slabs, width):
    value = slabs.astype(F32)
    return value.reshape(value.size // width, width).astype(BF)


def main_kernel(
    z, clip_in, w_time_in, w_down_in, w_embed_in, w_qkv_in, w_out_in, w_up_in, embed, cot_in,
    out_o, gc_o, ra_o, y_o, tap_o, w_aug_o,
    clip, w_time, w_down, w_embed, w_qkv, w_out, w_up, cot,
    out, grad_clip, ra_full, y_full, tap_full, w_aug,
    clip_l, clip_r, hidden, hg, hg_l, hg_r, acc,
    w_t, w_qkvp, w2, w2s, mh, mhl, wdu,
    p_send, g_send, p_got, g_got, p_all, g_all, dg_all, att_all,
    ls_send, ls_got, slab_send, slab_got,
    fp, fp_pair, fp_sum, fp_got, tp, tp_pair, tp_sum, tp_got, tq_sum, tq_got,
    y_send, y_got, x_buf,
    in_s, out_s,
    halo_s, halo_r, hgs, hgr, a2a_s, a2a_r, ag_s, ag_r, rs_s, rs_r, sl_s, sl_r,
    pair_s, pair_r, fr_s, fr_r, ff_s, ff_r, fw_s, fw_r,
    th_s, th_r, tf_s, tf_r, tg_s, tg_r, ta_s, ta_r, tw_s, tw_r,
    ys_s, ys_r, yh_s, yh_r, yf_s, yf_r, yw_s, yw_r,
):
    nf, nh, nc, nx = z.nf, z.nh, z.nc, z.nx
    f, h = lax.axis_index("frames"), lax.axis_index("heads")
    chip, core = f // 2, lax.rem(f, 2)
    partner = (chip * 2 + 1 - core, h)

    def send(src, dst, ssem, rsem, to):
        pltpu.make_async_remote_copy(
            src_ref=src, dst_ref=dst, send_sem=ssem, recv_sem=rsem, device_id=to, device_id_type=MESH
        ).start()

    def wait_send(src, sem):
        pltpu.make_async_remote_copy(
            src_ref=src, dst_ref=src, send_sem=sem, recv_sem=sem, device_id=(f, h), device_id_type=MESH
        ).wait_send()

    def wait_recv(dst, sem):
        pltpu.make_async_remote_copy(
            src_ref=dst, dst_ref=dst, send_sem=sem, recv_sem=sem, device_id=(f, h), device_id_type=MESH
        ).wait_recv()

    def other_f(k):
        return lax.rem(f + k, nf)

    def other_h(k):
        return lax.rem(h + k, nh)

    def other_c(k):
        return lax.rem(chip + k, nc)

    pulls = [
        (cot_in, cot), (clip_in, clip), (w_time_in, w_time), (w_embed_in, w_embed),
        (w_down_in, w_down), (w_qkv_in, w_qkv), (w_up_in, w_up), (w_out_in, w_out),
    ]
    pulls = [pltpu.make_async_copy(a, b, in_s.at[i]) for i, (a, b) in enumerate(pulls)]
    for pull in pulls:
        pull.start()

    def push(i, src, dst):
        pltpu.make_async_copy(src, dst, out_s.at[i]).start()

    barrier = pltpu.get_barrier_semaphore()
    for k in range(1, nf):
        pl.semaphore_signal(barrier, inc=1, device_id=(other_f(k), h), device_id_type=MESH)
    for k in range(1, nh):
        pl.semaphore_signal(barrier, inc=1, device_id=(f, other_h(k)), device_id_type=MESH)

    srow, scell = iota((8 * nf, z.cells), 0), iota((8 * nf, z.cells), 1)
    spos, sp = (srow // 8) * 4, lax.rem(srow, 8)
    column = lax.rem(scell, z.cols) // 2
    pool_p = ones_where((sp < 4) & (spos + sp == column))
    pool_g = ones_where((sp >= 4) & (spos + sp - 4 == column))
    pulls[0].wait()
    g_slab = mm_t1(pool_g, wide(cot[0])) + mm_t1(pool_g, wide(cot[1]))
    g_send[...] = jnp.zeros_like(g_send)
    g_send[:, :, 0:C] = g_slab.reshape(nf, 8, C).astype(BF)
    pulls[1].wait()

    pl.semaphore_wait(barrier, nf + nh - 2)

    @pl.when(f > 0)
    def _():
        send(clip.at[0], clip_r, halo_s.at[0], halo_r.at[0], (f - 1, h))

    @pl.when(f < nf - 1)
    def _():
        send(clip.at[1], clip_l, halo_s.at[1], halo_r.at[1], (f + 1, h))

    for k in range(1, nf):
        to = other_f(k)
        send(g_send.at[to], g_got.at[f], a2a_s.at[0, to], a2a_r.at[0, f], (to, h))
    g_got[f] = g_send[f]

    pulls[2].wait()
    unit = eye(C)
    for k in range(3):
        w_t[k] = mm_t0(w_time[k], unit).astype(BF)
    first, last = wide(clip[0]), wide(clip[1])
    acc[0] = mm(w_t[1], first) + mm(w_t[2], last)
    acc[1] = mm(w_t[0], first) + mm(w_t[1], last)

    sel_rows, sel_cols = iota((z.tok, 8 * nf), 0), iota((z.tok, 8 * nf), 1)
    want = (sel_rows // 4) * 8 + lax.rem(sel_rows, 4)
    sel_p = ones_where(sel_cols == want)
    sel_g = ones_where(sel_cols == want + 4)

    for k in range(1, nf):
        fr = other_f(k)
        wait_recv(g_got.at[fr], a2a_r.at[0, fr])
    g_all[h] = mm(sel_g, flat(g_got[...], CA)).astype(BF)
    for k in range(1, nh):
        to = other_h(k)
        send(g_all.at[h], g_all.at[h], ag_s.at[0, to], ag_r.at[0, h], (f, to))

    @pl.when(f > 0)
    def _():
        wait_recv(clip_l, halo_r.at[1])

    @pl.when(f == 0)
    def _():
        clip_l[...] = jnp.zeros_like(clip_l)

    @pl.when(f < nf - 1)
    def _():
        wait_recv(clip_r, halo_r.at[0])

    @pl.when(f == nf - 1)
    def _():
        clip_r[...] = jnp.zeros_like(clip_r)

    hidden[0] = (first.astype(F32) + acc[0] + mm(w_t[0], wide(clip_l))).astype(BF)
    hidden[1] = (last.astype(F32) + acc[1] + mm(w_t[2], wide(clip_r))).astype(BF)
    p_slab = (mm_t1(pool_p, hidden[0]) + mm_t1(pool_p, hidden[1])) * 0.125
    lane, prow = iota((nf, 8, CA), 2), iota((nf, 8, CA), 1)
    p_send[...] = ones_where((lane == C) & (prow < 4))
    p_send[:, :, 0:C] = p_slab.reshape(nf, 8, C).astype(BF)
    for k in range(1, nf):
        to = other_f(k)
        send(p_send.at[to], p_got.at[f], a2a_s.at[1, to], a2a_r.at[1, f], (to, h))
    p_got[f] = p_send[f]

    for pull in pulls[3:]:
        pull.wait()
    shift = mm(embed[...], w_embed[...])
    w_aug[0:C] = w_down[...]
    w_aug[C:CA] = jnp.where(iota((CA - C, CC), 0) == 0, jnp.broadcast_to(shift[0:1], (CA - C, CC)), 0.0).astype(BF)
    push(0, w_aug, w_aug_o)
    w_qkvp[...] = jnp.zeros_like(w_qkvp)
    for i in range(6):
        w_qkvp[128 * i : 128 * i + HD] = w_qkv[HD * i : HD * i + HD]
    w2_value = mm_t1(w_aug[...], w_qkvp[...]).astype(BF)
    w2[...] = w2_value
    w2s[0:C] = jnp.zeros((C, 768), BF)
    w2s[C:LW] = w2_value[0:C]
    mix = mm_t1(w_out[...], w_up[...]).astype(BF)
    for ref in (mh, mhl):
        ref[...] = jnp.zeros_like(ref)
        ref[0:HD, 0:C] = mix[0:HD]
        ref[128 : 128 + HD, 0:C] = mix[HD : 2 * HD]
    wdu[...] = jnp.zeros_like(wdu)
    wdu[:, 0:C] = mm_t1(w_aug[...], w_up[...]).astype(BF)

    for k in range(1, nf):
        fr = other_f(k)
        wait_recv(p_got.at[fr], a2a_r.at[1, fr])
    p_all[h] = mm(sel_p, flat(p_got[...], CA)).astype(BF)
    for k in range(1, nh):
        to = other_h(k)
        send(p_all.at[h], p_all.at[h], ag_s.at[1, to], ag_r.at[1, h], (f, to))

    bt = 2 * z.tok
    arow, acol = iota((bt, bt), 0), iota((bt, bt), 1)
    mask = (arow // z.tok == acol // z.tok) & (lax.rem(arow, 4) == lax.rem(acol, 4))

    def rows_needed(off):
        mine = 2 * (h // 2) + 1 - lax.rem(h, 2)
        base = 2 * lax.rem(h // 2 + off, nx)
        return [mine] if off == 0 else [base, base + 1]

    def block(off):
        b = lax.rem(h // 2 + off, nx)
        two = pl.ds(2 * b, 2)
        rows = pl.ds(pl.multiple_of(b * bt, bt), bt)
        pb = p_all[two].reshape(bt, CA)
        gb = g_all[two].reshape(bt, CA)
        qkv = mm(pb, w2[...]).astype(BF)
        ag = mm_t1(gb, mh[...]).astype(BF)
        grads, atts = [], []
        for n in range(2):
            q, k, v = (qkv[:, (3 * n + i) * 128 : (3 * n + i + 1) * 128] for i in range(3))
            a = ag[:, n * 128 : (n + 1) * 128]
            scores = jnp.where(mask, mm_t1(q, k) * SCALE, -1e30)
            e = jnp.exp(scores - jnp.max(scores, axis=1, keepdims=True))
            probs = e / jnp.sum(e, axis=1, keepdims=True)
            weights = probs.astype(BF)
            atts.append(mm(weights, v).astype(BF))
            wg = mm_t1(a, v)
            sg = (probs * (wg - jnp.sum(probs * wg, axis=1, keepdims=True)) * SCALE).astype(BF)
            grads += [mm(sg, k).astype(BF), mm_t0(sg, q).astype(BF), mm_t0(weights, a).astype(BF)]
        dg = jnp.concatenate(grads, axis=1)
        att = jnp.concatenate(atts, axis=1)
        dg_all[rows] = dg
        att_all[rows] = att
        ls_send[two] = (mm(att, mhl[...]) + mm_t1(dg, w2s[...])).astype(BF).reshape(2, z.tok, LW)

    offs = [0, 1, 3, 2] if nx == 4 else list(range(nx))
    for pair in [offs[i : i + 2] for i in range(0, nx, 2)]:
        for off in pair:
            for fr in rows_needed(off):
                wait_recv(g_all.at[fr], ag_r.at[0, fr])
                wait_recv(p_all.at[fr], ag_r.at[1, fr])
        for off in pair:
            block(off)
        for off in pair:
            for to in rows_needed(off):
                send(ls_send.at[to], ls_got.at[h], rs_s.at[to], rs_r.at[h], (f, to))

    tokens = nh * z.tok
    p_mat, g_mat = p_all[...].reshape(tokens, CA), g_all[...].reshape(tokens, CA)
    r_pad = mm_t0(p_mat, dg_all[...]).astype(BF)
    a_pad = mm_t0(g_mat, att_all[...]).astype(BF)
    rrow, rcol = iota((768, RAW), 0), iota((768, RAW), 1)
    sel_r = ones_where((rrow // 128 == rcol // HD) & (lax.rem(rrow, 128) == lax.rem(rcol, HD)))
    arow2, acol2 = iota((256, RAW), 0), iota((256, RAW), 1)
    sel_a = ones_where((arow2 // 128 + 6 == acol2 // HD) & (lax.rem(arow2, 128) == lax.rem(acol2, HD)))
    ra = mm(r_pad, sel_r) + mm(a_pad, sel_a)
    slabs = (nc, 2, z.nr, 8)
    fp[:, :, :, :, 0:RAW] = ra.reshape(*slabs, RAW).astype(BF)
    fp[:, :, :, :, RAW : RAW + CA] = mm_t0(p_mat, g_mat).reshape(*slabs, CA).astype(BF)
    fp[:, :, :, :, RAW + CA : FPW] = mm_t0(g_mat, p_mat).reshape(*slabs, CA).astype(BF)
    send(fp.at[:, 1 - core], fp_pair, pair_s.at[0], pair_r.at[0], partner)

    local = mm(flat(p_send[...], CA), wdu[...]) + mm_t1(flat(g_send[...], CA), wdu[...])

    wait_recv(fp_pair, pair_r.at[0])
    fp_sum[...] = (fp[:, core].astype(F32) + fp_pair[...].astype(F32)).astype(BF)
    for k in range(1, nc):
        to = other_c(k)
        send(fp_sum.at[to], fp_got.at[chip], fr_s.at[to], fr_r.at[chip], (to * 2 + core, h))

    ls = ls_send[h].astype(F32)
    for k in range(1, nh):
        fr = other_h(k)
        wait_recv(ls_got.at[fr], rs_r.at[fr])
        ls = ls + ls_got[fr].astype(F32)
    erow, ecol = iota((8 * nf, z.tok), 0), iota((8 * nf, z.tok), 1)
    ep, et = lax.rem(erow, 8), (erow // 8) * 4
    put_l = ones_where((ep < 4) & (et + ep == ecol))
    put_s = ones_where((ep >= 4) & (et + ep - 4 == ecol))
    slab = mm(put_l, ls[:, 0:C].astype(BF)) + mm(put_s, ls[:, C:LW].astype(BF))
    slab_send[:, :, 0:C] = slab.reshape(nf, 8, C).astype(BF)
    slab_send[:, :, C:CA] = jnp.zeros((nf, 8, CA - C), BF)
    for k in range(1, nf):
        to = other_f(k)
        send(slab_send.at[to], slab_got.at[f], sl_s.at[to], sl_r.at[f], (to, h))
    slab_got[f] = slab_send[f]

    fsum = fp_sum[chip].astype(F32)
    for k in range(1, nc):
        fr = other_c(k)
        wait_recv(fp_got.at[fr], fr_r.at[fr])
        fsum = fsum + fp_got[fr].astype(F32)
    fsum = fsum.reshape(8 * z.nr, FPW).astype(BF)
    down = mm(fsum[:, 0:480], w_qkv[...])
    lift = mm(fsum[:, 480:RAW], w_out[...])
    part = jnp.concatenate([down, lift], axis=0)
    y_send[...] = part.reshape(z.na, z.ns, 8, CC).astype(BF)
    for j in range(z.na):

        @pl.when(h != j)
        def _():
            send(y_send.at[j], y_got.at[h], ys_s.at[j], ys_r.at[h], (f, j))

    x_part = jnp.concatenate(
        [mm(fsum[:, RAW : RAW + C], w_up[...]), mm(fsum[:, RAW + CA : FPW], w_aug[...])], axis=0
    )
    x_buf[...] = x_part.reshape(z.na, z.ns, 8, CC)
    ra_full[chip, core] = fsum[:, 0:RAW].astype(F32).reshape(z.nr, 8, RAW).astype(BF)
    for k in range(1, nc):
        to = other_c(k)
        send(ra_full.at[chip, core], ra_full.at[chip, core], ff_s.at[to], ff_r.at[chip], (to * 2 + core, h))
    send(ra_full.at[chip, core], ra_full.at[chip, core], fw_s.at[chip], fw_r.at[chip], partner)

    for k in range(1, nf):
        fr = other_f(k)
        wait_recv(slab_got.at[fr], sl_r.at[fr])
    lsf = (slab_got[...].astype(F32).reshape(8 * nf, CA) + local).astype(BF)[:, 0:C]
    spread = mm_t0(lsf, pool_g) * 0.125
    grads_now = []
    for t in range(2):
        value = (wide(cot[t]).astype(F32) + spread).astype(BF)
        grads_now.append(value)
        for r in range(2):
            hg[t, r] = value[:, r * z.cols : (r + 1) * z.cols]

    @pl.when(f > 0)
    def _():
        send(hg.at[0], hg_r, hgs.at[0], hgr.at[0], (f - 1, h))

    @pl.when(f < nf - 1)
    def _():
        send(hg.at[1], hg_l, hgs.at[1], hgr.at[1], (f + 1, h))

    hg0, hg1 = grads_now
    left, right = wide(clip_l), wide(clip_r)
    taps = jnp.concatenate(
        [
            mm_t1(left, hg0) + mm_t1(first, hg1),
            mm_t1(first, hg0) + mm_t1(last, hg1),
            mm_t1(last, hg0) + mm_t1(right, hg1),
            jnp.zeros((64, C), F32),
        ],
        axis=0,
    )
    tp[...] = jnp.zeros_like(tp)
    tp[:, :, :, :, 0:C] = taps.reshape(2, nh, nc, z.tr, C).astype(BF)
    send(tp.at[1 - core], tp_pair, pair_s.at[1], pair_r.at[1], partner)

    lifted = mm_t0(lsf, pool_p)
    for t in range(2):
        value = (hidden[t].astype(F32) + lifted).astype(BF)
        for r in range(2):
            out[t, r] = value[:, r * z.cols : (r + 1) * z.cols]
    push(1, out, out_o)

    wait_recv(tp_pair, pair_r.at[1])
    tp_sum[...] = (tp[core].astype(F32) + tp_pair[...].astype(F32)).astype(BF)
    for k in range(1, nh):
        to = other_h(k)
        send(tp_sum.at[to], tp_got.at[h], th_s.at[to], th_r.at[h], (f, to))

    @pl.when(h < z.na)
    def _():
        value = y_send[h].astype(F32) + x_buf[h]
        for k in range(1, nh):
            fr = other_h(k)
            wait_recv(y_got.at[fr], ys_r.at[fr])
            value = value + y_got[fr].astype(F32)
        y_full[chip, core, h] = value.astype(BF)
        for k in range(1, nh):
            to = other_h(k)
            send(y_full.at[chip, core, h], y_full.at[chip, core, h], yh_s.at[to], yh_r.at[h], (f, to))

    for k in range(1, nc):
        fr = other_c(k)
        wait_recv(ra_full.at[fr, core], ff_r.at[fr])
        send(ra_full.at[fr, core], ra_full.at[fr, core], fw_s.at[fr], fw_r.at[fr], partner)

    value = tp_sum[h].astype(F32)
    for k in range(1, nh):
        fr = other_h(k)
        wait_recv(tp_got.at[fr], th_r.at[fr])
        value = value + tp_got[fr].astype(F32)
    tq_sum[...] = value.astype(BF)
    for k in range(1, nc):
        to = other_c(k)
        send(tq_sum.at[to], tq_got.at[chip], tf_s.at[to], tf_r.at[chip], (to * 2 + core, h))

    for j in range(z.na):

        @pl.when(h != j)
        def _():
            wait_recv(y_full.at[chip, core, j], yh_r.at[j])

    for k in range(1, nc):
        to = other_c(k)
        send(y_full.at[chip, core], y_full.at[chip, core], yf_s.at[to], yf_r.at[chip], (to * 2 + core, h))
    send(y_full.at[chip, core], y_full.at[chip, core], yw_s.at[chip], yw_r.at[chip], partner)

    @pl.when(f > 0)
    def _():
        wait_recv(hg_l, hgr.at[1])

    @pl.when(f == 0)
    def _():
        hg_l[...] = jnp.zeros_like(hg_l)

    @pl.when(f < nf - 1)
    def _():
        wait_recv(hg_r, hgr.at[0])

    @pl.when(f == nf - 1)
    def _():
        hg_r[...] = jnp.zeros_like(hg_r)

    acc[0] = hg0.astype(F32) + mm(w_time[0], hg1) + mm(w_time[1], hg0) + mm(w_time[2], wide(hg_l))
    acc[1] = hg1.astype(F32) + mm(w_time[0], wide(hg_r)) + mm(w_time[1], hg1) + mm(w_time[2], hg0)
    for t in range(2):
        for r in range(2):
            grad_clip[t, r] = acc[t, :, r * z.cols : (r + 1) * z.cols]
    push(2, grad_clip, gc_o)

    for k in range(nc):
        wait_recv(ra_full.at[other_c(k), 1 - core], fw_r.at[other_c(k)])
    push(3, ra_full, ra_o)

    value = tq_sum[chip].astype(F32)
    for k in range(1, nc):
        fr = other_c(k)
        wait_recv(tq_got.at[fr], tf_r.at[fr])
        value = value + tq_got[fr].astype(F32)
    tap_full[core, h, chip] = value.astype(BF)
    for k in range(1, nc):
        to = other_c(k)
        here = tap_full.at[core, h, chip]
        send(here, here, tg_s.at[to], tg_r.at[chip], (to * 2 + core, h))
    for k in range(1, nc):
        fr = other_c(k)
        wait_recv(tap_full.at[core, h, fr], tg_r.at[fr])
    for k in range(1, nh):
        to = other_h(k)
        send(tap_full.at[core, h], tap_full.at[core, h], ta_s.at[to], ta_r.at[h], (f, to))
    send(tap_full.at[core, h], tap_full.at[core, h], tw_s.at[h], tw_r.at[h], partner)

    for k in range(1, nc):
        fr = other_c(k)
        wait_recv(y_full.at[fr, core], yf_r.at[fr])
        send(y_full.at[fr, core], y_full.at[fr, core], yw_s.at[fr], yw_r.at[fr], partner)
    for k in range(1, nh):
        fr = other_h(k)
        wait_recv(tap_full.at[core, fr], ta_r.at[fr])
        send(tap_full.at[core, fr], tap_full.at[core, fr], tw_s.at[fr], tw_r.at[fr], partner)
    for k in range(nc):
        wait_recv(y_full.at[other_c(k), 1 - core], yw_r.at[other_c(k)])
    push(4, y_full, y_o)
    for k in range(nh):
        wait_recv(tap_full.at[1 - core, other_h(k)], tw_r.at[other_h(k)])
    push(5, tap_full, tap_o)

    @pl.when(f > 0)
    def _():
        wait_send(clip.at[0], halo_s.at[0])
        wait_send(hg.at[0], hgs.at[0])

    @pl.when(f < nf - 1)
    def _():
        wait_send(clip.at[1], halo_s.at[1])
        wait_send(hg.at[1], hgs.at[1])

    for k in range(1, nf):
        to = other_f(k)
        wait_send(g_send.at[to], a2a_s.at[0, to])
        wait_send(p_send.at[to], a2a_s.at[1, to])
        wait_send(slab_send.at[to], sl_s.at[to])
    for k in range(1, nh):
        to = other_h(k)
        wait_send(g_all.at[h], ag_s.at[0, to])
        wait_send(p_all.at[h], ag_s.at[1, to])
        wait_send(ls_send.at[to], rs_s.at[to])
        wait_send(tp_sum.at[to], th_s.at[to])
        wait_send(tap_full.at[core, h], ta_s.at[to])
    for k in range(nh):
        wait_send(tap_full.at[core, other_h(k)], tw_s.at[other_h(k)])
    wait_send(fp_pair, pair_s.at[0])
    wait_send(tp_pair, pair_s.at[1])
    for k in range(1, nc):
        to = other_c(k)
        wait_send(fp_sum.at[to], fr_s.at[to])
        wait_send(ra_full.at[chip, core], ff_s.at[to])
        wait_send(tq_sum.at[to], tf_s.at[to])
        wait_send(tap_full.at[core, h, chip], tg_s.at[to])
        wait_send(y_full.at[chip, core], yf_s.at[to])
    for k in range(nc):
        to = other_c(k)
        wait_send(ra_full.at[to, core], fw_s.at[to])
        wait_send(y_full.at[to, core], yw_s.at[to])
    for j in range(z.na):

        @pl.when(h != j)
        def _():
            wait_send(y_send.at[j], ys_s.at[j])

    @pl.when(h < z.na)
    def _():
        for k in range(1, nh):
            wait_send(y_full.at[chip, core, h], yh_s.at[other_h(k)])

    pushes = [(w_aug, w_aug_o), (out, out_o), (grad_clip, gc_o), (ra_full, ra_o), (y_full, y_o), (tap_full, tap_o)]
    for i, (a, b) in enumerate(pushes):
        pltpu.make_async_copy(a, b, out_s.at[i]).wait()


def final_kernel(
    z, ra_in, y_in, tap_in, w_aug_in, w_up_in, embed_col, out_in, gc_in,
    out_o, gc_o, time_o, down_o, embed_o, qkv_o, wout_o, up_o,
    ra, y, tap, w_aug, w_up, out, gc, time, down, emb, qkv, wout, up, in_s, out_s,
):
    pulls = [(out_in, out), (gc_in, gc), (ra_in, ra), (w_aug_in, w_aug), (w_up_in, w_up), (y_in, y), (tap_in, tap)]
    pulls = [pltpu.make_async_copy(a, b, in_s.at[i]) for i, (a, b) in enumerate(pulls)]
    for pull in pulls:
        pull.start()
    pushes = []

    def push(src, dst):
        copy = pltpu.make_async_copy(src, dst, out_s.at[len(pushes)])
        copy.start()
        pushes.append(copy)

    pulls[0].wait()
    push(out, out_o)
    pulls[1].wait()
    push(gc, gc_o)
    pulls[2].wait()
    pulls[3].wait()
    sums = flat(ra[...], RAW)
    qkv[...] = mm_t0(sums[:, 0:480], w_aug[...])
    push(qkv, qkv_o)
    pulls[4].wait()
    wout[...] = mm_t0(sums[0:C, 480:RAW], w_up[...])
    push(wout, wout_o)
    pulls[5].wait()
    both = y[...].astype(F32)
    grad_down = both[:, 0].reshape(CA, CC)
    down[...] = grad_down[0:C]
    push(down, down_o)
    emb[...] = embed_col[...] * grad_down[C : C + 1]
    push(emb, embed_o)
    up[...] = both[:, 1].reshape(CA, CC)[0:C]
    push(up, up_o)
    pulls[6].wait()
    time[...] = tap[...].astype(F32).reshape(1024, CA)[0:960, 0:C]
    push(time, time_o)
    for copy in pushes:
        copy.wait()


def shards(z, clip, w_time, w_down, w_embed, w_qkv, w_out, w_up, timestep, cotangent):
    nf, nh, nc = z.nf, z.nh, z.nc
    embed = time_embed(timestep, w_embed.shape[0])
    embed_rows = jnp.broadcast_to(embed[None, :], (16, C))
    vm = pl.BlockSpec(memory_space=pltpu.VMEM)
    hbm = pl.BlockSpec(memory_space=pl.ANY)
    dma = pltpu.SemaphoreType.DMA

    def bf(*shape):
        return pltpu.VMEM(shape, BF)

    def f32(*shape):
        return pltpu.VMEM(shape, F32)

    def like(kind, dtype):
        return jax.ShapeDtypeStruct(kind, dtype)

    frames = (2, 2, C, z.cols)
    ra_shape, y_shape = (nc, 2, z.nr, 8, RAW), (nc, 2, z.na, z.ns, 8, CC)
    tap_shape = (2, nh, nc, z.tr, CA)
    w_up_t = w_up.T
    outs = pl.pallas_call(
        functools.partial(main_kernel, z),
        out_shape=(
            like(frames, BF), like(frames, F32), like(ra_shape, BF), like(y_shape, BF),
            like(tap_shape, BF), like((CA, CC), BF),
        ),
        in_specs=[hbm] * 7 + [vm, hbm],
        out_specs=(hbm,) * 6,
        scratch_shapes=[
            bf(*frames), bf(3, C, C), bf(C, CC), bf(C, CC), bf(480, CC), bf(2 * HD, CC), bf(C, CC), bf(*frames),
            bf(*frames), f32(*frames), bf(*ra_shape), bf(*y_shape), bf(*tap_shape), bf(CA, CC),
            bf(*frames[1:]), bf(*frames[1:]), bf(2, C, z.cells), bf(*frames), bf(*frames[1:]), bf(*frames[1:]),
            f32(2, C, z.cells),
            bf(3, C, C), bf(768, CC), bf(CA, 768), bf(LW, 768), bf(256, CA), bf(256, LW), bf(CA, CA),
            bf(nf, 8, CA), bf(nf, 8, CA), bf(nf, 8, CA), bf(nf, 8, CA),
            bf(nh, z.tok, CA), bf(nh, z.tok, CA), bf(nh * z.tok, 768), bf(nh * z.tok, 256),
            bf(nh, z.tok, LW), bf(nh, z.tok, LW), bf(nf, 8, CA), bf(nf, 8, CA),
            bf(nc, 2, z.nr, 8, FPW), bf(nc, z.nr, 8, FPW), bf(nc, z.nr, 8, FPW), bf(nc, z.nr, 8, FPW),
            bf(*tap_shape), bf(nh, nc, z.tr, CA), bf(nh, nc, z.tr, CA), bf(nh, nc, z.tr, CA),
            bf(nc, z.tr, CA), bf(nc, z.tr, CA),
            bf(z.na, z.ns, 8, CC), bf(nh, z.ns, 8, CC), f32(z.na, z.ns, 8, CC),
            dma((8,)), dma((6,)),
            dma((2,)), dma((2,)), dma((2,)), dma((2,)),
            dma((2, nf)), dma((2, nf)), dma((2, nh)), dma((2, nh)),
            dma((nh,)), dma((nh,)), dma((nf,)), dma((nf,)),
            dma((2,)), dma((2,)), dma((nc,)), dma((nc,)), dma((nc,)), dma((nc,)), dma((nc,)), dma((nc,)),
            dma((nh,)), dma((nh,)), dma((nc,)), dma((nc,)), dma((nc,)), dma((nc,)),
            dma((nh,)), dma((nh,)), dma((nh,)), dma((nh,)),
            dma((nh,)), dma((nh,)), dma((nh,)), dma((nh,)), dma((nc,)), dma((nc,)), dma((nc,)), dma((nc,)),
        ],
        compiler_params=pltpu.CompilerParams(
            collective_id=0, has_side_effects=True, vmem_limit_bytes=60 * 1024 * 1024
        ),
    )(
        jnp.swapaxes(clip, 2, 3), w_time, w_down, w_embed, w_qkv.T, w_out, w_up_t, embed_rows,
        jnp.swapaxes(cotangent, 2, 3),
    )
    out, grad_clip, ra_full, y_full, tap_full, w_aug = outs
    grads = pl.pallas_call(
        functools.partial(final_kernel, z),
        out_shape=(
            like(frames, BF), like(frames, F32), like((960, C), F32), like((C, CC), F32), like((C, CC), F32),
            like((480, CC), F32), like((2 * HD, CC), F32), like((C, CC), F32),
        ),
        in_specs=[hbm] * 5 + [vm, hbm, hbm],
        out_specs=(hbm,) * 8,
        scratch_shapes=[
            bf(*ra_shape), bf(nf, 2, z.nr, 8, CC), bf(*tap_shape), bf(CA, CC), bf(C, CC), bf(*frames), f32(*frames),
            f32(960, C), f32(C, CC), f32(C, CC), f32(480, CC), f32(2 * HD, CC), f32(C, CC),
            dma((7,)), dma((8,)),
        ],
        compiler_params=pltpu.CompilerParams(vmem_limit_bytes=60 * 1024 * 1024),
    )(
        ra_full, y_full.reshape(nf, 2, z.nr, 8, CC), tap_full, w_aug, w_up_t, embed.astype(F32)[:, None],
        out, grad_clip,
    )
    out, grad_clip, grad_time, grad_down, grad_embed, grad_qkv, grad_out, grad_up = grads
    return (
        jnp.swapaxes(out, 2, 3),
        jnp.swapaxes(grad_clip, 2, 3),
        grad_time.reshape(3, C, C),
        grad_down,
        grad_embed,
        grad_qkv.T,
        grad_out,
        grad_up.T,
    )


def solution(mesh, cols=128):
    z = Sizes(mesh.shape["frames"], mesh.shape["heads"], cols)
    return jax.shard_map(
        functools.partial(shards, z),
        mesh=mesh,
        in_specs=(
            P("frames", "heads", None, None),
            P(),
            P(),
            P(),
            P(None, "heads"),
            P("heads", None),
            P(),
            P(),
            P("frames", "heads", None, None),
        ),
        out_specs=(
            P("frames", "heads", None, None),
            P("frames", "heads", None, None),
            P(),
            P(),
            P(),
            P(None, "heads"),
            P("heads", None),
            P(),
        ),
        check_vma=False,
    )
```

```python
import functools
import math

import jax
import jax.numpy as jnp
from jax import lax
from jax.experimental import pallas as pl
from jax.experimental.pallas import tpu as pltpu
from jax.sharding import PartitionSpec as P

HD = 80
MESH = pl.DeviceIdType.MESH
BF = jnp.bfloat16
F32 = jnp.float32
SCALE = 1.0 / math.sqrt(HD)
C = 320
CA = 384
CC = 1280
LW = 2 * C
RAW = 8 * HD


def mm(a, b):
    return jnp.dot(a, b, preferred_element_type=F32)


def mm_t0(a, b):
    return lax.dot_general(a, b, (((0,), (0,)), ((), ())), preferred_element_type=F32)


def mm_t1(a, b):
    return lax.dot_general(a, b, (((1,), (1,)), ((), ())), preferred_element_type=F32)


def iota(shape, dim):
    return lax.broadcasted_iota(jnp.int32, shape, dim)


def ones_where(cond):
    return jnp.where(cond, 1.0, 0.0).astype(BF)


def eye(n):
    return ones_where(iota((n, n), 0) == iota((n, n), 1))


def time_embed(timestep, width):
    half = width // 2
    freqs = jnp.exp(-math.log(10000.0) * jnp.arange(half, dtype=jnp.float32) / half)
    angle = timestep.astype(jnp.float32)[0] * freqs
    return jax.nn.silu(jnp.concatenate([jnp.cos(angle), jnp.sin(angle)])).astype(jnp.bfloat16)


class Sizes:
    def __init__(self, nf, nh, cols):
        self.nf, self.nh, self.cols = nf, nh, cols
        self.nc, self.nx = nf // 2, nh // 2
        self.cells = 2 * cols
        self.tok = 4 * nf
        self.nr = CA // nf // 8
        self.na = 6 if nh == 8 else nh
        self.ns = 2 * self.nr // self.na
        self.tr = 1024 // (2 * nh * self.nc)


def wide(frame):
    return jnp.concatenate([frame[0], frame[1]], axis=1)


def flat(slabs, width):
    value = slabs.astype(F32)
    return value.reshape(value.size // width, width).astype(BF)


def main_kernel(
    z, clip_in, w_time_in, w_down_in, w_embed_in, w_qkv_in, w_out_in, w_up_in, embed, cot_in,
    out_o, gc_o, ra_o, y_o, tap_o, w_aug_o,
    clip, w_time, w_down, w_embed, w_qkv, w_out, w_up, cot,
    out, grad_clip, ra_full, y_full, tap_full, w_aug,
    clip_l, clip_r, hidden, hg, hg_l, hg_r, acc,
    w_t, w_qkvp, w2, w2s, mh, mhl, wdu,
    p_send, g_send, p_got, g_got, p_all, g_all, dg_all, att_all,
    ls_send, ls_got, slab_send, slab_got,
    fp, fp_pair, fp_sum, fp_got, tp, tp_pair, tp_sum, tp_got, tq_sum, tq_got,
    y_send, y_got, x_buf, x_all, xs, xs_pair, xs_sum, xs_got,
    in_s, out_s, fx_s, fx_r,
    halo_s, halo_r, hgs, hgr, a2a_s, a2a_r, ag_s, ag_r, rs_s, rs_r, sl_s, sl_r,
    pair_s, pair_r, fr_s, fr_r, ff_s, ff_r, fw_s, fw_r,
    th_s, th_r, tf_s, tf_r, tg_s, tg_r, ta_s, ta_r, tw_s, tw_r,
    ys_s, ys_r, yh_s, yh_r, yf_s, yf_r, yw_s, yw_r,
):
    nf, nh, nc, nx = z.nf, z.nh, z.nc, z.nx
    f, h = lax.axis_index("frames"), lax.axis_index("heads")
    chip, core = f // 2, lax.rem(f, 2)
    partner = (chip * 2 + 1 - core, h)

    def send(src, dst, ssem, rsem, to):
        pltpu.make_async_remote_copy(
            src_ref=src, dst_ref=dst, send_sem=ssem, recv_sem=rsem, device_id=to, device_id_type=MESH
        ).start()

    def wait_send(src, sem):
        pltpu.make_async_remote_copy(
            src_ref=src, dst_ref=src, send_sem=sem, recv_sem=sem, device_id=(f, h), device_id_type=MESH
        ).wait_send()

    def wait_recv(dst, sem):
        pltpu.make_async_remote_copy(
            src_ref=dst, dst_ref=dst, send_sem=sem, recv_sem=sem, device_id=(f, h), device_id_type=MESH
        ).wait_recv()

    def other_f(k):
        return lax.rem(f + k, nf)

    def other_h(k):
        return lax.rem(h + k, nh)

    def other_c(k):
        return lax.rem(chip + k, nc)

    pulls = [
        (cot_in, cot), (clip_in, clip), (w_time_in, w_time), (w_embed_in, w_embed),
        (w_down_in, w_down), (w_qkv_in, w_qkv), (w_up_in, w_up), (w_out_in, w_out),
    ]
    pulls = [pltpu.make_async_copy(a, b, in_s.at[i]) for i, (a, b) in enumerate(pulls)]
    for pull in pulls:
        pull.start()

    def push(i, src, dst):
        pltpu.make_async_copy(src, dst, out_s.at[i]).start()

    barrier = pltpu.get_barrier_semaphore()
    for k in range(1, nf):
        pl.semaphore_signal(barrier, inc=1, device_id=(other_f(k), h), device_id_type=MESH)
    for k in range(1, nh):
        pl.semaphore_signal(barrier, inc=1, device_id=(f, other_h(k)), device_id_type=MESH)

    srow, scell = iota((8 * nf, z.cells), 0), iota((8 * nf, z.cells), 1)
    spos, sp = (srow // 8) * 4, lax.rem(srow, 8)
    column = lax.rem(scell, z.cols) // 2
    pool_p = ones_where((sp < 4) & (spos + sp == column))
    pool_g = ones_where((sp >= 4) & (spos + sp - 4 == column))
    pulls[0].wait()
    g_slab = mm_t1(pool_g, wide(cot[0])) + mm_t1(pool_g, wide(cot[1]))
    g_send[...] = jnp.zeros_like(g_send)
    g_send[:, :, 0:C] = g_slab.reshape(nf, 8, C).astype(BF)
    pulls[1].wait()

    pl.semaphore_wait(barrier, nf + nh - 2)

    @pl.when(f > 0)
    def _():
        send(clip.at[0], clip_r, halo_s.at[0], halo_r.at[0], (f - 1, h))

    @pl.when(f < nf - 1)
    def _():
        send(clip.at[1], clip_l, halo_s.at[1], halo_r.at[1], (f + 1, h))

    for k in range(1, nf):
        to = other_f(k)
        send(g_send.at[to], g_got.at[f], a2a_s.at[0, to], a2a_r.at[0, f], (to, h))
    g_got[f] = g_send[f]

    pulls[2].wait()
    unit = eye(C)
    for k in range(3):
        w_t[k] = mm_t0(w_time[k], unit).astype(BF)
    first, last = wide(clip[0]), wide(clip[1])
    acc[0] = mm(w_t[1], first) + mm(w_t[2], last)
    acc[1] = mm(w_t[0], first) + mm(w_t[1], last)

    for pull in pulls[3:]:
        pull.wait()
    shift = mm(jnp.broadcast_to(embed[...], (16, C)), w_embed[...])
    w_aug[0:C] = w_down[...]
    w_aug[C:CA] = jnp.where(iota((CA - C, CC), 0) == 0, jnp.broadcast_to(shift[0:1], (CA - C, CC)), 0.0).astype(BF)
    push(0, w_aug, w_aug_o)
    w_qkvp[...] = jnp.zeros_like(w_qkvp)
    for i in range(6):
        w_qkvp[128 * i : 128 * i + HD] = w_qkv[HD * i : HD * i + HD]
    w2_value = mm_t1(w_aug[...], w_qkvp[...]).astype(BF)
    w2[...] = w2_value
    w2s[0:C] = jnp.zeros((C, 768), BF)
    w2s[C:LW] = w2_value[0:C]
    mix = mm_t1(w_out[...], w_up[...]).astype(BF)
    for ref in (mh, mhl):
        ref[...] = jnp.zeros_like(ref)
        ref[0:HD, 0:C] = mix[0:HD]
        ref[128 : 128 + HD, 0:C] = mix[HD : 2 * HD]
    wdu[...] = jnp.zeros_like(wdu)
    wdu[:, 0:C] = mm_t1(w_aug[...], w_up[...]).astype(BF)

    sel_rows, sel_cols = iota((z.tok, 8 * nf), 0), iota((z.tok, 8 * nf), 1)
    want = (sel_rows // 4) * 8 + lax.rem(sel_rows, 4)
    sel_p = ones_where(sel_cols == want)
    sel_g = ones_where(sel_cols == want + 4)

    @pl.when(f > 0)
    def _():
        wait_recv(clip_l, halo_r.at[1])

    @pl.when(f == 0)
    def _():
        clip_l[...] = jnp.zeros_like(clip_l)

    @pl.when(f < nf - 1)
    def _():
        wait_recv(clip_r, halo_r.at[0])

    @pl.when(f == nf - 1)
    def _():
        clip_r[...] = jnp.zeros_like(clip_r)

    hidden[0] = (first.astype(F32) + acc[0] + mm(w_t[0], wide(clip_l))).astype(BF)
    hidden[1] = (last.astype(F32) + acc[1] + mm(w_t[2], wide(clip_r))).astype(BF)
    p_slab = (mm_t1(pool_p, hidden[0]) + mm_t1(pool_p, hidden[1])) * 0.125
    lane, prow = iota((nf, 8, CA), 2), iota((nf, 8, CA), 1)
    p_send[...] = ones_where((lane == C) & (prow < 4))
    p_send[:, :, 0:C] = p_slab.reshape(nf, 8, C).astype(BF)
    for k in range(1, nf):
        to = other_f(k)
        send(p_send.at[to], p_got.at[f], a2a_s.at[1, to], a2a_r.at[1, f], (to, h))
    p_got[f] = p_send[f]

    for k in range(1, nf):
        fr = other_f(k)
        wait_recv(g_got.at[fr], a2a_r.at[0, fr])
    g_all[h] = mm(sel_g, flat(g_got[...], CA)).astype(BF)
    for k in range(1, nh):
        to = other_h(k)
        send(g_all.at[h], g_all.at[h], ag_s.at[0, to], ag_r.at[0, h], (f, to))

    for k in range(1, nf):
        fr = other_f(k)
        wait_recv(p_got.at[fr], a2a_r.at[1, fr])
    p_all[h] = mm(sel_p, flat(p_got[...], CA)).astype(BF)
    for k in range(1, nh):
        to = other_h(k)
        send(p_all.at[h], p_all.at[h], ag_s.at[1, to], ag_r.at[1, h], (f, to))

    bt = 2 * z.tok
    arow, acol = iota((bt, bt), 0), iota((bt, bt), 1)
    mask = (arow // z.tok == acol // z.tok) & (lax.rem(arow, 4) == lax.rem(acol, 4))

    def rows_needed(off):
        mine = 2 * (h // 2) + 1 - lax.rem(h, 2)
        base = 2 * lax.rem(h // 2 + off, nx)
        return [mine] if off == 0 else [base, base + 1]

    def block(off):
        b = lax.rem(h // 2 + off, nx)
        two = pl.ds(2 * b, 2)
        rows = pl.ds(pl.multiple_of(b * bt, bt), bt)
        pb = p_all[two].reshape(bt, CA)
        gb = g_all[two].reshape(bt, CA)
        qkv = mm(pb, w2[...]).astype(BF)
        ag = mm_t1(gb, mh[...]).astype(BF)
        grads, atts = [], []
        for n in range(2):
            q, k, v = (qkv[:, (3 * n + i) * 128 : (3 * n + i + 1) * 128] for i in range(3))
            a = ag[:, n * 128 : (n + 1) * 128]
            scores = jnp.where(mask, mm_t1(q, k) * SCALE, -1e30)
            e = jnp.exp(scores - jnp.max(scores, axis=1, keepdims=True))
            probs = e / jnp.sum(e, axis=1, keepdims=True)
            weights = probs.astype(BF)
            atts.append(mm(weights, v).astype(BF))
            wg = mm_t1(a, v)
            sg = (probs * (wg - jnp.sum(probs * wg, axis=1, keepdims=True)) * SCALE).astype(BF)
            grads += [mm(sg, k).astype(BF), mm_t0(sg, q).astype(BF), mm_t0(weights, a).astype(BF)]
        dg = jnp.concatenate(grads, axis=1)
        att = jnp.concatenate(atts, axis=1)
        dg_all[rows] = dg
        att_all[rows] = att
        ls_send[two] = (mm(att, mhl[...]) + mm_t1(dg, w2s[...])).astype(BF).reshape(2, z.tok, LW)

    offs = [0, 1, 3, 2] if nx == 4 else list(range(nx))
    for pair in [offs[i : i + 2] for i in range(0, nx, 2)]:
        for off in pair:
            for fr in rows_needed(off):
                wait_recv(g_all.at[fr], ag_r.at[0, fr])
                wait_recv(p_all.at[fr], ag_r.at[1, fr])
        for off in pair:
            block(off)
        for off in pair:
            for to in rows_needed(off):
                send(ls_send.at[to], ls_got.at[h], rs_s.at[to], rs_r.at[h], (f, to))

    tokens = nh * z.tok
    p_mat, g_mat = p_all[...].reshape(tokens, CA), g_all[...].reshape(tokens, CA)
    r_pad = mm_t0(p_mat, dg_all[...]).astype(BF)
    a_pad = mm_t0(g_mat, att_all[...]).astype(BF)
    rrow, rcol = iota((768, RAW), 0), iota((768, RAW), 1)
    sel_r = ones_where((rrow // 128 == rcol // HD) & (lax.rem(rrow, 128) == lax.rem(rcol, HD)))
    arow2, acol2 = iota((256, RAW), 0), iota((256, RAW), 1)
    sel_a = ones_where((arow2 // 128 + 6 == acol2 // HD) & (lax.rem(arow2, 128) == lax.rem(acol2, HD)))
    ra = mm(r_pad, sel_r) + mm(a_pad, sel_a)
    slabs = (nc, 2, z.nr, 8)
    fp[...] = ra.reshape(*slabs, RAW).astype(BF)
    send(fp.at[:, 1 - core], fp_pair, pair_s.at[0], pair_r.at[0], partner)

    @pl.when(h < z.na // 2)
    def _():
        x_all[...] = mm_t0(p_mat, g_mat).reshape(*slabs, CA).astype(BF)

    @pl.when(h >= z.na // 2)
    def _():
        x_all[...] = mm_t0(g_mat, p_mat).reshape(*slabs, CA).astype(BF)

    mine = pl.ds(lax.rem(h, z.na // 2) * z.ns, z.ns)
    xs[...] = x_all[:, :, mine]
    send(xs.at[:, 1 - core], xs_pair, pair_s.at[2], pair_r.at[2], partner)

    local = mm(flat(p_send[...], CA), wdu[...]) + mm_t1(flat(g_send[...], CA), wdu[...])

    wait_recv(fp_pair, pair_r.at[0])
    fp_sum[...] = (fp[:, core].astype(F32) + fp_pair[...].astype(F32)).astype(BF)
    for k in range(1, nc):
        to = other_c(k)
        send(fp_sum.at[to], fp_got.at[chip], fr_s.at[to], fr_r.at[chip], (to * 2 + core, h))
    wait_recv(xs_pair, pair_r.at[2])
    xs_sum[...] = (xs[:, core].astype(F32) + xs_pair[...].astype(F32)).astype(BF)
    for k in range(1, nc):
        to = other_c(k)
        send(xs_sum.at[to], xs_got.at[chip], fx_s.at[to], fx_r.at[chip], (to * 2 + core, h))

    ls = ls_send[h].astype(F32)
    for k in range(1, nh):
        fr = other_h(k)
        wait_recv(ls_got.at[fr], rs_r.at[fr])
        ls = ls + ls_got[fr].astype(F32)
    erow, ecol = iota((8 * nf, z.tok), 0), iota((8 * nf, z.tok), 1)
    ep, et = lax.rem(erow, 8), (erow // 8) * 4
    put_l = ones_where((ep < 4) & (et + ep == ecol))
    put_s = ones_where((ep >= 4) & (et + ep - 4 == ecol))
    slab = mm(put_l, ls[:, 0:C].astype(BF)) + mm(put_s, ls[:, C:LW].astype(BF))
    slab_send[:, :, 0:C] = slab.reshape(nf, 8, C).astype(BF)
    slab_send[:, :, C:CA] = jnp.zeros((nf, 8, CA - C), BF)
    for k in range(1, nf):
        to = other_f(k)
        send(slab_send.at[to], slab_got.at[f], sl_s.at[to], sl_r.at[f], (to, h))
    slab_got[f] = slab_send[f]

    fsum = fp_sum[chip].astype(F32)
    for k in range(1, nc):
        fr = other_c(k)
        wait_recv(fp_got.at[fr], fr_r.at[fr])
        fsum = fsum + fp_got[fr].astype(F32)
    fsum = fsum.reshape(8 * z.nr, RAW).astype(BF)
    down = mm(fsum[:, 0:480], w_qkv[...])
    lift = mm(fsum[:, 480:RAW], w_out[...])
    part = jnp.concatenate([down, lift], axis=0)
    y_send[...] = part.reshape(z.na, z.ns, 8, CC).astype(BF)
    for j in range(z.na):

        @pl.when(h != j)
        def _():
            send(y_send.at[j], y_got.at[h], ys_s.at[j], ys_r.at[h], (f, j))

    ra_full[chip, core] = fsum[:, 0:RAW].astype(F32).reshape(z.nr, 8, RAW).astype(BF)
    for k in range(1, nf):
        fr = other_f(k)
        wait_recv(slab_got.at[fr], sl_r.at[fr])
    lsf = (slab_got[...].astype(F32).reshape(8 * nf, CA) + local).astype(BF)[:, 0:C]
    spread = mm_t0(lsf, pool_g) * 0.125
    grads_now = []
    for t in range(2):
        value = (wide(cot[t]).astype(F32) + spread).astype(BF)
        grads_now.append(value)
        for r in range(2):
            hg[t, r] = value[:, r * z.cols : (r + 1) * z.cols]

    @pl.when(f > 0)
    def _():
        send(hg.at[0], hg_r, hgs.at[0], hgr.at[0], (f - 1, h))

    @pl.when(f < nf - 1)
    def _():
        send(hg.at[1], hg_l, hgs.at[1], hgr.at[1], (f + 1, h))

    hg0, hg1 = grads_now
    left, right = wide(clip_l), wide(clip_r)
    taps = jnp.concatenate(
        [
            mm_t1(left, hg0) + mm_t1(first, hg1),
            mm_t1(first, hg0) + mm_t1(last, hg1),
            mm_t1(last, hg0) + mm_t1(right, hg1),
            jnp.zeros((64, C), F32),
        ],
        axis=0,
    )
    tp[...] = jnp.zeros_like(tp)
    tp[:, :, :, :, 0:C] = taps.reshape(2, nh, nc, z.tr, C).astype(BF)
    send(tp.at[1 - core], tp_pair, pair_s.at[1], pair_r.at[1], partner)

    @pl.when(h < z.na)
    def _():
        xsum = xs_sum[chip].astype(F32)
        for k in range(1, nc):
            fr = other_c(k)
            wait_recv(xs_got.at[fr], fx_r.at[fr])
            xsum = xsum + xs_got[fr].astype(F32)
        x_mat = xsum.reshape(8 * z.ns, CA).astype(BF)

        @pl.when(h < z.na // 2)
        def _():
            x_buf[...] = mm(x_mat[:, 0:C], w_up[...]).reshape(z.ns, 8, CC)

        @pl.when(h >= z.na // 2)
        def _():
            x_buf[...] = mm(x_mat, w_aug[...]).reshape(z.ns, 8, CC)

        value = y_send[h].astype(F32) + x_buf[...]
        for k in range(1, nh):
            fr = other_h(k)
            wait_recv(y_got.at[fr], ys_r.at[fr])
            value = value + y_got[fr].astype(F32)
        y_full[chip, core, h] = value.astype(BF)
        for k in range(1, nh):
            to = other_h(k)
            send(y_full.at[chip, core, h], y_full.at[chip, core, h], yh_s.at[to], yh_r.at[h], (f, to))

    @pl.when(h >= z.na)
    def _():
        for k in range(1, nc):
            fr = other_c(k)
            wait_recv(xs_got.at[fr], fx_r.at[fr])

    wait_recv(tp_pair, pair_r.at[1])
    tp_sum[...] = (tp[core].astype(F32) + tp_pair[...].astype(F32)).astype(BF)
    for k in range(1, nh):
        to = other_h(k)
        send(tp_sum.at[to], tp_got.at[h], th_s.at[to], th_r.at[h], (f, to))

    lifted = mm_t0(lsf, pool_p)
    for t in range(2):
        value = (hidden[t].astype(F32) + lifted).astype(BF)
        for r in range(2):
            out[t, r] = value[:, r * z.cols : (r + 1) * z.cols]
    push(1, out, out_o)

    @pl.when(f > 0)
    def _():
        wait_recv(hg_l, hgr.at[1])

    @pl.when(f == 0)
    def _():
        hg_l[...] = jnp.zeros_like(hg_l)

    @pl.when(f < nf - 1)
    def _():
        wait_recv(hg_r, hgr.at[0])

    @pl.when(f == nf - 1)
    def _():
        hg_r[...] = jnp.zeros_like(hg_r)

    acc[0] = hg0.astype(F32) + mm(w_time[0], hg1) + mm(w_time[1], hg0) + mm(w_time[2], wide(hg_l))
    acc[1] = hg1.astype(F32) + mm(w_time[0], wide(hg_r)) + mm(w_time[1], hg1) + mm(w_time[2], hg0)
    for t in range(2):
        for r in range(2):
            grad_clip[t, r] = acc[t, :, r * z.cols : (r + 1) * z.cols]
    push(2, grad_clip, gc_o)

    def y_half(i, c, k):
        return y_full.at[c, k, pl.ds(i * (z.na // 2), z.na // 2)]

    def y_start(i):
        for j in range(i * (z.na // 2), (i + 1) * (z.na // 2)):

            @pl.when(h != j)
            def _():
                wait_recv(y_full.at[chip, core, j], yh_r.at[j])

        mine = y_half(i, chip, core)
        for k in range(1, nc):
            to = other_c(k)
            send(mine, mine, yf_s.at[i, to], yf_r.at[i, chip], (to * 2 + core, h))
        send(mine, mine, yw_s.at[i, chip], yw_r.at[i, chip], partner)

    y_start(0)
    value = tp_sum[h].astype(F32)
    for k in range(1, nh):
        fr = other_h(k)
        wait_recv(tp_got.at[fr], th_r.at[fr])
        value = value + tp_got[fr].astype(F32)
    tq_sum[...] = value.astype(BF)
    for k in range(1, nc):
        to = other_c(k)
        send(tq_sum.at[to], tq_got.at[chip], tf_s.at[to], tf_r.at[chip], (to * 2 + core, h))

    value = tq_sum[chip].astype(F32)
    for k in range(1, nc):
        fr = other_c(k)
        wait_recv(tq_got.at[fr], tf_r.at[fr])
        value = value + tq_got[fr].astype(F32)
    tap_full[core, h, chip] = value.astype(BF)
    for k in range(1, nc):
        to = other_c(k)
        here = tap_full.at[core, h, chip]
        send(here, here, tg_s.at[to], tg_r.at[chip], (to * 2 + core, h))
    y_start(1)
    for k in range(1, nc):
        fr = other_c(k)
        wait_recv(tap_full.at[core, h, fr], tg_r.at[fr])
    for k in range(1, nh):
        to = other_h(k)
        send(tap_full.at[core, h], tap_full.at[core, h], ta_s.at[to], ta_r.at[h], (f, to))
    send(tap_full.at[core, h], tap_full.at[core, h], tw_s.at[h], tw_r.at[h], partner)

    for k in range(1, nc):
        to = other_c(k)
        send(ra_full.at[chip, core], ra_full.at[chip, core], ff_s.at[to], ff_r.at[chip], (to * 2 + core, h))
    send(ra_full.at[chip, core], ra_full.at[chip, core], fw_s.at[chip], fw_r.at[chip], partner)

    for i in range(2):
        for k in range(1, nc):
            fr = other_c(k)
            part = y_half(i, fr, core)
            wait_recv(part, yf_r.at[i, fr])
            send(part, part, yw_s.at[i, fr], yw_r.at[i, fr], partner)
    for k in range(1, nc):
        fr = other_c(k)
        wait_recv(ra_full.at[fr, core], ff_r.at[fr])
        send(ra_full.at[fr, core], ra_full.at[fr, core], fw_s.at[fr], fw_r.at[fr], partner)

    for k in range(1, nh):
        fr = other_h(k)
        wait_recv(tap_full.at[core, fr], ta_r.at[fr])
        send(tap_full.at[core, fr], tap_full.at[core, fr], tw_s.at[fr], tw_r.at[fr], partner)
    for k in range(nc):
        wait_recv(ra_full.at[other_c(k), 1 - core], fw_r.at[other_c(k)])
    push(3, ra_full, ra_o)

    for i in range(2):
        for k in range(nc):
            wait_recv(y_half(i, other_c(k), 1 - core), yw_r.at[i, other_c(k)])
    push(4, y_full, y_o)
    for k in range(nh):
        wait_recv(tap_full.at[1 - core, other_h(k)], tw_r.at[other_h(k)])
    push(5, tap_full, tap_o)

    @pl.when(f > 0)
    def _():
        wait_send(clip.at[0], halo_s.at[0])
        wait_send(hg.at[0], hgs.at[0])

    @pl.when(f < nf - 1)
    def _():
        wait_send(clip.at[1], halo_s.at[1])
        wait_send(hg.at[1], hgs.at[1])

    for k in range(1, nf):
        to = other_f(k)
        wait_send(g_send.at[to], a2a_s.at[0, to])
        wait_send(p_send.at[to], a2a_s.at[1, to])
        wait_send(slab_send.at[to], sl_s.at[to])
    for k in range(1, nh):
        to = other_h(k)
        wait_send(g_all.at[h], ag_s.at[0, to])
        wait_send(p_all.at[h], ag_s.at[1, to])
        wait_send(ls_send.at[to], rs_s.at[to])
        wait_send(tp_sum.at[to], th_s.at[to])
        wait_send(tap_full.at[core, h], ta_s.at[to])
    for k in range(nh):
        wait_send(tap_full.at[core, other_h(k)], tw_s.at[other_h(k)])
    wait_send(fp_pair, pair_s.at[0])
    wait_send(tp_pair, pair_s.at[1])
    wait_send(xs_pair, pair_s.at[2])
    for k in range(1, nc):
        to = other_c(k)
        wait_send(fp_sum.at[to], fr_s.at[to])
        wait_send(xs_sum.at[to], fx_s.at[to])
        wait_send(ra_full.at[chip, core], ff_s.at[to])
        wait_send(tq_sum.at[to], tf_s.at[to])
        wait_send(tap_full.at[core, h, chip], tg_s.at[to])
        for i in range(2):
            wait_send(y_half(i, chip, core), yf_s.at[i, to])
    for k in range(nc):
        to = other_c(k)
        wait_send(ra_full.at[to, core], fw_s.at[to])
        for i in range(2):
            wait_send(y_half(i, to, core), yw_s.at[i, to])
    for j in range(z.na):

        @pl.when(h != j)
        def _():
            wait_send(y_send.at[j], ys_s.at[j])

    @pl.when(h < z.na)
    def _():
        for k in range(1, nh):
            wait_send(y_full.at[chip, core, h], yh_s.at[other_h(k)])

    pushes = [(w_aug, w_aug_o), (out, out_o), (grad_clip, gc_o), (ra_full, ra_o), (y_full, y_o), (tap_full, tap_o)]
    for i, (a, b) in enumerate(pushes):
        pltpu.make_async_copy(a, b, out_s.at[i]).wait()


def final_kernel(
    z, ra_in, y_in, tap_in, w_aug_in, w_up_in, embed_row, out_in, gc_in,
    out_o, gc_o, time_o, down_o, embed_o, qkv_o, wout_o, up_o,
    ra, y, tap, w_aug, w_up, out, gc, time, down, emb, qkv, wout, up, in_s, out_s,
):
    pulls = [(y_in, y), (tap_in, tap), (ra_in, ra), (w_aug_in, w_aug), (w_up_in, w_up), (out_in, out), (gc_in, gc)]
    pulls = [pltpu.make_async_copy(a, b, in_s.at[i]) for i, (a, b) in enumerate(pulls)]
    for pull in pulls:
        pull.start()
    pushes = []

    def push(src, dst):
        copy = pltpu.make_async_copy(src, dst, out_s.at[len(pushes)])
        copy.start()
        pushes.append(copy)

    pulls[0].wait()
    grad_down = y[:, 0].astype(F32).reshape(CA, CC)
    down[...] = grad_down[0:C]
    push(down, down_o)
    emb[...] = mm_t1(eye(C), jnp.broadcast_to(embed_row[...], (16, C)))[:, 0:1] * grad_down[C : C + 1]
    push(emb, embed_o)
    up[...] = y[:, 1].astype(F32).reshape(CA, CC)[0:C]
    push(up, up_o)
    pulls[1].wait()
    time[...] = tap[...].astype(F32).reshape(1024, CA)[0:960, 0:C]
    push(time, time_o)
    pulls[2].wait()
    pulls[3].wait()
    sums = flat(ra[...], RAW)
    qkv[...] = mm_t0(sums[:, 0:480], w_aug[...])
    push(qkv, qkv_o)
    pulls[4].wait()
    wout[...] = mm_t0(sums[0:C, 480:RAW], w_up[...])
    push(wout, wout_o)
    pulls[5].wait()
    push(out, out_o)
    pulls[6].wait()
    push(gc, gc_o)
    for copy in pushes:
        copy.wait()


def shards(z, clip, w_time, w_down, w_embed, w_qkv, w_out, w_up, timestep, cotangent):
    nf, nh, nc = z.nf, z.nh, z.nc
    embed = time_embed(timestep, w_embed.shape[0])
    embed_row = embed[None, :]
    vm = pl.BlockSpec(memory_space=pltpu.VMEM)
    hbm = pl.BlockSpec(memory_space=pl.ANY)
    dma = pltpu.SemaphoreType.DMA

    def bf(*shape):
        return pltpu.VMEM(shape, BF)

    def f32(*shape):
        return pltpu.VMEM(shape, F32)

    def like(kind, dtype):
        return jax.ShapeDtypeStruct(kind, dtype)

    frames = (2, 2, C, z.cols)
    ra_shape, y_shape = (nc, 2, z.nr, 8, RAW), (nc, 2, z.na, z.ns, 8, CC)
    tap_shape = (2, nh, nc, z.tr, CA)
    w_up_t = w_up.T
    outs = pl.pallas_call(
        functools.partial(main_kernel, z),
        out_shape=(
            like(frames, BF), like(frames, F32), like(ra_shape, BF), like(y_shape, BF),
            like(tap_shape, BF), like((CA, CC), BF),
        ),
        in_specs=[hbm] * 7 + [vm, hbm],
        out_specs=(hbm,) * 6,
        scratch_shapes=[
            bf(*frames), bf(3, C, C), bf(C, CC), bf(C, CC), bf(480, CC), bf(2 * HD, CC), bf(C, CC), bf(*frames),
            bf(*frames), f32(*frames), bf(*ra_shape), bf(*y_shape), bf(*tap_shape), bf(CA, CC),
            bf(*frames[1:]), bf(*frames[1:]), bf(2, C, z.cells), bf(*frames), bf(*frames[1:]), bf(*frames[1:]),
            f32(2, C, z.cells),
            bf(3, C, C), bf(768, CC), bf(CA, 768), bf(LW, 768), bf(256, CA), bf(256, LW), bf(CA, CA),
            bf(nf, 8, CA), bf(nf, 8, CA), bf(nf, 8, CA), bf(nf, 8, CA),
            bf(nh, z.tok, CA), bf(nh, z.tok, CA), bf(nh * z.tok, 768), bf(nh * z.tok, 256),
            bf(nh, z.tok, LW), bf(nh, z.tok, LW), bf(nf, 8, CA), bf(nf, 8, CA),
            bf(*ra_shape), bf(nc, z.nr, 8, RAW), bf(nc, z.nr, 8, RAW), bf(nc, z.nr, 8, RAW),
            bf(*tap_shape), bf(nh, nc, z.tr, CA), bf(nh, nc, z.tr, CA), bf(nh, nc, z.tr, CA),
            bf(nc, z.tr, CA), bf(nc, z.tr, CA),
            bf(z.na, z.ns, 8, CC), bf(nh, z.ns, 8, CC), f32(z.ns, 8, CC),
            bf(nc, 2, z.nr, 8, CA), bf(nc, 2, z.ns, 8, CA), bf(nc, z.ns, 8, CA), bf(nc, z.ns, 8, CA), bf(nc, z.ns, 8, CA),
            dma((8,)), dma((6,)), dma((nc,)), dma((nc,)),
            dma((2,)), dma((2,)), dma((2,)), dma((2,)),
            dma((2, nf)), dma((2, nf)), dma((2, nh)), dma((2, nh)),
            dma((nh,)), dma((nh,)), dma((nf,)), dma((nf,)),
            dma((3,)), dma((3,)), dma((nc,)), dma((nc,)), dma((nc,)), dma((nc,)), dma((nc,)), dma((nc,)),
            dma((nh,)), dma((nh,)), dma((nc,)), dma((nc,)), dma((nc,)), dma((nc,)),
            dma((nh,)), dma((nh,)), dma((nh,)), dma((nh,)),
            dma((nh,)), dma((nh,)), dma((nh,)), dma((nh,)), dma((2, nc)), dma((2, nc)), dma((2, nc)), dma((2, nc)),
        ],
        compiler_params=pltpu.CompilerParams(
            collective_id=0, has_side_effects=True, vmem_limit_bytes=60 * 1024 * 1024
        ),
    )(
        jnp.swapaxes(clip, 2, 3), w_time, w_down, w_embed, w_qkv.T, w_out, w_up_t, embed_row,
        jnp.swapaxes(cotangent, 2, 3),
    )
    out, grad_clip, ra_full, y_full, tap_full, w_aug = outs
    grads = pl.pallas_call(
        functools.partial(final_kernel, z),
        out_shape=(
            like(frames, BF), like(frames, F32), like((960, C), F32), like((C, CC), F32), like((C, CC), F32),
            like((480, CC), F32), like((2 * HD, CC), F32), like((C, CC), F32),
        ),
        in_specs=[hbm] * 5 + [vm, hbm, hbm],
        out_specs=(hbm,) * 8,
        scratch_shapes=[
            bf(*ra_shape), bf(nf, 2, z.nr, 8, CC), bf(*tap_shape), bf(CA, CC), bf(C, CC), bf(*frames), f32(*frames),
            f32(960, C), f32(C, CC), f32(C, CC), f32(480, CC), f32(2 * HD, CC), f32(C, CC),
            dma((7,)), dma((8,)),
        ],
        compiler_params=pltpu.CompilerParams(vmem_limit_bytes=60 * 1024 * 1024),
    )(
        ra_full, y_full.reshape(nf, 2, z.nr, 8, CC), tap_full, w_aug, w_up_t, embed_row,
        out, grad_clip,
    )
    out, grad_clip, grad_time, grad_down, grad_embed, grad_qkv, grad_out, grad_up = grads
    return (
        jnp.swapaxes(out, 2, 3),
        jnp.swapaxes(grad_clip, 2, 3),
        grad_time.reshape(3, C, C),
        grad_down,
        grad_embed,
        grad_qkv.T,
        grad_out,
        grad_up.T,
    )


def solution(mesh, cols=128):
    z = Sizes(mesh.shape["frames"], mesh.shape["heads"], cols)
    return jax.shard_map(
        functools.partial(shards, z),
        mesh=mesh,
        in_specs=(
            P("frames", "heads", None, None),
            P(),
            P(),
            P(),
            P(None, "heads"),
            P("heads", None),
            P(),
            P(),
            P("frames", "heads", None, None),
        ),
        out_specs=(
            P("frames", "heads", None, None),
            P("frames", "heads", None, None),
            P(),
            P(),
            P(),
            P(None, "heads"),
            P("heads", None),
            P(),
        ),
        check_vma=False,
    )
```

```python
import functools
import math

import jax
import jax.numpy as jnp
from jax import lax
from jax.experimental import pallas as pl
from jax.experimental.pallas import tpu as pltpu
from jax.sharding import PartitionSpec as P

HD = 80
MESH = pl.DeviceIdType.MESH
BF = jnp.bfloat16
F32 = jnp.float32
SCALE = 1.0 / math.sqrt(HD)
C = 320
CA = 384
CC = 1280
LW = 2 * C
RAW = 8 * HD


def mm(a, b):
    return jnp.dot(a, b, preferred_element_type=F32)


def mm_t0(a, b):
    return lax.dot_general(a, b, (((0,), (0,)), ((), ())), preferred_element_type=F32)


def mm_t1(a, b):
    return lax.dot_general(a, b, (((1,), (1,)), ((), ())), preferred_element_type=F32)


def iota(shape, dim):
    return lax.broadcasted_iota(jnp.int32, shape, dim)


def ones_where(cond):
    return jnp.where(cond, 1.0, 0.0).astype(BF)


def eye(n):
    return ones_where(iota((n, n), 0) == iota((n, n), 1))


def time_embed(timestep, width):
    half = width // 2
    freqs = jnp.exp(-math.log(10000.0) * jnp.arange(half, dtype=jnp.float32) / half)
    angle = timestep.astype(jnp.float32)[0] * freqs
    return jax.nn.silu(jnp.concatenate([jnp.cos(angle), jnp.sin(angle)])).astype(jnp.bfloat16)


class Sizes:
    def __init__(self, nf, nh, cols):
        self.nf, self.nh, self.cols = nf, nh, cols
        self.nc, self.nx = nf // 2, nh // 2
        self.cells = 2 * cols
        self.tok = 4 * nf
        self.nr = CA // nf // 8
        self.na = 6 if nh == 8 else nh
        self.ns = 2 * self.nr // self.na
        self.tr = 1024 // (2 * nh * self.nc)


def wide(frame):
    return jnp.concatenate([frame[0], frame[1]], axis=1)


def flat(slabs, width):
    value = slabs.astype(F32)
    return value.reshape(value.size // width, width).astype(BF)


def main_kernel(
    z, clip_in, w_time_in, w_down_in, w_embed_in, w_qkv_in, w_out_in, w_up_in, embed, cot_in,
    out_o, gc_o, ra_o, y_o, tap_o, w_aug_o,
    clip, w_time, w_down, w_embed, w_qkv, w_out, w_up, cot,
    out, grad_clip, ra_full, y_full, tap_full, w_aug,
    clip_l, clip_r, hidden, hg, hg_l, hg_r, acc,
    w_t, w_qkvp, w2, w2s, mh, mhl, wdu,
    p_send, g_send, p_got, g_got, p_all, g_all, dg_all, att_all,
    ls_send, ls_got, slab_send, slab_got,
    fp, fp_pair, fp_sum, fp_got, tp, tp_pair, tp_sum, tp_got, tq_sum, tq_got,
    y_send, y_got, x_buf, x_all, xs, xs_pair, xs_sum, xs_got,
    in_s, out_s, fx_s, fx_r, yx_s, yx_r,
    halo_s, halo_r, hgs, hgr, a2a_s, a2a_r, ag_s, ag_r, rs_s, rs_r, sl_s, sl_r,
    pair_s, pair_r, fr_s, fr_r, ff_s, ff_r, fw_s, fw_r,
    th_s, th_r, tf_s, tf_r, tg_s, tg_r, ta_s, ta_r, tw_s, tw_r,
    ys_s, ys_r, yh_s, yh_r, yf_s, yf_r, yw_s, yw_r,
):
    nf, nh, nc, nx, nz = z.nf, z.nh, z.nc, z.nx, z.nc // 2
    f, h = lax.axis_index("frames"), lax.axis_index("heads")
    chip, core = f // 2, lax.rem(f, 2)
    partner = (chip * 2 + 1 - core, h)

    def send(src, dst, ssem, rsem, to):
        pltpu.make_async_remote_copy(
            src_ref=src, dst_ref=dst, send_sem=ssem, recv_sem=rsem, device_id=to, device_id_type=MESH
        ).start()

    def wait_send(src, sem):
        pltpu.make_async_remote_copy(
            src_ref=src, dst_ref=src, send_sem=sem, recv_sem=sem, device_id=(f, h), device_id_type=MESH
        ).wait_send()

    def wait_recv(dst, sem):
        pltpu.make_async_remote_copy(
            src_ref=dst, dst_ref=dst, send_sem=sem, recv_sem=sem, device_id=(f, h), device_id_type=MESH
        ).wait_recv()

    def other_f(k):
        return lax.rem(f + k, nf)

    def other_h(k):
        return lax.rem(h + k, nh)

    def heads_out():
        for off in ([2, nx - 1, 1, 0] if nx == 4 else range(nx)):
            base = 2 * lax.rem(h // 2 + off, nx)
            if off == 0:
                yield base + 1 - lax.rem(h, 2)
            else:
                yield base + lax.rem(h, 2)
                yield base + 1 - lax.rem(h, 2)

    def other_c(k):
        return lax.rem(chip + k, nc)

    pulls = [
        (cot_in, cot), (clip_in, clip), (w_time_in, w_time), (w_embed_in, w_embed),
        (w_down_in, w_down), (w_qkv_in, w_qkv), (w_up_in, w_up), (w_out_in, w_out),
    ]
    pulls = [pltpu.make_async_copy(a, b, in_s.at[i]) for i, (a, b) in enumerate(pulls)]
    for pull in pulls:
        pull.start()

    def push(i, src, dst):
        pltpu.make_async_copy(src, dst, out_s.at[i]).start()

    barrier = pltpu.get_barrier_semaphore()
    for k in range(1, nf):
        pl.semaphore_signal(barrier, inc=1, device_id=(other_f(k), h), device_id_type=MESH)
    for k in range(1, nh):
        pl.semaphore_signal(barrier, inc=1, device_id=(f, other_h(k)), device_id_type=MESH)

    srow, scell = iota((8 * nf, z.cells), 0), iota((8 * nf, z.cells), 1)
    spos, sp = (srow // 8) * 4, lax.rem(srow, 8)
    column = lax.rem(scell, z.cols) // 2
    pool_p = ones_where((sp < 4) & (spos + sp == column))
    pool_g = ones_where((sp >= 4) & (spos + sp - 4 == column))
    pulls[0].wait()
    g_slab = mm_t1(pool_g, wide(cot[0])) + mm_t1(pool_g, wide(cot[1]))
    g_send[...] = jnp.zeros_like(g_send)
    g_send[:, :, 0:C] = g_slab.reshape(nf, 8, C).astype(BF)
    pulls[1].wait()

    pl.semaphore_wait(barrier, nf + nh - 2)

    @pl.when(f > 0)
    def _():
        send(clip.at[0], clip_r, halo_s.at[0], halo_r.at[0], (f - 1, h))

    @pl.when(f < nf - 1)
    def _():
        send(clip.at[1], clip_l, halo_s.at[1], halo_r.at[1], (f + 1, h))

    for k in range(1, nf):
        to = other_f(k)
        send(g_send.at[to], g_got.at[f], a2a_s.at[0, to], a2a_r.at[0, f], (to, h))
    g_got[f] = g_send[f]

    pulls[2].wait()
    unit = eye(C)
    for k in range(3):
        w_t[k] = mm_t0(w_time[k], unit).astype(BF)
    first, last = wide(clip[0]), wide(clip[1])
    acc[0] = mm(w_t[1], first) + mm(w_t[2], last)
    acc[1] = mm(w_t[0], first) + mm(w_t[1], last)

    for pull in pulls[3:]:
        pull.wait()
    shift = mm(jnp.broadcast_to(embed[...], (16, C)), w_embed[...])
    w_aug[0:C] = w_down[...]
    w_aug[C:CA] = jnp.where(iota((CA - C, CC), 0) == 0, jnp.broadcast_to(shift[0:1], (CA - C, CC)), 0.0).astype(BF)
    push(0, w_aug, w_aug_o)
    w_qkvp[...] = jnp.zeros_like(w_qkvp)
    for i in range(6):
        w_qkvp[128 * i : 128 * i + HD] = w_qkv[HD * i : HD * i + HD]
    w2_value = mm_t1(w_aug[...], w_qkvp[...]).astype(BF)
    w2[...] = w2_value
    w2s[0:C] = jnp.zeros((C, 768), BF)
    w2s[C:LW] = w2_value[0:C]
    mix = mm_t1(w_out[...], w_up[...]).astype(BF)
    for ref in (mh, mhl):
        ref[...] = jnp.zeros_like(ref)
        ref[0:HD, 0:C] = mix[0:HD]
        ref[128 : 128 + HD, 0:C] = mix[HD : 2 * HD]
    wdu[...] = jnp.zeros_like(wdu)
    wdu[:, 0:C] = mm_t1(w_aug[...], w_up[...]).astype(BF)

    sel_rows, sel_cols = iota((z.tok, 8 * nf), 0), iota((z.tok, 8 * nf), 1)
    want = (sel_rows // 4) * 8 + lax.rem(sel_rows, 4)
    sel_p = ones_where(sel_cols == want)
    sel_g = ones_where(sel_cols == want + 4)

    @pl.when(f > 0)
    def _():
        wait_recv(clip_l, halo_r.at[1])

    @pl.when(f == 0)
    def _():
        clip_l[...] = jnp.zeros_like(clip_l)

    @pl.when(f < nf - 1)
    def _():
        wait_recv(clip_r, halo_r.at[0])

    @pl.when(f == nf - 1)
    def _():
        clip_r[...] = jnp.zeros_like(clip_r)

    hidden[0] = (first.astype(F32) + acc[0] + mm(w_t[0], wide(clip_l))).astype(BF)
    hidden[1] = (last.astype(F32) + acc[1] + mm(w_t[2], wide(clip_r))).astype(BF)
    p_slab = (mm_t1(pool_p, hidden[0]) + mm_t1(pool_p, hidden[1])) * 0.125
    lane, prow = iota((nf, 8, CA), 2), iota((nf, 8, CA), 1)
    p_send[...] = ones_where((lane == C) & (prow < 4))
    p_send[:, :, 0:C] = p_slab.reshape(nf, 8, C).astype(BF)
    for k in range(1, nf):
        to = other_f(k)
        send(p_send.at[to], p_got.at[f], a2a_s.at[1, to], a2a_r.at[1, f], (to, h))
    p_got[f] = p_send[f]

    for k in range(1, nf):
        fr = other_f(k)
        wait_recv(g_got.at[fr], a2a_r.at[0, fr])
    g_all[h] = mm(sel_g, flat(g_got[...], CA)).astype(BF)
    for to in heads_out():
        send(g_all.at[h], g_all.at[h], ag_s.at[0, to], ag_r.at[0, h], (f, to))

    for k in range(1, nf):
        fr = other_f(k)
        wait_recv(p_got.at[fr], a2a_r.at[1, fr])
    p_all[h] = mm(sel_p, flat(p_got[...], CA)).astype(BF)
    for to in heads_out():
        send(p_all.at[h], p_all.at[h], ag_s.at[1, to], ag_r.at[1, h], (f, to))

    bt = 2 * z.tok
    arow, acol = iota((bt, bt), 0), iota((bt, bt), 1)
    mask = (arow // z.tok == acol // z.tok) & (lax.rem(arow, 4) == lax.rem(acol, 4))

    def rows_needed(off):
        mine = 2 * (h // 2) + 1 - lax.rem(h, 2)
        base = 2 * lax.rem(h // 2 + off, nx)
        return [mine] if off == 0 else [base, base + 1]

    def blocks(group):
        where = [lax.rem(h // 2 + off, nx) for off in group]
        twos = [pl.ds(2 * b, 2) for b in where]
        pb = jnp.concatenate([p_all[two].reshape(bt, CA) for two in twos], axis=0)
        gb = jnp.concatenate([g_all[two].reshape(bt, CA) for two in twos], axis=0)
        qkv = mm(pb, w2[...]).astype(BF)
        ag = mm_t1(gb, mh[...]).astype(BF)
        dgs, atts = [], []
        for i, b in enumerate(where):
            grads, att = [], []
            for n in range(2):
                own = slice(i * bt, (i + 1) * bt)
                q, k, v = (qkv[own, (3 * n + m) * 128 : (3 * n + m + 1) * 128] for m in range(3))
                a = ag[own, n * 128 : (n + 1) * 128]
                scores = jnp.where(mask, mm_t1(q, k) * SCALE, -1e30)
                e = jnp.exp(scores - jnp.max(scores, axis=1, keepdims=True))
                probs = e / jnp.sum(e, axis=1, keepdims=True)
                weights = probs.astype(BF)
                att.append(mm(weights, v).astype(BF))
                wg = mm_t1(a, v)
                sg = (probs * (wg - jnp.sum(probs * wg, axis=1, keepdims=True)) * SCALE).astype(BF)
                grads += [mm(sg, k).astype(BF), mm_t0(sg, q).astype(BF), mm_t0(weights, a).astype(BF)]
            dgs.append(jnp.concatenate(grads, axis=1))
            atts.append(jnp.concatenate(att, axis=1))
            rows = pl.ds(pl.multiple_of(b * bt, bt), bt)
            dg_all[rows] = dgs[i]
            att_all[rows] = atts[i]
        dg, att = jnp.concatenate(dgs, axis=0), jnp.concatenate(atts, axis=0)
        ls = (mm(att, mhl[...]) + mm_t1(dg, w2s[...])).astype(BF)
        for i, two in enumerate(twos):
            ls_send[two] = ls[i * bt : (i + 1) * bt].reshape(2, z.tok, LW)

    for group in [[2, 1], [3, 0]] if nx == 4 else [list(range(nx))]:
        for off in group:
            for fr in rows_needed(off):
                wait_recv(g_all.at[fr], ag_r.at[0, fr])
                wait_recv(p_all.at[fr], ag_r.at[1, fr])
        blocks(group)
        for off in group:
            for to in rows_needed(off):
                send(ls_send.at[to], ls_got.at[h], rs_s.at[to], rs_r.at[h], (f, to))

    tokens = nh * z.tok
    p_mat, g_mat = p_all[...].reshape(tokens, CA), g_all[...].reshape(tokens, CA)
    r_pad = mm_t0(p_mat, dg_all[...]).astype(BF)
    a_pad = mm_t0(g_mat, att_all[...]).astype(BF)
    rrow, rcol = iota((768, RAW), 0), iota((768, RAW), 1)
    sel_r = ones_where((rrow // 128 == rcol // HD) & (lax.rem(rrow, 128) == lax.rem(rcol, HD)))
    arow2, acol2 = iota((256, RAW), 0), iota((256, RAW), 1)
    sel_a = ones_where((arow2 // 128 + 6 == acol2 // HD) & (lax.rem(arow2, 128) == lax.rem(acol2, HD)))
    ra = mm(r_pad, sel_r) + mm(a_pad, sel_a)
    slabs = (nc, 2, z.nr, 8)
    fp[...] = ra.reshape(*slabs, RAW).astype(BF)
    send(fp.at[:, 1 - core], fp_pair, pair_s.at[0], pair_r.at[0], partner)

    @pl.when(h < z.na // 2)
    def _():
        x_all[...] = mm_t0(p_mat, g_mat).reshape(*slabs, CA).astype(BF)

    @pl.when(h >= z.na // 2)
    def _():
        x_all[...] = mm_t0(g_mat, p_mat).reshape(*slabs, CA).astype(BF)

    mine = pl.ds(lax.rem(h, z.na // 2) * z.ns, z.ns)
    xs[...] = x_all[:, :, mine]
    send(xs.at[:, 1 - core], xs_pair, pair_s.at[2], pair_r.at[2], partner)

    local = mm(flat(p_send[...], CA), wdu[...]) + mm_t1(flat(g_send[...], CA), wdu[...])

    wait_recv(fp_pair, pair_r.at[0])
    fp_sum[...] = (fp[:, core].astype(F32) + fp_pair[...].astype(F32)).astype(BF)
    for k in range(1, nc):
        to = other_c(k)
        send(fp_sum.at[to], fp_got.at[chip], fr_s.at[to], fr_r.at[chip], (to * 2 + core, h))
    wait_recv(xs_pair, pair_r.at[2])
    xs_sum[...] = (xs[:, core].astype(F32) + xs_pair[...].astype(F32)).astype(BF)
    for k in range(1, nc):
        to = other_c(k)
        send(xs_sum.at[to], xs_got.at[chip], fx_s.at[to], fx_r.at[chip], (to * 2 + core, h))

    ls = ls_send[h].astype(F32)
    for k in range(1, nh):
        fr = other_h(k)
        wait_recv(ls_got.at[fr], rs_r.at[fr])
        ls = ls + ls_got[fr].astype(F32)
    erow, ecol = iota((8 * nf, z.tok), 0), iota((8 * nf, z.tok), 1)
    ep, et = lax.rem(erow, 8), (erow // 8) * 4
    put_l = ones_where((ep < 4) & (et + ep == ecol))
    put_s = ones_where((ep >= 4) & (et + ep - 4 == ecol))
    slab = mm(put_l, ls[:, 0:C].astype(BF)) + mm(put_s, ls[:, C:LW].astype(BF))
    slab_send[:, :, 0:C] = slab.reshape(nf, 8, C).astype(BF)
    slab_send[:, :, C:CA] = jnp.zeros((nf, 8, CA - C), BF)
    for k in range(1, nf):
        to = other_f(k)
        send(slab_send.at[to], slab_got.at[f], sl_s.at[to], sl_r.at[f], (to, h))
    slab_got[f] = slab_send[f]

    fsum = fp_sum[chip].astype(F32)
    for k in range(1, nc):
        fr = other_c(k)
        wait_recv(fp_got.at[fr], fr_r.at[fr])
        fsum = fsum + fp_got[fr].astype(F32)
    fsum = fsum.reshape(8 * z.nr, RAW).astype(BF)
    down = mm(fsum[:, 0:480], w_qkv[...])
    lift = mm(fsum[:, 480:RAW], w_out[...])
    part = jnp.concatenate([down, lift], axis=0)
    y_send[...] = part.reshape(z.na, z.ns, 8, CC).astype(BF)
    for j in range(z.na):

        @pl.when(h != j)
        def _():
            send(y_send.at[j], y_got.at[h], ys_s.at[j], ys_r.at[h], (f, j))

    ra_full[chip, core] = fsum[:, 0:RAW].astype(F32).reshape(z.nr, 8, RAW).astype(BF)
    for k in range(1, nf):
        fr = other_f(k)
        wait_recv(slab_got.at[fr], sl_r.at[fr])
    lsf = (slab_got[...].astype(F32).reshape(8 * nf, CA) + local).astype(BF)[:, 0:C]
    spread = mm_t0(lsf, pool_g) * 0.125
    grads_now = []
    for t in range(2):
        value = (wide(cot[t]).astype(F32) + spread).astype(BF)
        grads_now.append(value)
        for r in range(2):
            hg[t, r] = value[:, r * z.cols : (r + 1) * z.cols]

    @pl.when(f > 0)
    def _():
        send(hg.at[0], hg_r, hgs.at[0], hgr.at[0], (f - 1, h))

    @pl.when(f < nf - 1)
    def _():
        send(hg.at[1], hg_l, hgs.at[1], hgr.at[1], (f + 1, h))

    hg0, hg1 = grads_now
    left, right = wide(clip_l), wide(clip_r)
    taps = jnp.concatenate(
        [
            mm_t1(left, hg0) + mm_t1(first, hg1),
            mm_t1(first, hg0) + mm_t1(last, hg1),
            mm_t1(last, hg0) + mm_t1(right, hg1),
            jnp.zeros((64, C), F32),
        ],
        axis=0,
    )
    tp[...] = jnp.zeros_like(tp)
    tp[:, :, :, :, 0:C] = taps.reshape(2, nh, nc, z.tr, C).astype(BF)
    send(tp.at[1 - core], tp_pair, pair_s.at[1], pair_r.at[1], partner)

    for k in range(1, nc):
        to = other_c(k)
        send(ra_full.at[chip, core], ra_full.at[chip, core], ff_s.at[to], ff_r.at[chip], (to * 2 + core, h))
    send(ra_full.at[chip, core], ra_full.at[chip, core], fw_s.at[chip], fw_r.at[chip], partner)

    @pl.when(h < z.na)
    def _():
        xsum = xs_sum[chip].astype(F32)
        for k in range(1, nc):
            fr = other_c(k)
            wait_recv(xs_got.at[fr], fx_r.at[fr])
            xsum = xsum + xs_got[fr].astype(F32)
        x_mat = xsum.reshape(8 * z.ns, CA).astype(BF)

        @pl.when(h < z.na // 2)
        def _():
            x_buf[...] = mm(x_mat[:, 0:C], w_up[...]).reshape(z.ns, 8, CC)

        @pl.when(h >= z.na // 2)
        def _():
            x_buf[...] = mm(x_mat, w_aug[...]).reshape(z.ns, 8, CC)

        value = y_send[h].astype(F32) + x_buf[...]
        for k in range(1, nh):
            fr = other_h(k)
            wait_recv(y_got.at[fr], ys_r.at[fr])
            value = value + y_got[fr].astype(F32)
        y_full[chip, core, h] = value.astype(BF)
        for k in range(1, nh):
            to = other_h(k)
            send(y_full.at[chip, core, h], y_full.at[chip, core, h], yh_s.at[to], yh_r.at[h], (f, to))

    @pl.when(h >= z.na)
    def _():
        for k in range(1, nc):
            fr = other_c(k)
            wait_recv(xs_got.at[fr], fx_r.at[fr])

    wait_recv(tp_pair, pair_r.at[1])
    tp_sum[...] = (tp[core].astype(F32) + tp_pair[...].astype(F32)).astype(BF)
    for k in range(1, nh):
        to = other_h(k)
        send(tp_sum.at[to], tp_got.at[h], th_s.at[to], th_r.at[h], (f, to))

    lifted = mm_t0(lsf, pool_p)
    for t in range(2):
        value = (hidden[t].astype(F32) + lifted).astype(BF)
        for r in range(2):
            out[t, r] = value[:, r * z.cols : (r + 1) * z.cols]
    push(1, out, out_o)

    @pl.when(f > 0)
    def _():
        wait_recv(hg_l, hgr.at[1])

    @pl.when(f == 0)
    def _():
        hg_l[...] = jnp.zeros_like(hg_l)

    @pl.when(f < nf - 1)
    def _():
        wait_recv(hg_r, hgr.at[0])

    @pl.when(f == nf - 1)
    def _():
        hg_r[...] = jnp.zeros_like(hg_r)

    acc[0] = hg0.astype(F32) + mm(w_time[0], hg1) + mm(w_time[1], hg0) + mm(w_time[2], wide(hg_l))
    acc[1] = hg1.astype(F32) + mm(w_time[0], wide(hg_r)) + mm(w_time[1], hg1) + mm(w_time[2], hg0)
    for t in range(2):
        for r in range(2):
            grad_clip[t, r] = acc[t, :, r * z.cols : (r + 1) * z.cols]
    push(2, grad_clip, gc_o)

    zz, yy = chip // 2, lax.rem(chip, 2)
    across = ((zz * 2 + 1 - yy) * 2 + core, h)

    def y_half(i, c, k):
        return y_full.at[pl.ds(2 * c, 2), k, pl.ds(i * (z.na // 2), z.na // 2)]

    up_z, down_z = lax.rem(zz + 1, nz), lax.rem(zz + nz - 1, nz)

    def y_send_z(i, c, to, slot):
        part = y_half(i, c, core)
        send(part, part, yf_s.at[i, slot], yf_r.at[i, c], ((to * 2 + yy) * 2 + core, h))

    def y_pass(i, c):
        part = y_half(i, c, core)
        send(part, part, yw_s.at[i, c], yw_r.at[i, c], partner)

    def y_start():
        wait_recv(y_full.at[zz * 2 + 1 - yy, core], yx_r.at[0])
        if nz > 1:
            y_send_z(0, zz, up_z, 0)
            y_send_z(1, zz, down_z, 0)
            y_send_z(1, zz, up_z, 1)
            y_send_z(0, zz, down_z, 1)
        for i in range(2):
            y_pass(i, zz)

    for j in range(z.na):

        @pl.when(h != j)
        def _():
            wait_recv(y_full.at[chip, core, j], yh_r.at[j])

    send(y_full.at[chip, core], y_full.at[chip, core], yx_s.at[0], yx_r.at[0], across)

    value = tp_sum[h].astype(F32)
    for k in range(1, nh):
        fr = other_h(k)
        wait_recv(tp_got.at[fr], th_r.at[fr])
        value = value + tp_got[fr].astype(F32)
    tq_sum[...] = value.astype(BF)
    for k in range(1, nc):
        to = other_c(k)
        send(tq_sum.at[to], tq_got.at[chip], tf_s.at[to], tf_r.at[chip], (to * 2 + core, h))

    value = tq_sum[chip].astype(F32)
    for k in range(1, nc):
        fr = other_c(k)
        wait_recv(tq_got.at[fr], tf_r.at[fr])
        value = value + tq_got[fr].astype(F32)
    tap_full[core, h, chip] = value.astype(BF)
    for k in range(1, nc):
        to = other_c(k)
        here = tap_full.at[core, h, chip]
        send(here, here, tg_s.at[to], tg_r.at[chip], (to * 2 + core, h))
    y_start()
    for k in range(1, nc):
        fr = other_c(k)
        wait_recv(tap_full.at[core, h, fr], tg_r.at[fr])
    for k in range(1, nh):
        to = other_h(k)
        send(tap_full.at[core, h], tap_full.at[core, h], ta_s.at[to], ta_r.at[h], (f, to))
    send(tap_full.at[core, h], tap_full.at[core, h], tw_s.at[h], tw_r.at[h], partner)

    if nz > 1:
        far = lax.rem(zz + 2, nz)
        wait_recv(y_half(0, down_z, core), yf_r.at[0, down_z])
        y_send_z(0, down_z, up_z, 2)
        wait_recv(y_half(1, up_z, core), yf_r.at[1, up_z])
        y_send_z(1, up_z, down_z, 2)
        y_pass(0, down_z)
        y_pass(1, up_z)
        wait_recv(y_half(1, down_z, core), yf_r.at[1, down_z])
        y_pass(1, down_z)
        wait_recv(y_half(0, up_z, core), yf_r.at[0, up_z])
        y_pass(0, up_z)
        for i in range(2):
            wait_recv(y_half(i, far, core), yf_r.at[i, far])
            y_pass(i, far)
    for k in range(1, nc):
        fr = other_c(k)
        wait_recv(ra_full.at[fr, core], ff_r.at[fr])
        send(ra_full.at[fr, core], ra_full.at[fr, core], fw_s.at[fr], fw_r.at[fr], partner)

    for k in range(1, nh):
        fr = other_h(k)
        wait_recv(tap_full.at[core, fr], ta_r.at[fr])
        send(tap_full.at[core, fr], tap_full.at[core, fr], tw_s.at[fr], tw_r.at[fr], partner)
    for k in range(nc):
        wait_recv(ra_full.at[other_c(k), 1 - core], fw_r.at[other_c(k)])
    push(3, ra_full, ra_o)

    for i in range(2):
        for k in range(nz):
            fr = lax.rem(zz + k, nz)
            wait_recv(y_half(i, fr, 1 - core), yw_r.at[i, fr])
    push(4, y_full, y_o)
    for k in range(nh):
        wait_recv(tap_full.at[1 - core, other_h(k)], tw_r.at[other_h(k)])
    push(5, tap_full, tap_o)

    @pl.when(f > 0)
    def _():
        wait_send(clip.at[0], halo_s.at[0])
        wait_send(hg.at[0], hgs.at[0])

    @pl.when(f < nf - 1)
    def _():
        wait_send(clip.at[1], halo_s.at[1])
        wait_send(hg.at[1], hgs.at[1])

    for k in range(1, nf):
        to = other_f(k)
        wait_send(g_send.at[to], a2a_s.at[0, to])
        wait_send(p_send.at[to], a2a_s.at[1, to])
        wait_send(slab_send.at[to], sl_s.at[to])
    for k in range(1, nh):
        to = other_h(k)
        wait_send(g_all.at[h], ag_s.at[0, to])
        wait_send(p_all.at[h], ag_s.at[1, to])
        wait_send(ls_send.at[to], rs_s.at[to])
        wait_send(tp_sum.at[to], th_s.at[to])
        wait_send(tap_full.at[core, h], ta_s.at[to])
    for k in range(nh):
        wait_send(tap_full.at[core, other_h(k)], tw_s.at[other_h(k)])
    wait_send(fp_pair, pair_s.at[0])
    wait_send(tp_pair, pair_s.at[1])
    wait_send(xs_pair, pair_s.at[2])
    for k in range(1, nc):
        to = other_c(k)
        wait_send(fp_sum.at[to], fr_s.at[to])
        wait_send(xs_sum.at[to], fx_s.at[to])
        wait_send(ra_full.at[chip, core], ff_s.at[to])
        wait_send(tq_sum.at[to], tf_s.at[to])
        wait_send(tap_full.at[core, h, chip], tg_s.at[to])
    for k in range(nc):
        to = other_c(k)
        wait_send(ra_full.at[to, core], fw_s.at[to])
    wait_send(y_full.at[chip, core], yx_s.at[0])
    for i in range(2):
        for k in range(nz):
            to = lax.rem(zz + k, nz)
            wait_send(y_half(i, to, core), yw_s.at[i, to])
        for slot in range(3 if nz > 1 else 0):
            wait_send(y_half(i, zz, core), yf_s.at[i, slot])
    for j in range(z.na):

        @pl.when(h != j)
        def _():
            wait_send(y_send.at[j], ys_s.at[j])

    @pl.when(h < z.na)
    def _():
        for k in range(1, nh):
            wait_send(y_full.at[chip, core, h], yh_s.at[other_h(k)])

    pushes = [(w_aug, w_aug_o), (out, out_o), (grad_clip, gc_o), (ra_full, ra_o), (y_full, y_o), (tap_full, tap_o)]
    for i, (a, b) in enumerate(pushes):
        pltpu.make_async_copy(a, b, out_s.at[i]).wait()


def final_kernel(
    z, ra_in, y_in, tap_in, w_aug_in, w_up_in, embed_row, out_in, gc_in,
    out_o, gc_o, time_o, down_o, embed_o, qkv_o, wout_o, up_o,
    ra, y, tap, w_aug, w_up, out, gc, time, down, emb, qkv, wout, up, in_s, out_s,
):
    pulls = [(y_in, y), (tap_in, tap), (ra_in, ra), (w_aug_in, w_aug), (w_up_in, w_up), (out_in, out), (gc_in, gc)]
    pulls = [pltpu.make_async_copy(a, b, in_s.at[i]) for i, (a, b) in enumerate(pulls)]
    for pull in pulls:
        pull.start()
    pushes = []

    def push(src, dst):
        copy = pltpu.make_async_copy(src, dst, out_s.at[len(pushes)])
        copy.start()
        pushes.append(copy)

    pulls[0].wait()
    grad_down = y[:, 0].astype(F32).reshape(CA, CC)
    down[...] = grad_down[0:C]
    push(down, down_o)
    emb[...] = mm_t1(eye(C), jnp.broadcast_to(embed_row[...], (16, C)))[:, 0:1] * grad_down[C : C + 1]
    push(emb, embed_o)
    up[...] = y[:, 1].astype(F32).reshape(CA, CC)[0:C]
    push(up, up_o)
    pulls[1].wait()
    time[...] = tap[...].astype(F32).reshape(1024, CA)[0:960, 0:C]
    push(time, time_o)
    pulls[2].wait()
    pulls[3].wait()
    sums = flat(ra[...], RAW)
    qkv[...] = mm_t0(sums[:, 0:480], w_aug[...])
    push(qkv, qkv_o)
    pulls[4].wait()
    wout[...] = mm_t0(sums[0:C, 480:RAW], w_up[...])
    push(wout, wout_o)
    pulls[5].wait()
    push(out, out_o)
    pulls[6].wait()
    push(gc, gc_o)
    for copy in pushes:
        copy.wait()


def shards(z, clip, w_time, w_down, w_embed, w_qkv, w_out, w_up, timestep, cotangent):
    nf, nh, nc = z.nf, z.nh, z.nc
    embed = time_embed(timestep, w_embed.shape[0])
    embed_row = embed[None, :]
    vm = pl.BlockSpec(memory_space=pltpu.VMEM)
    hbm = pl.BlockSpec(memory_space=pl.ANY)
    dma = pltpu.SemaphoreType.DMA

    def bf(*shape):
        return pltpu.VMEM(shape, BF)

    def f32(*shape):
        return pltpu.VMEM(shape, F32)

    def like(kind, dtype):
        return jax.ShapeDtypeStruct(kind, dtype)

    frames = (2, 2, C, z.cols)
    ra_shape, y_shape = (nc, 2, z.nr, 8, RAW), (nc, 2, z.na, z.ns, 8, CC)
    tap_shape = (2, nh, nc, z.tr, CA)
    w_up_t = w_up.T
    outs = pl.pallas_call(
        functools.partial(main_kernel, z),
        out_shape=(
            like(frames, BF), like(frames, F32), like(ra_shape, BF), like(y_shape, BF),
            like(tap_shape, BF), like((CA, CC), BF),
        ),
        in_specs=[hbm] * 7 + [vm, hbm],
        out_specs=(hbm,) * 6,
        scratch_shapes=[
            bf(*frames), bf(3, C, C), bf(C, CC), bf(C, CC), bf(480, CC), bf(2 * HD, CC), bf(C, CC), bf(*frames),
            bf(*frames), f32(*frames), bf(*ra_shape), bf(*y_shape), bf(*tap_shape), bf(CA, CC),
            bf(*frames[1:]), bf(*frames[1:]), bf(2, C, z.cells), bf(*frames), bf(*frames[1:]), bf(*frames[1:]),
            f32(2, C, z.cells),
            bf(3, C, C), bf(768, CC), bf(CA, 768), bf(LW, 768), bf(256, CA), bf(256, LW), bf(CA, CA),
            bf(nf, 8, CA), bf(nf, 8, CA), bf(nf, 8, CA), bf(nf, 8, CA),
            bf(nh, z.tok, CA), bf(nh, z.tok, CA), bf(nh * z.tok, 768), bf(nh * z.tok, 256),
            bf(nh, z.tok, LW), bf(nh, z.tok, LW), bf(nf, 8, CA), bf(nf, 8, CA),
            bf(*ra_shape), bf(nc, z.nr, 8, RAW), bf(nc, z.nr, 8, RAW), bf(nc, z.nr, 8, RAW),
            bf(*tap_shape), bf(nh, nc, z.tr, CA), bf(nh, nc, z.tr, CA), bf(nh, nc, z.tr, CA),
            bf(nc, z.tr, CA), bf(nc, z.tr, CA),
            bf(z.na, z.ns, 8, CC), bf(nh, z.ns, 8, CC), f32(z.ns, 8, CC),
            bf(nc, 2, z.nr, 8, CA), bf(nc, 2, z.ns, 8, CA), bf(nc, z.ns, 8, CA), bf(nc, z.ns, 8, CA), bf(nc, z.ns, 8, CA),
            dma((8,)), dma((6,)), dma((nc,)), dma((nc,)), dma((1,)), dma((1,)),
            dma((2,)), dma((2,)), dma((2,)), dma((2,)),
            dma((2, nf)), dma((2, nf)), dma((2, nh)), dma((2, nh)),
            dma((nh,)), dma((nh,)), dma((nf,)), dma((nf,)),
            dma((3,)), dma((3,)), dma((nc,)), dma((nc,)), dma((nc,)), dma((nc,)), dma((nc,)), dma((nc,)),
            dma((nh,)), dma((nh,)), dma((nc,)), dma((nc,)), dma((nc,)), dma((nc,)),
            dma((nh,)), dma((nh,)), dma((nh,)), dma((nh,)),
            dma((nh,)), dma((nh,)), dma((nh,)), dma((nh,)), dma((2, nc)), dma((2, nc)), dma((2, nc)), dma((2, nc)),
        ],
        compiler_params=pltpu.CompilerParams(
            collective_id=0, has_side_effects=True, vmem_limit_bytes=60 * 1024 * 1024
        ),
    )(
        jnp.swapaxes(clip, 2, 3), w_time, w_down, w_embed, w_qkv.T, w_out, w_up_t, embed_row,
        jnp.swapaxes(cotangent, 2, 3),
    )
    out, grad_clip, ra_full, y_full, tap_full, w_aug = outs
    grads = pl.pallas_call(
        functools.partial(final_kernel, z),
        out_shape=(
            like(frames, BF), like(frames, F32), like((960, C), F32), like((C, CC), F32), like((C, CC), F32),
            like((480, CC), F32), like((2 * HD, CC), F32), like((C, CC), F32),
        ),
        in_specs=[hbm] * 5 + [vm, hbm, hbm],
        out_specs=(hbm,) * 8,
        scratch_shapes=[
            bf(*ra_shape), bf(nf, 2, z.nr, 8, CC), bf(*tap_shape), bf(CA, CC), bf(C, CC), bf(*frames), f32(*frames),
            f32(960, C), f32(C, CC), f32(C, CC), f32(480, CC), f32(2 * HD, CC), f32(C, CC),
            dma((7,)), dma((8,)),
        ],
        compiler_params=pltpu.CompilerParams(vmem_limit_bytes=60 * 1024 * 1024),
    )(
        ra_full, y_full.reshape(nf, 2, z.nr, 8, CC), tap_full, w_aug, w_up_t, embed_row,
        out, grad_clip,
    )
    out, grad_clip, grad_time, grad_down, grad_embed, grad_qkv, grad_out, grad_up = grads
    return (
        jnp.swapaxes(out, 2, 3),
        jnp.swapaxes(grad_clip, 2, 3),
        grad_time.reshape(3, C, C),
        grad_down,
        grad_embed,
        grad_qkv.T,
        grad_out,
        grad_up.T,
    )


def solution(mesh, cols=128):
    z = Sizes(mesh.shape["frames"], mesh.shape["heads"], cols)
    return jax.shard_map(
        functools.partial(shards, z),
        mesh=mesh,
        in_specs=(
            P("frames", "heads", None, None),
            P(),
            P(),
            P(),
            P(None, "heads"),
            P("heads", None),
            P(),
            P(),
            P("frames", "heads", None, None),
        ),
        out_specs=(
            P("frames", "heads", None, None),
            P("frames", "heads", None, None),
            P(),
            P(),
            P(),
            P(None, "heads"),
            P("heads", None),
            P(),
        ),
        check_vma=False,
    )
```

```python
import functools
import math

import jax
import jax.numpy as jnp
from jax import lax
from jax.experimental import pallas as pl
from jax.experimental.pallas import tpu as pltpu
from jax.sharding import PartitionSpec as P

HD = 80
MESH = pl.DeviceIdType.MESH
BF = jnp.bfloat16
F32 = jnp.float32
SCALE = 1.0 / math.sqrt(HD)
C = 320
CA = 384
CC = 1280
LW = 2 * C
RAW = 8 * HD


def mm(a, b):
    return jnp.dot(a, b, preferred_element_type=F32)


def mm_t0(a, b):
    return lax.dot_general(a, b, (((0,), (0,)), ((), ())), preferred_element_type=F32)


def mm_t1(a, b):
    return lax.dot_general(a, b, (((1,), (1,)), ((), ())), preferred_element_type=F32)


def iota(shape, dim):
    return lax.broadcasted_iota(jnp.int32, shape, dim)


def ones_where(cond):
    return jnp.where(cond, 1.0, 0.0).astype(BF)


def eye(n):
    return ones_where(iota((n, n), 0) == iota((n, n), 1))


def time_embed(timestep, width):
    half = width // 2
    freqs = jnp.exp(-math.log(10000.0) * jnp.arange(half, dtype=jnp.float32) / half)
    angle = timestep.astype(jnp.float32)[0] * freqs
    return jax.nn.silu(jnp.concatenate([jnp.cos(angle), jnp.sin(angle)])).astype(jnp.bfloat16)


class Sizes:
    def __init__(self, nf, nh, cols):
        self.nf, self.nh, self.cols = nf, nh, cols
        self.nc, self.nx = nf // 2, nh // 2
        self.cells = 2 * cols
        self.tok = 4 * nf
        self.nr = CA // nf // 8
        self.na = 6 if nh == 8 else nh
        self.ns = 2 * self.nr // self.na
        self.tr = 1024 // (2 * nh * self.nc)


def wide(frame):
    return jnp.concatenate([frame[0], frame[1]], axis=1)


def flat(slabs, width):
    value = slabs.astype(F32)
    return value.reshape(value.size // width, width).astype(BF)


def main_kernel(
    z, clip_in, w_time_in, w_down_in, w_embed_in, w_qkv_in, w_out_in, w_up_in, embed, cot_in,
    out, grad_clip, ra_full, y_full, tap_full, w_aug,
    clip, w_time, w_down, w_embed, w_qkv, w_out, w_up, cot,
    clip_l, clip_r, hidden, hg, hg_l, hg_r, acc,
    w_t, w_qkvp, w2, w2s, mh, mhl, wdu,
    p_send, g_send, p_got, g_got, p_all, g_all, dg_all, att_all,
    ls_send, ls_got, slab_send, slab_got,
    fp, fp_pair, fp_sum, fp_got, tp, tp_pair, tp_sum, tp_got, tq_sum, tq_got,
    y_send, y_got, x_buf, x_all, xs, xs_pair, xs_sum, xs_got,
    in_s, fx_s, fx_r, yx_s, yx_r,
    halo_s, halo_r, hgs, hgr, a2a_s, a2a_r, ag_s, ag_r, rs_s, rs_r, sl_s, sl_r,
    pair_s, pair_r, fr_s, fr_r, ff_s, ff_r, fw_s, fw_r,
    th_s, th_r, tf_s, tf_r, tg_s, tg_r, ta_s, ta_r, tw_s, tw_r,
    ys_s, ys_r, yh_s, yh_r, yf_s, yf_r, yw_s, yw_r,
):
    nf, nh, nc, nx, nz = z.nf, z.nh, z.nc, z.nx, z.nc // 2
    f, h = lax.axis_index("frames"), lax.axis_index("heads")
    chip, core = f // 2, lax.rem(f, 2)
    partner = (chip * 2 + 1 - core, h)

    def send(src, dst, ssem, rsem, to):
        pltpu.make_async_remote_copy(
            src_ref=src, dst_ref=dst, send_sem=ssem, recv_sem=rsem, device_id=to, device_id_type=MESH
        ).start()

    def wait_send(src, sem):
        pltpu.make_async_remote_copy(
            src_ref=src, dst_ref=src, send_sem=sem, recv_sem=sem, device_id=(f, h), device_id_type=MESH
        ).wait_send()

    def wait_recv(dst, sem):
        pltpu.make_async_remote_copy(
            src_ref=dst, dst_ref=dst, send_sem=sem, recv_sem=sem, device_id=(f, h), device_id_type=MESH
        ).wait_recv()

    def other_f(k):
        return lax.rem(f + k, nf)

    def other_h(k):
        return lax.rem(h + k, nh)

    def heads_out():
        for off in ([2, nx - 1, 1, 0] if nx == 4 else range(nx)):
            base = 2 * lax.rem(h // 2 + off, nx)
            if off == 0:
                yield base + 1 - lax.rem(h, 2)
            else:
                yield base + lax.rem(h, 2)
                yield base + 1 - lax.rem(h, 2)

    def other_c(k):
        return lax.rem(chip + k, nc)

    pulls = [
        (cot_in, cot), (clip_in, clip), (w_time_in, w_time), (w_embed_in, w_embed),
        (w_down_in, w_down), (w_qkv_in, w_qkv), (w_up_in, w_up), (w_out_in, w_out),
    ]
    pulls = [pltpu.make_async_copy(a, b, in_s.at[i]) for i, (a, b) in enumerate(pulls)]
    for pull in pulls:
        pull.start()

    barrier = pltpu.get_barrier_semaphore()
    for k in range(1, nf):
        pl.semaphore_signal(barrier, inc=1, device_id=(other_f(k), h), device_id_type=MESH)
    for k in range(1, nh):
        pl.semaphore_signal(barrier, inc=1, device_id=(f, other_h(k)), device_id_type=MESH)

    srow, scell = iota((8 * nf, z.cells), 0), iota((8 * nf, z.cells), 1)
    spos, sp = (srow // 8) * 4, lax.rem(srow, 8)
    column = lax.rem(scell, z.cols) // 2
    pool_p = ones_where((sp < 4) & (spos + sp == column))
    pool_g = ones_where((sp >= 4) & (spos + sp - 4 == column))
    pulls[0].wait()
    g_slab = mm_t1(pool_g, wide(cot[0])) + mm_t1(pool_g, wide(cot[1]))
    g_send[...] = jnp.zeros_like(g_send)
    g_send[:, :, 0:C] = g_slab.reshape(nf, 8, C).astype(BF)
    pulls[1].wait()

    pl.semaphore_wait(barrier, nf + nh - 2)

    @pl.when(f > 0)
    def _():
        send(clip.at[0], clip_r, halo_s.at[0], halo_r.at[0], (f - 1, h))

    @pl.when(f < nf - 1)
    def _():
        send(clip.at[1], clip_l, halo_s.at[1], halo_r.at[1], (f + 1, h))

    for k in range(1, nf):
        to = other_f(k)
        send(g_send.at[to], g_got.at[f], a2a_s.at[0, to], a2a_r.at[0, f], (to, h))
    g_got[f] = g_send[f]

    pulls[2].wait()
    unit = eye(C)
    for k in range(3):
        w_t[k] = mm_t0(w_time[k], unit).astype(BF)
    first, last = wide(clip[0]), wide(clip[1])
    acc[0] = mm(w_t[1], first) + mm(w_t[2], last)
    acc[1] = mm(w_t[0], first) + mm(w_t[1], last)

    for pull in pulls[3:]:
        pull.wait()
    shift = mm(jnp.broadcast_to(embed[...], (16, C)), w_embed[...])
    w_aug[0:C] = w_down[...]
    w_aug[C:CA] = jnp.where(iota((CA - C, CC), 0) == 0, jnp.broadcast_to(shift[0:1], (CA - C, CC)), 0.0).astype(BF)
    w_qkvp[...] = jnp.zeros_like(w_qkvp)
    for i in range(6):
        w_qkvp[128 * i : 128 * i + HD] = w_qkv[HD * i : HD * i + HD]
    w2_value = mm_t1(w_aug[...], w_qkvp[...]).astype(BF)
    w2[...] = w2_value
    w2s[0:C] = jnp.zeros((C, 768), BF)
    w2s[C:LW] = w2_value[0:C]
    mix = mm_t1(w_out[...], w_up[...]).astype(BF)
    for ref in (mh, mhl):
        ref[...] = jnp.zeros_like(ref)
        ref[0:HD, 0:C] = mix[0:HD]
        ref[128 : 128 + HD, 0:C] = mix[HD : 2 * HD]
    wdu[...] = jnp.zeros_like(wdu)
    wdu[:, 0:C] = mm_t1(w_aug[...], w_up[...]).astype(BF)

    sel_rows, sel_cols = iota((z.tok, 8 * nf), 0), iota((z.tok, 8 * nf), 1)
    want = (sel_rows // 4) * 8 + lax.rem(sel_rows, 4)
    sel_p = ones_where(sel_cols == want)
    sel_g = ones_where(sel_cols == want + 4)

    @pl.when(f > 0)
    def _():
        wait_recv(clip_l, halo_r.at[1])

    @pl.when(f == 0)
    def _():
        clip_l[...] = jnp.zeros_like(clip_l)

    @pl.when(f < nf - 1)
    def _():
        wait_recv(clip_r, halo_r.at[0])

    @pl.when(f == nf - 1)
    def _():
        clip_r[...] = jnp.zeros_like(clip_r)

    hidden[0] = (first.astype(F32) + acc[0] + mm(w_t[0], wide(clip_l))).astype(BF)
    hidden[1] = (last.astype(F32) + acc[1] + mm(w_t[2], wide(clip_r))).astype(BF)
    p_slab = (mm_t1(pool_p, hidden[0]) + mm_t1(pool_p, hidden[1])) * 0.125
    lane, prow = iota((nf, 8, CA), 2), iota((nf, 8, CA), 1)
    p_send[...] = ones_where((lane == C) & (prow < 4))
    p_send[:, :, 0:C] = p_slab.reshape(nf, 8, C).astype(BF)
    for k in range(1, nf):
        to = other_f(k)
        send(p_send.at[to], p_got.at[f], a2a_s.at[1, to], a2a_r.at[1, f], (to, h))
    p_got[f] = p_send[f]

    for k in range(1, nf):
        fr = other_f(k)
        wait_recv(g_got.at[fr], a2a_r.at[0, fr])
    g_all[h] = mm(sel_g, flat(g_got[...], CA)).astype(BF)
    for to in heads_out():
        send(g_all.at[h], g_all.at[h], ag_s.at[0, to], ag_r.at[0, h], (f, to))

    for k in range(1, nf):
        fr = other_f(k)
        wait_recv(p_got.at[fr], a2a_r.at[1, fr])
    p_all[h] = mm(sel_p, flat(p_got[...], CA)).astype(BF)
    for to in heads_out():
        send(p_all.at[h], p_all.at[h], ag_s.at[1, to], ag_r.at[1, h], (f, to))

    bt = 2 * z.tok
    arow, acol = iota((bt, bt), 0), iota((bt, bt), 1)
    mask = (arow // z.tok == acol // z.tok) & (lax.rem(arow, 4) == lax.rem(acol, 4))

    def rows_needed(off):
        mine = 2 * (h // 2) + 1 - lax.rem(h, 2)
        base = 2 * lax.rem(h // 2 + off, nx)
        return [mine] if off == 0 else [base, base + 1]

    def blocks(group):
        where = [lax.rem(h // 2 + off, nx) for off in group]
        twos = [pl.ds(2 * b, 2) for b in where]
        pb = jnp.concatenate([p_all[two].reshape(bt, CA) for two in twos], axis=0)
        gb = jnp.concatenate([g_all[two].reshape(bt, CA) for two in twos], axis=0)
        qkv = mm(pb, w2[...]).astype(BF)
        ag = mm_t1(gb, mh[...]).astype(BF)
        dgs, atts = [], []
        for i, b in enumerate(where):
            grads, att = [], []
            for n in range(2):
                own = slice(i * bt, (i + 1) * bt)
                q, k, v = (qkv[own, (3 * n + m) * 128 : (3 * n + m + 1) * 128] for m in range(3))
                a = ag[own, n * 128 : (n + 1) * 128]
                scores = jnp.where(mask, mm_t1(q, k) * SCALE, -1e30)
                e = jnp.exp(scores - jnp.max(scores, axis=1, keepdims=True))
                probs = e / jnp.sum(e, axis=1, keepdims=True)
                weights = probs.astype(BF)
                att.append(mm(weights, v).astype(BF))
                wg = mm_t1(a, v)
                sg = (probs * (wg - jnp.sum(probs * wg, axis=1, keepdims=True)) * SCALE).astype(BF)
                grads += [mm(sg, k).astype(BF), mm_t0(sg, q).astype(BF), mm_t0(weights, a).astype(BF)]
            dgs.append(jnp.concatenate(grads, axis=1))
            atts.append(jnp.concatenate(att, axis=1))
            rows = pl.ds(pl.multiple_of(b * bt, bt), bt)
            dg_all[rows] = dgs[i]
            att_all[rows] = atts[i]
        dg, att = jnp.concatenate(dgs, axis=0), jnp.concatenate(atts, axis=0)
        ls = (mm(att, mhl[...]) + mm_t1(dg, w2s[...])).astype(BF)
        for i, two in enumerate(twos):
            ls_send[two] = ls[i * bt : (i + 1) * bt].reshape(2, z.tok, LW)

    for group in [[2, 1], [3, 0]] if nx == 4 else [list(range(nx))]:
        for off in group:
            for fr in rows_needed(off):
                wait_recv(g_all.at[fr], ag_r.at[0, fr])
                wait_recv(p_all.at[fr], ag_r.at[1, fr])
        blocks(group)
        for off in group:
            for to in rows_needed(off):
                send(ls_send.at[to], ls_got.at[h], rs_s.at[to], rs_r.at[h], (f, to))

    tokens = nh * z.tok
    p_mat, g_mat = p_all[...].reshape(tokens, CA), g_all[...].reshape(tokens, CA)
    r_pad = mm_t0(p_mat, dg_all[...]).astype(BF)
    a_pad = mm_t0(g_mat, att_all[...]).astype(BF)
    rrow, rcol = iota((768, RAW), 0), iota((768, RAW), 1)
    sel_r = ones_where((rrow // 128 == rcol // HD) & (lax.rem(rrow, 128) == lax.rem(rcol, HD)))
    arow2, acol2 = iota((256, RAW), 0), iota((256, RAW), 1)
    sel_a = ones_where((arow2 // 128 + 6 == acol2 // HD) & (lax.rem(arow2, 128) == lax.rem(acol2, HD)))
    ra = mm(r_pad, sel_r) + mm(a_pad, sel_a)
    slabs = (nc, 2, z.nr, 8)
    fp[...] = ra.reshape(*slabs, RAW).astype(BF)
    send(fp.at[:, 1 - core], fp_pair, pair_s.at[0], pair_r.at[0], partner)

    @pl.when(h < z.na // 2)
    def _():
        x_all[...] = mm_t0(p_mat, g_mat).reshape(*slabs, CA).astype(BF)

    @pl.when(h >= z.na // 2)
    def _():
        x_all[...] = mm_t0(g_mat, p_mat).reshape(*slabs, CA).astype(BF)

    mine = pl.ds(lax.rem(h, z.na // 2) * z.ns, z.ns)
    xs[...] = x_all[:, :, mine]
    send(xs.at[:, 1 - core], xs_pair, pair_s.at[2], pair_r.at[2], partner)

    local = mm(flat(p_send[...], CA), wdu[...]) + mm_t1(flat(g_send[...], CA), wdu[...])

    wait_recv(fp_pair, pair_r.at[0])
    fp_sum[...] = (fp[:, core].astype(F32) + fp_pair[...].astype(F32)).astype(BF)
    for k in range(1, nc):
        to = other_c(k)
        send(fp_sum.at[to], fp_got.at[chip], fr_s.at[to], fr_r.at[chip], (to * 2 + core, h))
    wait_recv(xs_pair, pair_r.at[2])
    xs_sum[...] = (xs[:, core].astype(F32) + xs_pair[...].astype(F32)).astype(BF)
    for k in range(1, nc):
        to = other_c(k)
        send(xs_sum.at[to], xs_got.at[chip], fx_s.at[to], fx_r.at[chip], (to * 2 + core, h))

    ls = ls_send[h].astype(F32)
    for k in range(1, nh):
        fr = other_h(k)
        wait_recv(ls_got.at[fr], rs_r.at[fr])
        ls = ls + ls_got[fr].astype(F32)
    erow, ecol = iota((8 * nf, z.tok), 0), iota((8 * nf, z.tok), 1)
    ep, et = lax.rem(erow, 8), (erow // 8) * 4
    put_l = ones_where((ep < 4) & (et + ep == ecol))
    put_s = ones_where((ep >= 4) & (et + ep - 4 == ecol))
    slab = mm(put_l, ls[:, 0:C].astype(BF)) + mm(put_s, ls[:, C:LW].astype(BF))
    slab_send[:, :, 0:C] = slab.reshape(nf, 8, C).astype(BF)
    slab_send[:, :, C:CA] = jnp.zeros((nf, 8, CA - C), BF)
    for k in range(1, nf):
        to = other_f(k)
        send(slab_send.at[to], slab_got.at[f], sl_s.at[to], sl_r.at[f], (to, h))
    slab_got[f] = slab_send[f]

    fsum = fp_sum[chip].astype(F32)
    for k in range(1, nc):
        fr = other_c(k)
        wait_recv(fp_got.at[fr], fr_r.at[fr])
        fsum = fsum + fp_got[fr].astype(F32)
    fsum = fsum.reshape(8 * z.nr, RAW).astype(BF)
    down = mm(fsum[:, 0:480], w_qkv[...])
    lift = mm(fsum[:, 480:RAW], w_out[...])
    part = jnp.concatenate([down, lift], axis=0)
    y_send[...] = part.reshape(z.na, z.ns, 8, CC).astype(BF)
    for j in range(z.na):

        @pl.when(h != j)
        def _():
            send(y_send.at[j], y_got.at[h], ys_s.at[j], ys_r.at[h], (f, j))

    ra_full[chip, core] = fsum[:, 0:RAW].astype(F32).reshape(z.nr, 8, RAW).astype(BF)
    for k in range(1, nf):
        fr = other_f(k)
        wait_recv(slab_got.at[fr], sl_r.at[fr])
    lsf = (slab_got[...].astype(F32).reshape(8 * nf, CA) + local).astype(BF)[:, 0:C]
    spread = mm_t0(lsf, pool_g) * 0.125
    grads_now = []
    for t in range(2):
        value = (wide(cot[t]).astype(F32) + spread).astype(BF)
        grads_now.append(value)
        for r in range(2):
            hg[t, r] = value[:, r * z.cols : (r + 1) * z.cols]

    @pl.when(f > 0)
    def _():
        send(hg.at[0], hg_r, hgs.at[0], hgr.at[0], (f - 1, h))

    @pl.when(f < nf - 1)
    def _():
        send(hg.at[1], hg_l, hgs.at[1], hgr.at[1], (f + 1, h))

    hg0, hg1 = grads_now
    left, right = wide(clip_l), wide(clip_r)
    taps = jnp.concatenate(
        [
            mm_t1(left, hg0) + mm_t1(first, hg1),
            mm_t1(first, hg0) + mm_t1(last, hg1),
            mm_t1(last, hg0) + mm_t1(right, hg1),
            jnp.zeros((64, C), F32),
        ],
        axis=0,
    )
    tp[...] = jnp.zeros_like(tp)
    tp[:, :, :, :, 0:C] = taps.reshape(2, nh, nc, z.tr, C).astype(BF)
    send(tp.at[1 - core], tp_pair, pair_s.at[1], pair_r.at[1], partner)

    for k in range(1, nc):
        to = other_c(k)
        send(ra_full.at[chip, core], ra_full.at[chip, core], ff_s.at[to], ff_r.at[chip], (to * 2 + core, h))
    send(ra_full.at[chip, core], ra_full.at[chip, core], fw_s.at[chip], fw_r.at[chip], partner)

    @pl.when(h < z.na)
    def _():
        xsum = xs_sum[chip].astype(F32)
        for k in range(1, nc):
            fr = other_c(k)
            wait_recv(xs_got.at[fr], fx_r.at[fr])
            xsum = xsum + xs_got[fr].astype(F32)
        x_mat = xsum.reshape(8 * z.ns, CA).astype(BF)

        @pl.when(h < z.na // 2)
        def _():
            x_buf[...] = mm(x_mat[:, 0:C], w_up[...]).reshape(z.ns, 8, CC)

        @pl.when(h >= z.na // 2)
        def _():
            x_buf[...] = mm(x_mat, w_aug[...]).reshape(z.ns, 8, CC)

        value = y_send[h].astype(F32) + x_buf[...]
        for k in range(1, nh):
            fr = other_h(k)
            wait_recv(y_got.at[fr], ys_r.at[fr])
            value = value + y_got[fr].astype(F32)
        y_full[chip, core, h] = value.astype(BF)
        for k in range(1, nh):
            to = other_h(k)
            send(y_full.at[chip, core, h], y_full.at[chip, core, h], yh_s.at[to], yh_r.at[h], (f, to))

    @pl.when(h >= z.na)
    def _():
        for k in range(1, nc):
            fr = other_c(k)
            wait_recv(xs_got.at[fr], fx_r.at[fr])

    wait_recv(tp_pair, pair_r.at[1])
    tp_sum[...] = (tp[core].astype(F32) + tp_pair[...].astype(F32)).astype(BF)
    for k in range(1, nh):
        to = other_h(k)
        send(tp_sum.at[to], tp_got.at[h], th_s.at[to], th_r.at[h], (f, to))

    lifted = mm_t0(lsf, pool_p)
    for t in range(2):
        value = (hidden[t].astype(F32) + lifted).astype(BF)
        for r in range(2):
            out[t, r] = value[:, r * z.cols : (r + 1) * z.cols]

    @pl.when(f > 0)
    def _():
        wait_recv(hg_l, hgr.at[1])

    @pl.when(f == 0)
    def _():
        hg_l[...] = jnp.zeros_like(hg_l)

    @pl.when(f < nf - 1)
    def _():
        wait_recv(hg_r, hgr.at[0])

    @pl.when(f == nf - 1)
    def _():
        hg_r[...] = jnp.zeros_like(hg_r)

    acc[0] = hg0.astype(F32) + mm(w_time[0], hg1) + mm(w_time[1], hg0) + mm(w_time[2], wide(hg_l))
    acc[1] = hg1.astype(F32) + mm(w_time[0], wide(hg_r)) + mm(w_time[1], hg1) + mm(w_time[2], hg0)
    for t in range(2):
        for r in range(2):
            grad_clip[t, r] = acc[t, :, r * z.cols : (r + 1) * z.cols]

    zz, yy = chip // 2, lax.rem(chip, 2)
    across = ((zz * 2 + 1 - yy) * 2 + core, h)

    def y_half(i, c, k):
        return y_full.at[pl.ds(2 * c, 2), k, pl.ds(i * (z.na // 2), z.na // 2)]

    up_z, down_z = lax.rem(zz + 1, nz), lax.rem(zz + nz - 1, nz)

    def y_send_z(i, c, to, slot):
        part = y_half(i, c, core)
        send(part, part, yf_s.at[i, slot], yf_r.at[i, c], ((to * 2 + yy) * 2 + core, h))

    def y_pass(i, c):
        part = y_half(i, c, core)
        send(part, part, yw_s.at[i, c], yw_r.at[i, c], partner)

    def y_start():
        wait_recv(y_full.at[zz * 2 + 1 - yy, core], yx_r.at[0])
        if nz > 1:
            y_send_z(0, zz, up_z, 0)
            y_send_z(1, zz, down_z, 0)
            y_send_z(1, zz, up_z, 1)
            y_send_z(0, zz, down_z, 1)
        for i in range(2):
            y_pass(i, zz)

    for j in range(z.na):

        @pl.when(h != j)
        def _():
            wait_recv(y_full.at[chip, core, j], yh_r.at[j])

    send(y_full.at[chip, core], y_full.at[chip, core], yx_s.at[0], yx_r.at[0], across)

    value = tp_sum[h].astype(F32)
    for k in range(1, nh):
        fr = other_h(k)
        wait_recv(tp_got.at[fr], th_r.at[fr])
        value = value + tp_got[fr].astype(F32)
    tq_sum[...] = value.astype(BF)
    for k in range(1, nc):
        to = other_c(k)
        send(tq_sum.at[to], tq_got.at[chip], tf_s.at[to], tf_r.at[chip], (to * 2 + core, h))

    value = tq_sum[chip].astype(F32)
    for k in range(1, nc):
        fr = other_c(k)
        wait_recv(tq_got.at[fr], tf_r.at[fr])
        value = value + tq_got[fr].astype(F32)
    tap_full[core, h, chip] = value.astype(BF)
    for k in range(1, nc):
        to = other_c(k)
        here = tap_full.at[core, h, chip]
        send(here, here, tg_s.at[to], tg_r.at[chip], (to * 2 + core, h))
    y_start()
    for k in range(1, nc):
        fr = other_c(k)
        wait_recv(tap_full.at[core, h, fr], tg_r.at[fr])
    for k in range(1, nh):
        to = other_h(k)
        send(tap_full.at[core, h], tap_full.at[core, h], ta_s.at[to], ta_r.at[h], (f, to))
    send(tap_full.at[core, h], tap_full.at[core, h], tw_s.at[h], tw_r.at[h], partner)

    if nz > 1:
        far = lax.rem(zz + 2, nz)
        wait_recv(y_half(0, down_z, core), yf_r.at[0, down_z])
        y_send_z(0, down_z, up_z, 2)
        wait_recv(y_half(1, up_z, core), yf_r.at[1, up_z])
        y_send_z(1, up_z, down_z, 2)
        y_pass(0, down_z)
        y_pass(1, up_z)
        wait_recv(y_half(1, down_z, core), yf_r.at[1, down_z])
        y_pass(1, down_z)
        wait_recv(y_half(0, up_z, core), yf_r.at[0, up_z])
        y_pass(0, up_z)
        for i in range(2):
            wait_recv(y_half(i, far, core), yf_r.at[i, far])
            y_pass(i, far)
    for k in range(1, nc):
        fr = other_c(k)
        wait_recv(ra_full.at[fr, core], ff_r.at[fr])
        send(ra_full.at[fr, core], ra_full.at[fr, core], fw_s.at[fr], fw_r.at[fr], partner)

    for k in range(1, nh):
        fr = other_h(k)
        wait_recv(tap_full.at[core, fr], ta_r.at[fr])
        send(tap_full.at[core, fr], tap_full.at[core, fr], tw_s.at[fr], tw_r.at[fr], partner)
    for k in range(nc):
        wait_recv(ra_full.at[other_c(k), 1 - core], fw_r.at[other_c(k)])

    for i in range(2):
        for k in range(nz):
            fr = lax.rem(zz + k, nz)
            wait_recv(y_half(i, fr, 1 - core), yw_r.at[i, fr])
    for k in range(nh):
        wait_recv(tap_full.at[1 - core, other_h(k)], tw_r.at[other_h(k)])

    @pl.when(f > 0)
    def _():
        wait_send(clip.at[0], halo_s.at[0])
        wait_send(hg.at[0], hgs.at[0])

    @pl.when(f < nf - 1)
    def _():
        wait_send(clip.at[1], halo_s.at[1])
        wait_send(hg.at[1], hgs.at[1])

    for k in range(1, nf):
        to = other_f(k)
        wait_send(g_send.at[to], a2a_s.at[0, to])
        wait_send(p_send.at[to], a2a_s.at[1, to])
        wait_send(slab_send.at[to], sl_s.at[to])
    for k in range(1, nh):
        to = other_h(k)
        wait_send(g_all.at[h], ag_s.at[0, to])
        wait_send(p_all.at[h], ag_s.at[1, to])
        wait_send(ls_send.at[to], rs_s.at[to])
        wait_send(tp_sum.at[to], th_s.at[to])
        wait_send(tap_full.at[core, h], ta_s.at[to])
    for k in range(nh):
        wait_send(tap_full.at[core, other_h(k)], tw_s.at[other_h(k)])
    wait_send(fp_pair, pair_s.at[0])
    wait_send(tp_pair, pair_s.at[1])
    wait_send(xs_pair, pair_s.at[2])
    for k in range(1, nc):
        to = other_c(k)
        wait_send(fp_sum.at[to], fr_s.at[to])
        wait_send(xs_sum.at[to], fx_s.at[to])
        wait_send(ra_full.at[chip, core], ff_s.at[to])
        wait_send(tq_sum.at[to], tf_s.at[to])
        wait_send(tap_full.at[core, h, chip], tg_s.at[to])
    for k in range(nc):
        to = other_c(k)
        wait_send(ra_full.at[to, core], fw_s.at[to])
    wait_send(y_full.at[chip, core], yx_s.at[0])
    for i in range(2):
        for k in range(nz):
            to = lax.rem(zz + k, nz)
            wait_send(y_half(i, to, core), yw_s.at[i, to])
        for slot in range(3 if nz > 1 else 0):
            wait_send(y_half(i, zz, core), yf_s.at[i, slot])
    for j in range(z.na):

        @pl.when(h != j)
        def _():
            wait_send(y_send.at[j], ys_s.at[j])

    @pl.when(h < z.na)
    def _():
        for k in range(1, nh):
            wait_send(y_full.at[chip, core, h], yh_s.at[other_h(k)])


def final_kernel(
    z, ra, y, tap, w_aug, w_up_in, embed_row, out, gc,
    out_o, gc_o, time_o, down_o, embed_o, qkv_o, wout_o, up_o,
    w_up, time, down, emb, qkv, wout, up, in_s, out_s,
):
    pull = pltpu.make_async_copy(w_up_in, w_up, in_s.at[0])
    pull.start()
    pushes = []

    def push(src, dst):
        copy = pltpu.make_async_copy(src, dst, out_s.at[len(pushes)])
        copy.start()
        pushes.append(copy)

    push(gc, gc_o)
    push(out, out_o)
    grad_down = y[:, 0].astype(F32).reshape(CA, CC)
    down[...] = grad_down[0:C]
    push(down, down_o)
    emb[...] = mm_t1(eye(C), jnp.broadcast_to(embed_row[...], (16, C)))[:, 0:1] * grad_down[C : C + 1]
    push(emb, embed_o)
    up[...] = y[:, 1].astype(F32).reshape(CA, CC)[0:C]
    push(up, up_o)
    time[...] = tap[...].astype(F32).reshape(1024, CA)[0:960, 0:C]
    push(time, time_o)
    sums = flat(ra[...], RAW)
    qkv[...] = mm_t0(sums[:, 0:480], w_aug[...])
    push(qkv, qkv_o)
    pull.wait()
    wout[...] = mm_t0(sums[0:C, 480:RAW], w_up[...])
    push(wout, wout_o)
    for copy in pushes:
        copy.wait()


def shards(z, clip, w_time, w_down, w_embed, w_qkv, w_out, w_up, timestep, cotangent):
    nf, nh, nc = z.nf, z.nh, z.nc
    embed = time_embed(timestep, w_embed.shape[0])
    embed_row = embed[None, :]
    vm = pl.BlockSpec(memory_space=pltpu.VMEM)
    hbm = pl.BlockSpec(memory_space=pltpu.HBM)
    dma = pltpu.SemaphoreType.DMA

    def bf(*shape):
        return pltpu.VMEM(shape, BF)

    def f32(*shape):
        return pltpu.VMEM(shape, F32)

    def far(x):
        return pltpu.with_memory_space_constraint(x, pltpu.HBM)

    def like(kind, dtype):
        return jax.ShapeDtypeStruct(kind, dtype)

    frames = (2, 2, C, z.cols)
    ra_shape, y_shape = (nc, 2, z.nr, 8, RAW), (nc, 2, z.na, z.ns, 8, CC)
    tap_shape = (2, nh, nc, z.tr, CA)
    w_up_t = w_up.T
    outs = pl.pallas_call(
        functools.partial(main_kernel, z),
        out_shape=(
            like(frames, BF), like(frames, F32), like(ra_shape, BF), like(y_shape, BF),
            like(tap_shape, BF), like((CA, CC), BF),
        ),
        in_specs=[hbm] * 7 + [vm, hbm],
        out_specs=(vm,) * 6,
        scratch_shapes=[
            bf(*frames), bf(3, C, C), bf(C, CC), bf(C, CC), bf(480, CC), bf(2 * HD, CC), bf(C, CC), bf(*frames),
            bf(*frames[1:]), bf(*frames[1:]), bf(2, C, z.cells), bf(*frames), bf(*frames[1:]), bf(*frames[1:]),
            f32(2, C, z.cells),
            bf(3, C, C), bf(768, CC), bf(CA, 768), bf(LW, 768), bf(256, CA), bf(256, LW), bf(CA, CA),
            bf(nf, 8, CA), bf(nf, 8, CA), bf(nf, 8, CA), bf(nf, 8, CA),
            bf(nh, z.tok, CA), bf(nh, z.tok, CA), bf(nh * z.tok, 768), bf(nh * z.tok, 256),
            bf(nh, z.tok, LW), bf(nh, z.tok, LW), bf(nf, 8, CA), bf(nf, 8, CA),
            bf(*ra_shape), bf(nc, z.nr, 8, RAW), bf(nc, z.nr, 8, RAW), bf(nc, z.nr, 8, RAW),
            bf(*tap_shape), bf(nh, nc, z.tr, CA), bf(nh, nc, z.tr, CA), bf(nh, nc, z.tr, CA),
            bf(nc, z.tr, CA), bf(nc, z.tr, CA),
            bf(z.na, z.ns, 8, CC), bf(nh, z.ns, 8, CC), f32(z.ns, 8, CC),
            bf(nc, 2, z.nr, 8, CA), bf(nc, 2, z.ns, 8, CA), bf(nc, z.ns, 8, CA), bf(nc, z.ns, 8, CA), bf(nc, z.ns, 8, CA),
            dma((8,)), dma((nc,)), dma((nc,)), dma((1,)), dma((1,)),
            dma((2,)), dma((2,)), dma((2,)), dma((2,)),
            dma((2, nf)), dma((2, nf)), dma((2, nh)), dma((2, nh)),
            dma((nh,)), dma((nh,)), dma((nf,)), dma((nf,)),
            dma((3,)), dma((3,)), dma((nc,)), dma((nc,)), dma((nc,)), dma((nc,)), dma((nc,)), dma((nc,)),
            dma((nh,)), dma((nh,)), dma((nc,)), dma((nc,)), dma((nc,)), dma((nc,)),
            dma((nh,)), dma((nh,)), dma((nh,)), dma((nh,)),
            dma((nh,)), dma((nh,)), dma((nh,)), dma((nh,)), dma((2, nc)), dma((2, nc)), dma((2, nc)), dma((2, nc)),
        ],
        compiler_params=pltpu.CompilerParams(
            collective_id=0, has_side_effects=True, vmem_limit_bytes=36 * 1024 * 1024
        ),
    )(
        far(jnp.swapaxes(clip, 2, 3)), far(w_time), far(w_down), far(w_embed), far(w_qkv.T), far(w_out),
        far(w_up_t), embed_row, far(jnp.swapaxes(cotangent, 2, 3)),
    )
    out, grad_clip, ra_full, y_full, tap_full, w_aug = outs
    grads = pl.pallas_call(
        functools.partial(final_kernel, z),
        out_shape=(
            like(frames, BF), like(frames, F32), like((960, C), F32), like((C, CC), F32), like((C, CC), F32),
            like((480, CC), F32), like((2 * HD, CC), F32), like((C, CC), F32),
        ),
        in_specs=[vm] * 4 + [hbm, vm, vm, vm],
        out_specs=(hbm,) * 8,
        scratch_shapes=[
            bf(C, CC),
            f32(960, C), f32(C, CC), f32(C, CC), f32(480, CC), f32(2 * HD, CC), f32(C, CC),
            dma((1,)), dma((8,)),
        ],
        compiler_params=pltpu.CompilerParams(vmem_limit_bytes=36 * 1024 * 1024),
    )(
        ra_full, y_full.reshape(nf, 2, z.nr, 8, CC), tap_full, w_aug, far(w_up_t), embed_row,
        out, grad_clip,
    )
    out, grad_clip, grad_time, grad_down, grad_embed, grad_qkv, grad_out, grad_up = grads
    return (
        jnp.swapaxes(out, 2, 3),
        jnp.swapaxes(grad_clip, 2, 3),
        grad_time.reshape(3, C, C),
        grad_down,
        grad_embed,
        grad_qkv.T,
        grad_out,
        grad_up.T,
    )


def solution(mesh, cols=128):
    z = Sizes(mesh.shape["frames"], mesh.shape["heads"], cols)
    return jax.shard_map(
        functools.partial(shards, z),
        mesh=mesh,
        in_specs=(
            P("frames", "heads", None, None),
            P(),
            P(),
            P(),
            P(None, "heads"),
            P("heads", None),
            P(),
            P(),
            P("frames", "heads", None, None),
        ),
        out_specs=(
            P("frames", "heads", None, None),
            P("frames", "heads", None, None),
            P(),
            P(),
            P(),
            P(None, "heads"),
            P("heads", None),
            P(),
        ),
        check_vma=False,
    )
```

```python
import functools
import math

import jax
import jax.numpy as jnp
from jax import lax
from jax.experimental import pallas as pl
from jax.experimental.pallas import tpu as pltpu
from jax.sharding import PartitionSpec as P

HD = 80
MESH = pl.DeviceIdType.MESH
BF = jnp.bfloat16
F32 = jnp.float32
SCALE = 1.0 / math.sqrt(HD)
C = 320
CA = 384
CC = 1280
LW = 2 * C
RAW = 8 * HD


def mm(a, b):
    return jnp.dot(a, b, preferred_element_type=F32)


def mm_t0(a, b):
    return lax.dot_general(a, b, (((0,), (0,)), ((), ())), preferred_element_type=F32)


def mm_t1(a, b):
    return lax.dot_general(a, b, (((1,), (1,)), ((), ())), preferred_element_type=F32)


def iota(shape, dim):
    return lax.broadcasted_iota(jnp.int32, shape, dim)


def ones_where(cond):
    return jnp.where(cond, 1.0, 0.0).astype(BF)


def eye(n):
    return ones_where(iota((n, n), 0) == iota((n, n), 1))


def time_embed(timestep, width):
    half = width // 2
    freqs = jnp.exp(-math.log(10000.0) * jnp.arange(half, dtype=jnp.float32) / half)
    angle = timestep.astype(jnp.float32)[0] * freqs
    return jax.nn.silu(jnp.concatenate([jnp.cos(angle), jnp.sin(angle)])).astype(jnp.bfloat16)


class Sizes:
    def __init__(self, nf, nh, cols):
        self.nf, self.nh, self.cols = nf, nh, cols
        self.nc, self.nx = nf // 2, nh // 2
        self.cells = 2 * cols
        self.tok = 4 * nf
        self.nr = CA // nf // 8
        self.na = 6 if nh == 8 else nh
        self.ns = 2 * self.nr // self.na
        self.tr = 1024 // (2 * nh * self.nc)


def wide(frame):
    return jnp.concatenate([frame[0], frame[1]], axis=1)


def flat(slabs, width):
    value = slabs.astype(F32)
    return value.reshape(value.size // width, width).astype(BF)


def main_kernel(
    z, clip_in, w_time_in, w_down_in, w_embed_in, w_qkv_in, w_out_in, w_up_in, embed, cot_in,
    out, grad_clip, ra_full, y_full, tap_full, w_aug,
    clip, w_time, w_down, w_embed, w_qkv, w_out, w_up, cot,
    clip_l, clip_r, hidden, hg, hg_l, hg_r, acc,
    w_t, w_qkvp, w2, w2s, mh, mhl, wdu,
    p_send, g_send, p_got, g_got, p_all, g_all, dg_all, att_all,
    ls_send, ls_got, slab_send, slab_got,
    fp, fp_pair, fp_sum, fp_got, tp, tp_pair, tp_sum, tp_got, tq_sum, tq_got,
    y_send, y_got, x_buf, x_all, xs, xs_pair, xs_sum, xs_got,
    in_s, fx_s, fx_r, yx_s, yx_r,
    halo_s, halo_r, hgs, hgr, a2a_s, a2a_r, ag_s, ag_r, rs_s, rs_r, sl_s, sl_r,
    pair_s, pair_r, fr_s, fr_r, ff_s, ff_r, fw_s, fw_r,
    th_s, th_r, tf_s, tf_r, tg_s, tg_r, ta_s, ta_r, tw_s, tw_r,
    ys_s, ys_r, yh_s, yh_r, yf_s, yf_r, yw_s, yw_r,
):
    nf, nh, nc, nx, nz = z.nf, z.nh, z.nc, z.nx, z.nc // 2
    f, h = lax.axis_index("frames"), lax.axis_index("heads")
    chip, core = f // 2, lax.rem(f, 2)
    partner = (chip * 2 + 1 - core, h)

    def send(src, dst, ssem, rsem, to):
        pltpu.make_async_remote_copy(
            src_ref=src, dst_ref=dst, send_sem=ssem, recv_sem=rsem, device_id=to, device_id_type=MESH
        ).start()

    def wait_send(src, sem):
        pltpu.make_async_remote_copy(
            src_ref=src, dst_ref=src, send_sem=sem, recv_sem=sem, device_id=(f, h), device_id_type=MESH
        ).wait_send()

    def wait_recv(dst, sem):
        pltpu.make_async_remote_copy(
            src_ref=dst, dst_ref=dst, send_sem=sem, recv_sem=sem, device_id=(f, h), device_id_type=MESH
        ).wait_recv()

    def other_f(k):
        return lax.rem(f + k, nf)

    def other_h(k):
        return lax.rem(h + k, nh)

    def heads_out():
        for off in ([2, nx - 1, 1, 0] if nx == 4 else range(nx)):
            base = 2 * lax.rem(h // 2 + off, nx)
            if off == 0:
                yield base + 1 - lax.rem(h, 2)
            else:
                yield base + lax.rem(h, 2)
                yield base + 1 - lax.rem(h, 2)

    def other_c(k):
        return lax.rem(chip + k, nc)

    pulls = [
        (cot_in, cot), (clip_in, clip), (w_time_in, w_time), (w_embed_in, w_embed),
        (w_down_in, w_down), (w_qkv_in, w_qkv), (w_up_in, w_up), (w_out_in, w_out),
    ]
    pulls = [pltpu.make_async_copy(a, b, in_s.at[i]) for i, (a, b) in enumerate(pulls)]
    for pull in pulls:
        pull.start()

    barrier = pltpu.get_barrier_semaphore()
    for k in range(1, nf):
        pl.semaphore_signal(barrier, inc=1, device_id=(other_f(k), h), device_id_type=MESH)
    for k in range(1, nh):
        pl.semaphore_signal(barrier, inc=1, device_id=(f, other_h(k)), device_id_type=MESH)

    srow, scell = iota((8 * nf, z.cells), 0), iota((8 * nf, z.cells), 1)
    spos, sp = (srow // 8) * 4, lax.rem(srow, 8)
    column = lax.rem(scell, z.cols) // 2
    pool_p = ones_where((sp < 4) & (spos + sp == column))
    pool_g = ones_where((sp >= 4) & (spos + sp - 4 == column))
    pulls[0].wait()
    g_slab = mm_t1(pool_g, wide(cot[0])) + mm_t1(pool_g, wide(cot[1]))
    g_send[...] = jnp.zeros_like(g_send)
    g_send[:, :, 0:C] = g_slab.reshape(nf, 8, C).astype(BF)
    pulls[1].wait()

    pl.semaphore_wait(barrier, nf + nh - 2)

    @pl.when(f > 0)
    def _():
        send(clip.at[0], clip_r, halo_s.at[0], halo_r.at[0], (f - 1, h))

    @pl.when(f < nf - 1)
    def _():
        send(clip.at[1], clip_l, halo_s.at[1], halo_r.at[1], (f + 1, h))

    for k in range(1, nf):
        to = other_f(k)
        send(g_send.at[to], g_got.at[f], a2a_s.at[0, to], a2a_r.at[0, f], (to, h))
    g_got[f] = g_send[f]

    pulls[2].wait()
    unit = eye(C)
    for k in range(3):
        w_t[k] = mm_t0(w_time[k], unit).astype(BF)
    first, last = wide(clip[0]), wide(clip[1])
    acc[0] = mm(w_t[1], first) + mm(w_t[2], last)
    acc[1] = mm(w_t[0], first) + mm(w_t[1], last)

    for pull in pulls[3:]:
        pull.wait()
    shift = mm(jnp.broadcast_to(embed[...], (16, C)), w_embed[...])
    w_aug[0:C] = w_down[...]
    w_aug[C:CA] = jnp.where(iota((CA - C, CC), 0) == 0, jnp.broadcast_to(shift[0:1], (CA - C, CC)), 0.0).astype(BF)
    w_qkvp[...] = jnp.zeros_like(w_qkvp)
    for i in range(6):
        w_qkvp[128 * i : 128 * i + HD] = w_qkv[HD * i : HD * i + HD]
    w2_value = mm_t1(w_aug[...], w_qkvp[...]).astype(BF)
    w2[...] = w2_value
    w2s[0:C] = jnp.zeros((C, 768), BF)
    w2s[C:LW] = w2_value[0:C]
    mix = mm_t1(w_out[...], w_up[...]).astype(BF)
    for ref in (mh, mhl):
        ref[...] = jnp.zeros_like(ref)
        ref[0:HD, 0:C] = mix[0:HD]
        ref[128 : 128 + HD, 0:C] = mix[HD : 2 * HD]
    wdu[...] = jnp.zeros_like(wdu)
    wdu[:, 0:C] = mm_t1(w_aug[...], w_up[...]).astype(BF)

    sel_rows, sel_cols = iota((z.tok, 8 * nf), 0), iota((z.tok, 8 * nf), 1)
    want = (sel_rows // 4) * 8 + lax.rem(sel_rows, 4)
    sel_p = ones_where(sel_cols == want)
    sel_g = ones_where(sel_cols == want + 4)

    @pl.when(f > 0)
    def _():
        wait_recv(clip_l, halo_r.at[1])

    @pl.when(f == 0)
    def _():
        clip_l[...] = jnp.zeros_like(clip_l)

    @pl.when(f < nf - 1)
    def _():
        wait_recv(clip_r, halo_r.at[0])

    @pl.when(f == nf - 1)
    def _():
        clip_r[...] = jnp.zeros_like(clip_r)

    hidden[0] = (first.astype(F32) + acc[0] + mm(w_t[0], wide(clip_l))).astype(BF)
    hidden[1] = (last.astype(F32) + acc[1] + mm(w_t[2], wide(clip_r))).astype(BF)
    p_slab = (mm_t1(pool_p, hidden[0]) + mm_t1(pool_p, hidden[1])) * 0.125
    lane, prow = iota((nf, 8, CA), 2), iota((nf, 8, CA), 1)
    p_send[...] = ones_where((lane == C) & (prow < 4))
    p_send[:, :, 0:C] = p_slab.reshape(nf, 8, C).astype(BF)
    for k in range(1, nf):
        to = other_f(k)
        send(p_send.at[to], p_got.at[f], a2a_s.at[1, to], a2a_r.at[1, f], (to, h))
    p_got[f] = p_send[f]

    for k in range(1, nf):
        fr = other_f(k)
        wait_recv(g_got.at[fr], a2a_r.at[0, fr])
    g_all[h] = mm(sel_g, flat(g_got[...], CA)).astype(BF)
    for to in heads_out():
        send(g_all.at[h], g_all.at[h], ag_s.at[0, to], ag_r.at[0, h], (f, to))

    tp[...] = jnp.zeros_like(tp)
    for k in range(1, nf):
        fr = other_f(k)
        wait_recv(p_got.at[fr], a2a_r.at[1, fr])
    p_all[h] = mm(sel_p, flat(p_got[...], CA)).astype(BF)
    for to in heads_out():
        send(p_all.at[h], p_all.at[h], ag_s.at[1, to], ag_r.at[1, h], (f, to))

    bt = 2 * z.tok
    arow, acol = iota((bt, bt), 0), iota((bt, bt), 1)
    mask = (arow // z.tok == acol // z.tok) & (lax.rem(arow, 4) == lax.rem(acol, 4))

    def rows_needed(off):
        mine = 2 * (h // 2) + 1 - lax.rem(h, 2)
        base = 2 * lax.rem(h // 2 + off, nx)
        return [mine] if off == 0 else [base, base + 1]

    def blocks(group):
        where = [lax.rem(h // 2 + off, nx) for off in group]
        twos = [pl.ds(2 * b, 2) for b in where]
        pb = jnp.concatenate([p_all[two].reshape(bt, CA) for two in twos], axis=0)
        gb = jnp.concatenate([g_all[two].reshape(bt, CA) for two in twos], axis=0)
        qkv = mm(pb, w2[...]).astype(BF)
        ag = mm_t1(gb, mh[...]).astype(BF)
        dgs, atts = [], []
        for i, b in enumerate(where):
            grads, att = [], []
            for n in range(2):
                own = slice(i * bt, (i + 1) * bt)
                q, k, v = (qkv[own, (3 * n + m) * 128 : (3 * n + m + 1) * 128] for m in range(3))
                a = ag[own, n * 128 : (n + 1) * 128]
                scores = jnp.where(mask, mm_t1(q, k) * SCALE, -1e30)
                e = jnp.exp(scores - jnp.max(scores, axis=1, keepdims=True))
                probs = e / jnp.sum(e, axis=1, keepdims=True)
                weights = probs.astype(BF)
                att.append(mm(weights, v).astype(BF))
                wg = mm_t1(a, v)
                sg = (probs * (wg - jnp.sum(probs * wg, axis=1, keepdims=True)) * SCALE).astype(BF)
                grads += [mm(sg, k).astype(BF), mm_t0(sg, q).astype(BF), mm_t0(weights, a).astype(BF)]
            dgs.append(jnp.concatenate(grads, axis=1))
            atts.append(jnp.concatenate(att, axis=1))
            rows = pl.ds(pl.multiple_of(b * bt, bt), bt)
            dg_all[rows] = dgs[i]
            att_all[rows] = atts[i]
        dg, att = jnp.concatenate(dgs, axis=0), jnp.concatenate(atts, axis=0)
        ls = (mm(att, mhl[...]) + mm_t1(dg, w2s[...])).astype(BF)
        for i, two in enumerate(twos):
            ls_send[two] = ls[i * bt : (i + 1) * bt].reshape(2, z.tok, LW)

    for group in [[2], [1], [3, 0]] if nx == 4 else [list(range(nx))]:
        for off in group:
            for fr in rows_needed(off):
                wait_recv(g_all.at[fr], ag_r.at[0, fr])
                wait_recv(p_all.at[fr], ag_r.at[1, fr])
        blocks(group)
        for off in group:
            for to in rows_needed(off):
                send(ls_send.at[to], ls_got.at[h], rs_s.at[to], rs_r.at[h], (f, to))

    tokens = nh * z.tok
    p_mat, g_mat = p_all[...].reshape(tokens, CA), g_all[...].reshape(tokens, CA)
    r_pad = mm_t0(p_mat, dg_all[...]).astype(BF)
    a_pad = mm_t0(g_mat, att_all[...]).astype(BF)
    rrow, rcol = iota((768, RAW), 0), iota((768, RAW), 1)
    sel_r = ones_where((rrow // 128 == rcol // HD) & (lax.rem(rrow, 128) == lax.rem(rcol, HD)))
    arow2, acol2 = iota((256, RAW), 0), iota((256, RAW), 1)
    sel_a = ones_where((arow2 // 128 + 6 == acol2 // HD) & (lax.rem(arow2, 128) == lax.rem(acol2, HD)))
    ra = mm(r_pad, sel_r) + mm(a_pad, sel_a)
    slabs = (nc, 2, z.nr, 8)
    fp[...] = ra.reshape(*slabs, RAW).astype(BF)
    send(fp.at[:, 1 - core], fp_pair, pair_s.at[0], pair_r.at[0], partner)

    @pl.when(h < z.na // 2)
    def _():
        x_all[...] = mm_t0(p_mat, g_mat).reshape(*slabs, CA).astype(BF)

    @pl.when(h >= z.na // 2)
    def _():
        x_all[...] = mm_t0(g_mat, p_mat).reshape(*slabs, CA).astype(BF)

    mine = pl.ds(lax.rem(h, z.na // 2) * z.ns, z.ns)
    xs[...] = x_all[:, :, mine]
    send(xs.at[:, 1 - core], xs_pair, pair_s.at[2], pair_r.at[2], partner)

    local = mm(flat(p_send[...], CA), wdu[...]) + mm_t1(flat(g_send[...], CA), wdu[...])

    wait_recv(fp_pair, pair_r.at[0])
    fp_sum[...] = (fp[:, core].astype(F32) + fp_pair[...].astype(F32)).astype(BF)
    for k in range(1, nc):
        to = other_c(k)
        send(fp_sum.at[to], fp_got.at[chip], fr_s.at[to], fr_r.at[chip], (to * 2 + core, h))
    wait_recv(xs_pair, pair_r.at[2])
    xs_sum[...] = (xs[:, core].astype(F32) + xs_pair[...].astype(F32)).astype(BF)
    for k in range(1, nc):
        to = other_c(k)
        send(xs_sum.at[to], xs_got.at[chip], fx_s.at[to], fx_r.at[chip], (to * 2 + core, h))

    ls = ls_send[h].astype(F32)
    for k in range(1, nh):
        fr = other_h(k)
        wait_recv(ls_got.at[fr], rs_r.at[fr])
        ls = ls + ls_got[fr].astype(F32)
    erow, ecol = iota((8 * nf, z.tok), 0), iota((8 * nf, z.tok), 1)
    ep, et = lax.rem(erow, 8), (erow // 8) * 4
    put_l = ones_where((ep < 4) & (et + ep == ecol))
    put_s = ones_where((ep >= 4) & (et + ep - 4 == ecol))
    slab = mm(put_l, ls[:, 0:C].astype(BF)) + mm(put_s, ls[:, C:LW].astype(BF))
    slab_send[:, :, 0:C] = slab.reshape(nf, 8, C).astype(BF)
    slab_send[:, :, C:CA] = jnp.zeros((nf, 8, CA - C), BF)
    for k in range(1, nf):
        to = other_f(k)
        send(slab_send.at[to], slab_got.at[f], sl_s.at[to], sl_r.at[f], (to, h))
    slab_got[f] = slab_send[f]

    fsum = fp_sum[chip].astype(F32)
    for k in range(1, nc):
        fr = other_c(k)
        wait_recv(fp_got.at[fr], fr_r.at[fr])
        fsum = fsum + fp_got[fr].astype(F32)
    fsum = fsum.reshape(8 * z.nr, RAW).astype(BF)
    down = mm(fsum[:, 0:480], w_qkv[...])
    lift = mm(fsum[:, 480:RAW], w_out[...])
    part = jnp.concatenate([down, lift], axis=0)
    y_send[...] = part.reshape(z.na, z.ns, 8, CC).astype(BF)
    for j in range(z.na):

        @pl.when(h != j)
        def _():
            send(y_send.at[j], y_got.at[h], ys_s.at[j], ys_r.at[h], (f, j))

    ra_full[chip, core] = fsum[:, 0:RAW].astype(F32).reshape(z.nr, 8, RAW).astype(BF)
    for k in range(1, nf):
        fr = other_f(k)
        wait_recv(slab_got.at[fr], sl_r.at[fr])
    lsf = (slab_got[...].astype(F32).reshape(8 * nf, CA) + local).astype(BF)[:, 0:C]
    spread = mm_t0(lsf, pool_g) * 0.125
    grads_now = []
    for t in range(2):
        value = (wide(cot[t]).astype(F32) + spread).astype(BF)
        grads_now.append(value)
        for r in range(2):
            hg[t, r] = value[:, r * z.cols : (r + 1) * z.cols]

    @pl.when(f > 0)
    def _():
        send(hg.at[0], hg_r, hgs.at[0], hgr.at[0], (f - 1, h))

    @pl.when(f < nf - 1)
    def _():
        send(hg.at[1], hg_l, hgs.at[1], hgr.at[1], (f + 1, h))

    hg0, hg1 = grads_now
    left, right = wide(clip_l), wide(clip_r)
    taps = jnp.concatenate(
        [
            mm_t1(left, hg0) + mm_t1(first, hg1),
            mm_t1(first, hg0) + mm_t1(last, hg1),
            mm_t1(last, hg0) + mm_t1(right, hg1),
            jnp.zeros((64, C), F32),
        ],
        axis=0,
    )
    tp[:, :, :, :, 0:C] = taps.reshape(2, nh, nc, z.tr, C).astype(BF)
    send(tp.at[1 - core], tp_pair, pair_s.at[1], pair_r.at[1], partner)

    for k in range(1, nc):
        to = other_c(k)
        send(ra_full.at[chip, core], ra_full.at[chip, core], ff_s.at[to], ff_r.at[chip], (to * 2 + core, h))
    send(ra_full.at[chip, core], ra_full.at[chip, core], fw_s.at[chip], fw_r.at[chip], partner)

    @pl.when(h < z.na)
    def _():
        xsum = xs_sum[chip].astype(F32)
        for k in range(1, nc):
            fr = other_c(k)
            wait_recv(xs_got.at[fr], fx_r.at[fr])
            xsum = xsum + xs_got[fr].astype(F32)
        x_mat = xsum.reshape(8 * z.ns, CA).astype(BF)

        @pl.when(h < z.na // 2)
        def _():
            x_buf[...] = mm(x_mat[:, 0:C], w_up[...]).reshape(z.ns, 8, CC)

        @pl.when(h >= z.na // 2)
        def _():
            x_buf[...] = mm(x_mat, w_aug[...]).reshape(z.ns, 8, CC)

        value = y_send[h].astype(F32) + x_buf[...]
        for k in range(1, nh):
            fr = other_h(k)
            wait_recv(y_got.at[fr], ys_r.at[fr])
            value = value + y_got[fr].astype(F32)
        y_full[chip, core, h] = value.astype(BF)
        for k in range(1, nh):
            to = other_h(k)
            send(y_full.at[chip, core, h], y_full.at[chip, core, h], yh_s.at[to], yh_r.at[h], (f, to))

    @pl.when(h >= z.na)
    def _():
        for k in range(1, nc):
            fr = other_c(k)
            wait_recv(xs_got.at[fr], fx_r.at[fr])

    wait_recv(tp_pair, pair_r.at[1])
    tp_sum[...] = (tp[core].astype(F32) + tp_pair[...].astype(F32)).astype(BF)
    for k in range(1, nh):
        to = other_h(k)
        send(tp_sum.at[to], tp_got.at[h], th_s.at[to], th_r.at[h], (f, to))

    lifted = mm_t0(lsf, pool_p)
    for t in range(2):
        value = (hidden[t].astype(F32) + lifted).astype(BF)
        for r in range(2):
            out[t, r] = value[:, r * z.cols : (r + 1) * z.cols]

    @pl.when(f > 0)
    def _():
        wait_recv(hg_l, hgr.at[1])

    @pl.when(f == 0)
    def _():
        hg_l[...] = jnp.zeros_like(hg_l)

    @pl.when(f < nf - 1)
    def _():
        wait_recv(hg_r, hgr.at[0])

    @pl.when(f == nf - 1)
    def _():
        hg_r[...] = jnp.zeros_like(hg_r)

    acc[0] = hg0.astype(F32) + mm(w_time[0], hg1) + mm(w_time[1], hg0) + mm(w_time[2], wide(hg_l))
    acc[1] = hg1.astype(F32) + mm(w_time[0], wide(hg_r)) + mm(w_time[1], hg1) + mm(w_time[2], hg0)
    for t in range(2):
        for r in range(2):
            grad_clip[t, r] = acc[t, :, r * z.cols : (r + 1) * z.cols]

    zz, yy = chip // 2, lax.rem(chip, 2)
    across = ((zz * 2 + 1 - yy) * 2 + core, h)

    def y_half(i, c, k):
        return y_full.at[pl.ds(2 * c, 2), k, pl.ds(i * (z.na // 2), z.na // 2)]

    up_z, down_z = lax.rem(zz + 1, nz), lax.rem(zz + nz - 1, nz)

    def y_send_z(i, c, to, slot):
        part = y_half(i, c, core)
        send(part, part, yf_s.at[i, slot], yf_r.at[i, c], ((to * 2 + yy) * 2 + core, h))

    def y_pass(i, c):
        part = y_half(i, c, core)
        send(part, part, yw_s.at[i, c], yw_r.at[i, c], partner)

    def y_start():
        wait_recv(y_full.at[zz * 2 + 1 - yy, core], yx_r.at[0])
        if nz > 1:
            y_send_z(0, zz, up_z, 0)
            y_send_z(1, zz, down_z, 0)
            y_send_z(1, zz, up_z, 1)
            y_send_z(0, zz, down_z, 1)
        for i in range(2):
            y_pass(i, zz)

    for j in range(z.na):

        @pl.when(h != j)
        def _():
            wait_recv(y_full.at[chip, core, j], yh_r.at[j])

    send(y_full.at[chip, core], y_full.at[chip, core], yx_s.at[0], yx_r.at[0], across)

    value = tp_sum[h].astype(F32)
    for k in range(1, nh):
        fr = other_h(k)
        wait_recv(tp_got.at[fr], th_r.at[fr])
        value = value + tp_got[fr].astype(F32)
    tq_sum[...] = value.astype(BF)
    for k in range(1, nc):
        to = other_c(k)
        send(tq_sum.at[to], tq_got.at[chip], tf_s.at[to], tf_r.at[chip], (to * 2 + core, h))

    value = tq_sum[chip].astype(F32)
    for k in range(1, nc):
        fr = other_c(k)
        wait_recv(tq_got.at[fr], tf_r.at[fr])
        value = value + tq_got[fr].astype(F32)
    tap_full[core, h, chip] = value.astype(BF)
    for k in range(1, nc):
        to = other_c(k)
        here = tap_full.at[core, h, chip]
        send(here, here, tg_s.at[to], tg_r.at[chip], (to * 2 + core, h))
    y_start()
    for k in range(1, nc):
        fr = other_c(k)
        wait_recv(tap_full.at[core, h, fr], tg_r.at[fr])
    for k in range(1, nh):
        to = other_h(k)
        send(tap_full.at[core, h], tap_full.at[core, h], ta_s.at[to], ta_r.at[h], (f, to))
    send(tap_full.at[core, h], tap_full.at[core, h], tw_s.at[h], tw_r.at[h], partner)

    if nz > 1:
        far = lax.rem(zz + 2, nz)
        wait_recv(y_half(0, down_z, core), yf_r.at[0, down_z])
        y_send_z(0, down_z, up_z, 2)
        wait_recv(y_half(1, up_z, core), yf_r.at[1, up_z])
        y_send_z(1, up_z, down_z, 2)
        y_pass(0, down_z)
        y_pass(1, up_z)
        wait_recv(y_half(1, down_z, core), yf_r.at[1, down_z])
        y_pass(1, down_z)
        wait_recv(y_half(0, up_z, core), yf_r.at[0, up_z])
        y_pass(0, up_z)
        for i in range(2):
            wait_recv(y_half(i, far, core), yf_r.at[i, far])
            y_pass(i, far)
    for k in range(1, nc):
        fr = other_c(k)
        wait_recv(ra_full.at[fr, core], ff_r.at[fr])
        send(ra_full.at[fr, core], ra_full.at[fr, core], fw_s.at[fr], fw_r.at[fr], partner)

    for k in range(1, nh):
        fr = other_h(k)
        wait_recv(tap_full.at[core, fr], ta_r.at[fr])
        send(tap_full.at[core, fr], tap_full.at[core, fr], tw_s.at[fr], tw_r.at[fr], partner)
    for k in range(nc):
        wait_recv(ra_full.at[other_c(k), 1 - core], fw_r.at[other_c(k)])

    for i in range(2):
        for k in range(nz):
            fr = lax.rem(zz + k, nz)
            wait_recv(y_half(i, fr, 1 - core), yw_r.at[i, fr])
    for k in range(nh):
        wait_recv(tap_full.at[1 - core, other_h(k)], tw_r.at[other_h(k)])

    @pl.when(f > 0)
    def _():
        wait_send(clip.at[0], halo_s.at[0])
        wait_send(hg.at[0], hgs.at[0])

    @pl.when(f < nf - 1)
    def _():
        wait_send(clip.at[1], halo_s.at[1])
        wait_send(hg.at[1], hgs.at[1])

    for k in range(1, nf):
        to = other_f(k)
        wait_send(g_send.at[to], a2a_s.at[0, to])
        wait_send(p_send.at[to], a2a_s.at[1, to])
        wait_send(slab_send.at[to], sl_s.at[to])
    for k in range(1, nh):
        to = other_h(k)
        wait_send(g_all.at[h], ag_s.at[0, to])
        wait_send(p_all.at[h], ag_s.at[1, to])
        wait_send(ls_send.at[to], rs_s.at[to])
        wait_send(tp_sum.at[to], th_s.at[to])
        wait_send(tap_full.at[core, h], ta_s.at[to])
    for k in range(nh):
        wait_send(tap_full.at[core, other_h(k)], tw_s.at[other_h(k)])
    wait_send(fp_pair, pair_s.at[0])
    wait_send(tp_pair, pair_s.at[1])
    wait_send(xs_pair, pair_s.at[2])
    for k in range(1, nc):
        to = other_c(k)
        wait_send(fp_sum.at[to], fr_s.at[to])
        wait_send(xs_sum.at[to], fx_s.at[to])
        wait_send(ra_full.at[chip, core], ff_s.at[to])
        wait_send(tq_sum.at[to], tf_s.at[to])
        wait_send(tap_full.at[core, h, chip], tg_s.at[to])
    for k in range(nc):
        to = other_c(k)
        wait_send(ra_full.at[to, core], fw_s.at[to])
    wait_send(y_full.at[chip, core], yx_s.at[0])
    for i in range(2):
        for k in range(nz):
            to = lax.rem(zz + k, nz)
            wait_send(y_half(i, to, core), yw_s.at[i, to])
        for slot in range(3 if nz > 1 else 0):
            wait_send(y_half(i, zz, core), yf_s.at[i, slot])
    for j in range(z.na):

        @pl.when(h != j)
        def _():
            wait_send(y_send.at[j], ys_s.at[j])

    @pl.when(h < z.na)
    def _():
        for k in range(1, nh):
            wait_send(y_full.at[chip, core, h], yh_s.at[other_h(k)])


def final_kernel(
    z, ra, y, tap, w_aug, w_up_in, embed_row, out, gc,
    out_o, gc_o, time_o, down_o, embed_o, qkv_o, wout_o, up_o,
    w_up, time, down, emb, qkv, wout, up, in_s, out_s,
):
    pull = pltpu.make_async_copy(w_up_in, w_up, in_s.at[0])
    pull.start()
    pushes = []

    def push(src, dst):
        copy = pltpu.make_async_copy(src, dst, out_s.at[len(pushes)])
        copy.start()
        pushes.append(copy)

    push(gc, gc_o)
    push(out, out_o)
    grad_down = y[:, 0].astype(F32).reshape(CA, CC)
    down[...] = grad_down[0:C]
    push(down, down_o)
    emb[...] = mm_t1(eye(C), jnp.broadcast_to(embed_row[...], (16, C)))[:, 0:1] * grad_down[C : C + 1]
    push(emb, embed_o)
    up[...] = y[:, 1].astype(F32).reshape(CA, CC)[0:C]
    push(up, up_o)
    time[...] = tap[...].astype(F32).reshape(1024, CA)[0:960, 0:C]
    push(time, time_o)
    sums = flat(ra[...], RAW)
    qkv[...] = mm_t0(sums[:, 0:480], w_aug[...])
    push(qkv, qkv_o)
    pull.wait()
    wout[...] = mm_t0(sums[0:C, 480:RAW], w_up[...])
    push(wout, wout_o)
    for copy in pushes:
        copy.wait()


def shards(z, clip, w_time, w_down, w_embed, w_qkv, w_out, w_up, timestep, cotangent):
    nf, nh, nc = z.nf, z.nh, z.nc
    embed = time_embed(timestep, w_embed.shape[0])
    embed_row = embed[None, :]
    vm = pl.BlockSpec(memory_space=pltpu.VMEM)
    hbm = pl.BlockSpec(memory_space=pltpu.HBM)
    dma = pltpu.SemaphoreType.DMA

    def bf(*shape):
        return pltpu.VMEM(shape, BF)

    def f32(*shape):
        return pltpu.VMEM(shape, F32)

    def far(x):
        return pltpu.with_memory_space_constraint(x, pltpu.HBM)

    def like(kind, dtype):
        return jax.ShapeDtypeStruct(kind, dtype)

    frames = (2, 2, C, z.cols)
    ra_shape, y_shape = (nc, 2, z.nr, 8, RAW), (nc, 2, z.na, z.ns, 8, CC)
    tap_shape = (2, nh, nc, z.tr, CA)
    w_up_t = w_up.T
    outs = pl.pallas_call(
        functools.partial(main_kernel, z),
        out_shape=(
            like(frames, BF), like(frames, F32), like(ra_shape, BF), like(y_shape, BF),
            like(tap_shape, BF), like((CA, CC), BF),
        ),
        in_specs=[hbm] * 7 + [vm, hbm],
        out_specs=(vm,) * 6,
        scratch_shapes=[
            bf(*frames), bf(3, C, C), bf(C, CC), bf(C, CC), bf(480, CC), bf(2 * HD, CC), bf(C, CC), bf(*frames),
            bf(*frames[1:]), bf(*frames[1:]), bf(2, C, z.cells), bf(*frames), bf(*frames[1:]), bf(*frames[1:]),
            f32(2, C, z.cells),
            bf(3, C, C), bf(768, CC), bf(CA, 768), bf(LW, 768), bf(256, CA), bf(256, LW), bf(CA, CA),
            bf(nf, 8, CA), bf(nf, 8, CA), bf(nf, 8, CA), bf(nf, 8, CA),
            bf(nh, z.tok, CA), bf(nh, z.tok, CA), bf(nh * z.tok, 768), bf(nh * z.tok, 256),
            bf(nh, z.tok, LW), bf(nh, z.tok, LW), bf(nf, 8, CA), bf(nf, 8, CA),
            bf(*ra_shape), bf(nc, z.nr, 8, RAW), bf(nc, z.nr, 8, RAW), bf(nc, z.nr, 8, RAW),
            bf(*tap_shape), bf(nh, nc, z.tr, CA), bf(nh, nc, z.tr, CA), bf(nh, nc, z.tr, CA),
            bf(nc, z.tr, CA), bf(nc, z.tr, CA),
            bf(z.na, z.ns, 8, CC), bf(nh, z.ns, 8, CC), f32(z.ns, 8, CC),
            bf(nc, 2, z.nr, 8, CA), bf(nc, 2, z.ns, 8, CA), bf(nc, z.ns, 8, CA), bf(nc, z.ns, 8, CA), bf(nc, z.ns, 8, CA),
            dma((8,)), dma((nc,)), dma((nc,)), dma((1,)), dma((1,)),
            dma((2,)), dma((2,)), dma((2,)), dma((2,)),
            dma((2, nf)), dma((2, nf)), dma((2, nh)), dma((2, nh)),
            dma((nh,)), dma((nh,)), dma((nf,)), dma((nf,)),
            dma((3,)), dma((3,)), dma((nc,)), dma((nc,)), dma((nc,)), dma((nc,)), dma((nc,)), dma((nc,)),
            dma((nh,)), dma((nh,)), dma((nc,)), dma((nc,)), dma((nc,)), dma((nc,)),
            dma((nh,)), dma((nh,)), dma((nh,)), dma((nh,)),
            dma((nh,)), dma((nh,)), dma((nh,)), dma((nh,)), dma((2, nc)), dma((2, nc)), dma((2, nc)), dma((2, nc)),
        ],
        compiler_params=pltpu.CompilerParams(
            collective_id=0, has_side_effects=True, vmem_limit_bytes=36 * 1024 * 1024
        ),
    )(
        far(jnp.swapaxes(clip, 2, 3)), far(w_time), far(w_down), far(w_embed), far(w_qkv.T), far(w_out),
        far(w_up_t), embed_row, far(jnp.swapaxes(cotangent, 2, 3)),
    )
    out, grad_clip, ra_full, y_full, tap_full, w_aug = outs
    grads = pl.pallas_call(
        functools.partial(final_kernel, z),
        out_shape=(
            like(frames, BF), like(frames, F32), like((960, C), F32), like((C, CC), F32), like((C, CC), F32),
            like((480, CC), F32), like((2 * HD, CC), F32), like((C, CC), F32),
        ),
        in_specs=[vm] * 4 + [hbm, vm, vm, vm],
        out_specs=(hbm,) * 8,
        scratch_shapes=[
            bf(C, CC),
            f32(960, C), f32(C, CC), f32(C, CC), f32(480, CC), f32(2 * HD, CC), f32(C, CC),
            dma((1,)), dma((8,)),
        ],
        compiler_params=pltpu.CompilerParams(vmem_limit_bytes=36 * 1024 * 1024),
    )(
        ra_full, y_full.reshape(nf, 2, z.nr, 8, CC), tap_full, w_aug, far(w_up_t), embed_row,
        out, grad_clip,
    )
    out, grad_clip, grad_time, grad_down, grad_embed, grad_qkv, grad_out, grad_up = grads
    return (
        jnp.swapaxes(out, 2, 3),
        jnp.swapaxes(grad_clip, 2, 3),
        grad_time.reshape(3, C, C),
        grad_down,
        grad_embed,
        grad_qkv.T,
        grad_out,
        grad_up.T,
    )


def solution(mesh, cols=128):
    z = Sizes(mesh.shape["frames"], mesh.shape["heads"], cols)
    return jax.shard_map(
        functools.partial(shards, z),
        mesh=mesh,
        in_specs=(
            P("frames", "heads", None, None),
            P(),
            P(),
            P(),
            P(None, "heads"),
            P("heads", None),
            P(),
            P(),
            P("frames", "heads", None, None),
        ),
        out_specs=(
            P("frames", "heads", None, None),
            P("frames", "heads", None, None),
            P(),
            P(),
            P(),
            P(None, "heads"),
            P("heads", None),
            P(),
        ),
        check_vma=False,
    )
```
